32 devices in a mesh: nest: 4 (over x, core), py: 2 (over y), px: 4 (over z).
Axes of the slice: x: 2, y: 2, z: 4, core: 2. Of those that a mesh axis runs over, the one named last changes fastest.
Arguments:
- initial_state: float32 [4, 4, 256, 256], P('nest', None, 'px', 'py'), may hold values from -6 to 6
- drive_modes: float32 [3, 4, 64, 64], replicated, may hold values from -6 to 6
- relax_rates: float32 [4, 4], P('nest'), may hold values from 0.2 to 0.9
- nest_offsets: int32 [4, 2], replicated, may hold values from 0 to 170
Outputs:
- final_state: float32 [4, 4, 256, 256], P('nest', None, 'px', 'py')
- final_modes: float32 [4, 4, 64, 64], P('nest')
The draws below stay inside these ranges and needn't reach their ends.
Inputs may be any that keep to these rules, and one draw needn't show every extreme that they name: `nest_offsets`: row 0 is not read.
All inputs are finite; a program needn't handle non-finite values.
Results may differ from the reference program's by a relative error of at most 0.0001.
Values sent between devices are 32-bit elements; how exact they have to be, the bound alone decides.
A program may use at most 64 MiB of HBM per device.

```python
import math
import jax
import jax.numpy as jnp
from jax import lax

LEV = 4
M = 64
RATIO = 3
WIN = 3
NX = 256
NY = 256
N_NEST = 4


def touch_ends(array, stream_key, smallest, high):
    place = [jax.random.randint(jax.random.fold_in(stream_key, axis), (), 0, length) for axis, length in enumerate(array.shape)]
    longest = array.shape.index(max(array.shape))
    next_to = place[:longest] + [(place[longest] + 1) % array.shape[longest]] + place[longest + 1:]
    return array.at[tuple(place)].set(smallest).at[tuple(next_to)].set(high)


def block_scale(rng, shape, split, least, largest):
    loudness = 1.0
    for dim, parts in split:
        heights = jax.random.uniform(jax.random.fold_in(jax.random.fold_in(rng, 6), dim), (parts,), jnp.float32, least / len(split), largest / len(split))
        loudness = loudness * jnp.repeat(jnp.exp(heights), shape[dim] // parts).reshape((-1,) + (1,) * (len(shape) - 1 - dim))
    return loudness


def bell_draw(key, shape, scale, most, split=(), kind=jnp.bfloat16):
    entries = scale * jax.random.normal(key, shape, jnp.float32)
    if split:
        entries = entries * block_scale(key, shape, split, -0.22, 0.18)
    return jnp.clip(entries, -most, most).astype(kind)


def setup_inputs(seed: int = 0) -> dict:
    splits = jax.random.split(jax.random.key(seed), 5)
    return {
        "initial_state": bell_draw(splits[0], (N_NEST, LEV, NX, NY), 1.0, 6.0, ((0, 4), (2, 4), (3, 2)), jnp.float32),
        "drive_modes": bell_draw(splits[1], (WIN, LEV, M, M), 1.0, 6.0, (), jnp.float32),
        "relax_rates": jnp.clip(jnp.exp(math.log(0.9) - 1.50407736 * jax.random.uniform(splits[2], (N_NEST, LEV), jnp.float32) ** block_scale(splits[2], (N_NEST, LEV), ((0, 4),), -0.2, 0.2)), 0.2, 0.9),
        "nest_offsets": touch_ends(jax.random.randint(splits[3], (N_NEST, 2), 0, min(NX, NY) - min(NX, NY) // RATIO), jax.random.fold_in(splits[3], 1), 0, (min(NX, NY) - min(NX, NY) // RATIO) - 1).astype(jnp.int32),
    }


highest = lax.Precision.HIGHEST
diffusion_rate = 0.2

def cosine_basis(numerator, cell_count, mode_count, refine):
    wavenum = jnp.arange(mode_count, dtype=jnp.int32)
    product = wavenum[None, :] * numerator[:, None] % (4 * refine * cell_count)
    angles = jnp.pi * product.astype(jnp.float32) / (2.0 * refine * cell_count)
    weight = jnp.where(wavenum == 0, 1.0, 2.0).astype(jnp.float32) / cell_count
    return jnp.sqrt(weight)[None, :] * jnp.cos(angles)

def diffuse(field_now):
    padded = jnp.pad(field_now, ((0, 0), (1, 1), (1, 1)))
    beside_all = padded[:, 2:, 1:-1] + padded[:, :-2, 1:-1] + padded[:, 1:-1, 2:] + padded[:, 1:-1, :-2]
    return field_now + diffusion_rate * (beside_all - 4.0 * field_now)

def reference(initial_state, drive_modes, relax_rates, nest_offsets):
    cells_x = jnp.arange(NX, dtype=jnp.int32)
    cells_y = jnp.arange(NY, dtype=jnp.int32)
    row_basis = cosine_basis(2 * cells_x + 1, NX, M, 1)
    col_basis = cosine_basis(2 * cells_y + 1, NY, M, 1)
    interp_maps = []
    for domain in range(N_NEST):
        shifted_x = cosine_basis(2 * RATIO * nest_offsets[domain, 0] + 2 * cells_x + 1, NX, M, RATIO)
        shifted_y = cosine_basis(2 * RATIO * nest_offsets[domain, 1] + 2 * cells_y + 1, NY, M, RATIO)
        interp_maps.append((jnp.dot(row_basis.T, shifted_x, precision=highest), jnp.dot(col_basis.T, shifted_y, precision=highest)))
    fields = [initial_state[domain] for domain in range(N_NEST)]
    coeffs = [None] * N_NEST
    for window in range(WIN):
        for domain in range(N_NEST):
            stepped = diffuse(fields[domain])
            partial_rows = jnp.einsum('lxy,ym->lxm', stepped, col_basis, precision=highest)
            own = jnp.einsum('xj,lxm->ljm', row_basis, partial_rows, precision=highest)
            if domain == 0:
                target = drive_modes[window]
            else:
                row_map, col_map = interp_maps[domain]
                target = jnp.einsum('jp,lpq,mq->ljm', row_map, coeffs[domain - 1], col_map, precision=highest)
            change = relax_rates[domain][:, None, None] * (target - own)
            coeffs[domain] = own + change
            back_rows = jnp.einsum('ljm,ym->ljy', change, col_basis, precision=highest)
            fields[domain] = stepped + jnp.einsum('xj,ljy->lxy', row_basis, back_rows, precision=highest)
    return (jnp.stack(fields), jnp.stack(coeffs))
```

```python
import functools
import math

import jax
import jax.numpy as jnp
import numpy as np
from jax import lax
from jax.experimental import pallas as pl
from jax.experimental.pallas import tpu as pltpu
from jax.sharding import PartitionSpec as P

RATIO = 3
RATE = 0.2
MESH = pl.DeviceIdType.MESH
F32, BF16 = jnp.float32, jnp.bfloat16


def basis(cells, modes, refine, fn=np.cos):
    j = np.arange(modes, dtype=np.int64)
    q = 2 * np.arange(cells, dtype=np.int64) + 1
    product = (j[None, :] * q[:, None]) % (4 * refine * cells)
    weight = np.where(j == 0, 1.0, 2.0) / cells
    return np.sqrt(weight)[None, :] * fn(np.pi * product / (2.0 * refine * cells))


def half_step(table):
    pad = np.pad(table, ((1, 1), (0, 0)))
    return (0.5 - 2 * RATE) * table + RATE * (pad[2:] + pad[:-2])


def powers(table, count):
    out = [table]
    for _ in range(count):
        out.append(half_step(out[-1]))
    return out


def halves(table):
    high = np.asarray(table, np.float32).astype(BF16)
    low = (np.asarray(table, np.float64) - high.astype(np.float64)).astype(np.float32)
    return np.stack([high, low.astype(BF16)])


def split(x):
    high = x.astype(BF16)
    return high, (x - high.astype(F32)).astype(BF16)


def mm(a, b):
    return lax.dot_general(a, b, (((1,), (0,)), ((), ())), preferred_element_type=F32)


def dot3(a, b):
    a = a if isinstance(a, tuple) else split(a)
    b = b if isinstance(b, tuple) else split(b)
    return mm(a[0], b[0]) + (mm(a[0], b[1]) + mm(a[1], b[0]))


def loop(n, fn):
    if n <= 16:
        for i in range(n):
            fn(i)
    else:
        lax.fori_loop(0, n, lambda i, c: (fn(i), c)[1], 0)


def kernel(
    dims, owners,
    field, drive, relax, offs, u_hbm, ut_hbm, v_hbm, vt_hbm, small_hbm,
    out, modes,
    fvm, fbuf, gbuf, fin, par, cbuf, tx, u_t, ut_t, v_t, vt_t, small,
    load_sem, a_send, a_recv, c_send, c_recv, f_send, f_recv, m_send, m_recv,
):
    nests, PY, PX, L, cx, cy, m, W = dims
    G, nx, ny = PY * PX, cx * PX, cy * PY
    k, py, px = lax.axis_index("nest"), lax.axis_index("py"), lax.axis_index("px")
    me = px * PY + py
    mine = [me == o for o in owners]
    level = sum(jnp.where(c, l, 0) for l, c in enumerate(mine))
    is_owner = functools.reduce(jnp.logical_or, mine)

    def at(g):
        return (k, g % PY, g // PY)

    def plain(g):
        return functools.reduce(jnp.logical_and, [g != o for o in owners])

    barrier = pltpu.get_barrier_semaphore()
    for l, o in enumerate(owners):
        @pl.when(me != o)
        def _():
            pl.semaphore_signal(barrier, inc=1, device_id=at(o), device_id_type=MESH)

    @pl.when(is_owner)
    def _():
        def greet(g):
            @pl.when(plain(g))
            def _():
                pl.semaphore_signal(barrier, inc=1, device_id=at(g), device_id_type=MESH)
        loop(G, greet)

        @pl.when(k > 0)
        def _():
            pl.semaphore_signal(barrier, inc=1, device_id=(k - 1, py, px), device_id_type=MESH)

        @pl.when(k < nests - 1)
        def _():
            pl.semaphore_signal(barrier, inc=1, device_id=(k + 1, py, px), device_id_type=MESH)

    loads = [pltpu.make_async_copy(field.at[0, l], fvm.at[l], load_sem.at[l]) for l in range(L)]
    for c in loads:
        c.start()
    tables = [
        pltpu.make_async_copy(src, dst, load_sem.at[L + i])
        for i, (src, dst) in enumerate(
            [(v_hbm, v_t), (ut_hbm, ut_t), (small_hbm, small), (u_hbm, u_t), (vt_hbm, vt_t)]
        )
    ]
    get_drive = pltpu.make_async_copy(drive.at[:, level], par, load_sem.at[L + 5])

    @pl.when(is_owner)
    def _():
        for c in tables:
            c.start()

        @pl.when(k == 0)
        def _():
            get_drive.start()

        pl.semaphore_wait(
            barrier, G - 1 + jnp.where(k > 0, 1, 0) + jnp.where(k < nests - 1, 1, 0)
        )

    @pl.when(jnp.logical_not(is_owner))
    def _():
        pl.semaphore_wait(barrier, L)

    def patch(ref, g, shift):
        return ref.at[
            pl.ds(pl.multiple_of((g // PY) * cx + shift, 8), cx),
            pl.ds(pl.multiple_of((g % PY) * cy, 128), cy),
        ]

    def gather(l):
        return pltpu.make_async_remote_copy(
            src_ref=fvm.at[l], dst_ref=patch(fbuf, me, 8), send_sem=a_send.at[l],
            recv_sem=a_recv.at[me], device_id=at(owners[l]), device_id_type=MESH,
        )

    def keep(l):
        return pltpu.make_async_copy(fvm.at[l], patch(fbuf, me, 8), a_send.at[l])

    for l, o in enumerate(owners):
        loads[l].wait()

        @pl.when(me != o)
        def _():
            gather(l).start()

        @pl.when(me == o)
        def _():
            keep(l).start()

    @pl.when(is_owner)
    def _():
        edge = jnp.zeros((8, ny), F32)
        for ref in (fbuf, gbuf):
            ref[0:8, :] = edge
            ref[nx + 8 : nx + 16, :] = edge
        tables[2].wait()
        gain = relax[0, level]
        rest = 2.0 * (1.0 - gain)

        def turn(cells, dim, axis):
            number = lax.broadcasted_iota(jnp.int32, (m, m), dim).astype(F32)
            product = number * (2 * RATIO * offs[k, axis]).astype(F32)
            period = float(4 * RATIO * cells)
            product = product - period * jnp.floor(product * (1.0 / period))
            angle = product * (math.pi / (2.0 * RATIO * cells))
            return jnp.cos(angle), jnp.sin(angle)

        eye = jnp.where(
            lax.broadcasted_iota(jnp.int32, (m, m), 0) == lax.broadcasted_iota(jnp.int32, (m, m), 1),
            1.0, 0.0,
        ).astype(F32)
        cos_x, sin_x = turn(nx, 1, 0)
        cos_y, sin_y = turn(ny, 0, 1)
        row = jnp.where(k == 0, eye, small[0] * cos_x - small[1] * sin_x)
        col = jnp.where(k == 0, eye, small[2] * cos_y - small[3] * sin_y)
        a1, b1 = split(small[4]), split(small[7])
        a2 = split(small[5] - gain * small[6])
        b2 = split(small[8] - gain * small[9])
        f0, g0 = split(row), split(col)
        f1, f2 = split(dot3(a1, f0)), split(dot3(a2, f0))
        g1, g2 = split(dot3(g0, b1)), split(dot3(g0, b2))

        def follow():
            c1, c2, c3 = (split(par[w]) for w in range(W))
            y10, y20, y30 = dot3(c1, g0), dot3(c2, g0), dot3(c3, g0)
            y11, y21, y12 = dot3(c1, g1), dot3(c2, g1), dot3(c1, g2)
            y10s = split(y10)
            tx[0] = dot3(f0, y10s)
            tx[1] = dot3(f0, y20)
            tx[2] = dot3(f0, y30)
            tx[3] = dot3(f1, y10s) + dot3(f0, y11)
            tx[4] = dot3(f0, y21 + y12) + dot3(f1, y20 + rest * y11) + dot3(f2, y10s)

        @pl.when(k == 0)
        def _():
            get_drive.wait()
            follow()

        tables[0].wait()
        tables[1].wait()

        def arrive(g):
            @pl.when(g == me)
            def _():
                keep(level).wait()

            @pl.when(g != me)
            def _():
                pltpu.make_async_remote_copy(
                    src_ref=fvm.at[0], dst_ref=patch(fbuf, g, 8), send_sem=a_send.at[0],
                    recv_sem=a_recv.at[g], device_id=at(me), device_id_type=MESH,
                ).wait_recv()
        loop(G, arrive)

        step = min(nx, 256)
        both = jnp.zeros(((W + 1) * m, (W + 1) * m), F32)
        for r in range(0, nx, step):
            part = dot3(fbuf[8 + r : 8 + r + step, :], (v_t[0], v_t[1]))
            both = both + dot3((ut_t[0, :, r : r + step], ut_t[1, :, r : r + step]), part)

        def block(i, j):
            return both[i * m : (i + 1) * m, j * m : (j + 1) * m]

        s1, s2, s3 = (
            sum(float(math.comb(w, i)) * block(i, w - i) for i in range(w + 1)) for w in (1, 2, 3)
        )
        s1s, s2s = split(s1), split(s2)
        z11 = dot3(s1s, b1)
        x2 = dot3(a1, s1s) + z11
        x3 = dot3(s2s, b1) + dot3(s1s, b2) + dot3(a1, s2 + rest * z11) + dot3(a2, s1s)
        o2, o3 = s2 - gain * x2, s3 - gain * x3

        rows = 32

        def free():
            col_id = lax.broadcasted_iota(jnp.int32, (rows, ny), 1)

            def sweep(src, dst):
                def some(r, carry):
                    start = pl.multiple_of(r * rows, 8)
                    wide = src[pl.ds(start, rows + 16), :]
                    mid = wide[8 : rows + 8]
                    near = wide[7 : rows + 7] + wide[9 : rows + 9]
                    near = near + jnp.where(col_id == 0, 0.0, pltpu.roll(mid, 1, 1))
                    near = near + jnp.where(col_id == ny - 1, 0.0, pltpu.roll(mid, ny - 1, 1))
                    dst[pl.ds(pl.multiple_of(start + 8, 8), rows), :] = mid + RATE * (near - 4.0 * mid)
                    return carry
                lax.fori_loop(0, nx // rows, some, 0)
            sweep(fbuf, gbuf)
            sweep(gbuf, fbuf)
            sweep(fbuf, gbuf)

        chain_in = pltpu.make_async_remote_copy(
            src_ref=cbuf, dst_ref=par, send_sem=c_send, recv_sem=c_recv,
            device_id=(k, py, px), device_id_type=MESH,
        )
        chain_out = pltpu.make_async_remote_copy(
            src_ref=cbuf, dst_ref=par, send_sem=c_send, recv_sem=c_recv,
            device_id=(k + 1, py, px), device_id_type=MESH,
        )

        @pl.when(k > 0)
        def _():
            free()
            chain_in.wait_recv()
            follow()

        own2, own3 = o2 + gain * tx[3], o3 + gain * tx[4]
        d1, d2, d3 = gain * (tx[0] - s1), gain * (tx[1] - own2), gain * (tx[2] - own3)
        cbuf[0] = s1 + d1
        cbuf[1] = own2 + d2
        cbuf[2] = own3 + d3

        @pl.when(k < nests - 1)
        def _():
            chain_out.start()

        def tell(g):
            return pltpu.make_async_remote_copy(
                src_ref=cbuf.at[W - 1], dst_ref=modes.at[0, level], send_sem=m_send.at[g],
                recv_sem=m_recv.at[level], device_id=at(g), device_id_type=MESH,
            )

        def tell_start(g):
            @pl.when(g != me)
            def _():
                tell(g).start()
        loop(G, tell_start)
        own_modes = pltpu.make_async_copy(cbuf.at[W - 1], modes.at[0, level], m_recv.at[level])
        own_modes.start()

        @pl.when(k == 0)
        def _():
            free()

        tables[3].wait()
        tables[4].wait()
        e1, e2, e3 = split(d1), split(d2), split(d3)
        vt = [(vt_t[0, i * m : (i + 1) * m, :], vt_t[1, i * m : (i + 1) * m, :]) for i in range(W)]
        w0 = dot3(e3, vt[0]) + dot3(e2, vt[1]) + dot3(e1, vt[2])
        w1 = dot3(e2, vt[0]) + 2.0 * dot3(e1, vt[1])
        w2 = dot3(e1, vt[0])
        mixed = split(jnp.concatenate([w0, w1, w2], 0))

        def send_back(g):
            return pltpu.make_async_remote_copy(
                src_ref=patch(fin, g, 0), dst_ref=out.at[0, level], send_sem=f_send.at[g],
                recv_sem=f_recv.at[level], device_id=at(g), device_id_type=MESH,
            )

        own_out = pltpu.make_async_copy(patch(fin, me, 0), out.at[0, level], f_recv.at[level])

        def finish(r):
            here = pl.ds(pl.multiple_of(r * cx, 8), cx)
            there = pl.ds(pl.multiple_of(r * cx + 8, 8), cx)
            fin[here, :] = gbuf[there, :] + dot3((u_t[0, here, :], u_t[1, here, :]), mixed)

            def give(j):
                g = r * PY + j

                @pl.when(g != me)
                def _():
                    send_back(g).start()

                @pl.when(g == me)
                def _():
                    own_out.start()
            loop(PY, give)
        loop(PX, finish)

        own_out.wait()
        own_modes.wait()

        def drain(g):
            @pl.when(g != me)
            def _():
                tell(g).wait_send()
                send_back(g).wait_send()
        loop(G, drain)

        @pl.when(k < nests - 1)
        def _():
            chain_out.wait_send()

    for l, o in enumerate(owners):
        @pl.when(me != o)
        def _():
            pltpu.make_async_remote_copy(
                src_ref=cbuf.at[W - 1], dst_ref=modes.at[0, l], send_sem=m_send.at[0],
                recv_sem=m_recv.at[l], device_id=at(o), device_id_type=MESH,
            ).wait_recv()
            pltpu.make_async_remote_copy(
                src_ref=patch(fin, 0, 0), dst_ref=out.at[0, l], send_sem=f_send.at[0],
                recv_sem=f_recv.at[l], device_id=at(o), device_id_type=MESH,
            ).wait_recv()
            gather(l).wait_send()


def body(dims, owners, initial_state, drive_modes, relax_rates, nest_offsets):
    nests, PY, PX, L, cx, cy, m, W = dims
    G, nx, ny = PY * PX, cx * PX, cy * PY
    rp, cp = powers(basis(nx, m, 1), W), powers(basis(ny, m, 1), W)
    u, v = np.concatenate(rp, 1), np.concatenate(cp, 1)
    a = [rp[0].T @ t for t in rp]
    b = [cp[0].T @ t for t in cp]
    even_x, odd_x = (rp[0].T @ basis(nx, m, RATIO, f) for f in (np.cos, np.sin))
    even_y, odd_y = ((cp[0].T @ basis(ny, m, RATIO, f)).T for f in (np.cos, np.sin))
    small = np.stack(
        [even_x, odd_x, even_y, odd_y, a[1], a[2], a[1] @ a[1], b[1], b[2], b[1] @ b[1]]
    ).astype(np.float32)
    wide, deep = W * m, (W + 1) * m
    tables = (halves(u[:, :wide]), halves(u.T), halves(v), halves(v.T[:wide]))
    any_space = pl.BlockSpec(memory_space=pl.ANY)
    vmem = pl.BlockSpec(memory_space=pltpu.VMEM)
    smem = pl.BlockSpec(memory_space=pltpu.SMEM)
    dma = pltpu.SemaphoreType.DMA
    return pl.pallas_call(
        functools.partial(kernel, dims, owners),
        out_shape=(
            jax.ShapeDtypeStruct((1, L, cx, cy), F32),
            jax.ShapeDtypeStruct((1, L, m, m), F32),
        ),
        in_specs=[any_space, any_space, smem, smem] + [any_space] * 5,
        out_specs=(vmem, vmem),
        scratch_shapes=[
            pltpu.VMEM((L, cx, cy), F32),
            pltpu.VMEM((nx + 16, ny), F32),
            pltpu.VMEM((nx + 16, ny), F32),
            pltpu.VMEM((nx, ny), F32),
            pltpu.VMEM((W, m, m), F32),
            pltpu.VMEM((W, m, m), F32),
            pltpu.VMEM((5, m, m), F32),
            pltpu.VMEM((2, nx, wide), BF16),
            pltpu.VMEM((2, deep, nx), BF16),
            pltpu.VMEM((2, ny, deep), BF16),
            pltpu.VMEM((2, wide, ny), BF16),
            pltpu.VMEM((10, m, m), F32),
            dma((L + 6,)),
            dma((L,)),
            dma((G,)),
            dma,
            dma,
            dma((G,)),
            dma((L,)),
            dma((G,)),
            dma((L,)),
        ],
        compiler_params=pltpu.CompilerParams(collective_id=0, has_side_effects=True),
    )(initial_state, drive_modes, relax_rates, nest_offsets,
      *(jnp.asarray(t) for t in tables), jnp.asarray(small))


def solution(mesh):
    nests, PY, PX = (mesh.shape[n] for n in ("nest", "py", "px"))
    spec = P("nest", None, "px", "py")

    def local(initial_state, drive_modes, relax_rates, nest_offsets):
        _, L, cx, cy = initial_state.shape
        W, _, m, _ = drive_modes.shape
        places = sorted(
            range(PY * PX),
            key=lambda g: (abs(2 * (g // PY) - PX + 1) + abs(2 * (g % PY) - PY + 1), g),
        )
        dims = (nests, PY, PX, L, cx, cy, m, W)
        return body(dims, tuple(places[:L]), initial_state, drive_modes, relax_rates, nest_offsets)

    return jax.shard_map(
        local,
        mesh=mesh,
        in_specs=(spec, P(), P("nest", None), P()),
        out_specs=(spec, P("nest", None, None, None)),
        check_vma=False,
    )
```

```python
import functools
import math

import jax
import jax.numpy as jnp
import numpy as np
from jax import lax
from jax.experimental import pallas as pl
from jax.experimental.pallas import tpu as pltpu
from jax.sharding import PartitionSpec as P

RATIO = 3
RATE = 0.2
MESH = pl.DeviceIdType.MESH
F32, BF16 = jnp.float32, jnp.bfloat16


def basis(cells, modes, refine, fn=np.cos):
    j = np.arange(modes, dtype=np.int64)
    q = 2 * np.arange(cells, dtype=np.int64) + 1
    product = (j[None, :] * q[:, None]) % (4 * refine * cells)
    weight = np.where(j == 0, 1.0, 2.0) / cells
    return np.sqrt(weight)[None, :] * fn(np.pi * product / (2.0 * refine * cells))


def half_step(table):
    pad = np.pad(table, ((1, 1), (0, 0)))
    return (0.5 - 2 * RATE) * table + RATE * (pad[2:] + pad[:-2])


def powers(table, count):
    out = [table]
    for _ in range(count):
        out.append(half_step(out[-1]))
    return out


def halves(table):
    high = np.asarray(table, np.float32).astype(BF16)
    low = (np.asarray(table, np.float64) - high.astype(np.float64)).astype(np.float32)
    return np.stack([high, low.astype(BF16)])


def split(x):
    high = x.astype(BF16)
    return high, (x - high.astype(F32)).astype(BF16)


def mm(a, b):
    return lax.dot_general(a, b, (((1,), (0,)), ((), ())), preferred_element_type=F32)


def dot3(a, b):
    a = a if isinstance(a, tuple) else split(a)
    b = b if isinstance(b, tuple) else split(b)
    return mm(a[0], b[0]) + (mm(a[0], b[1]) + mm(a[1], b[0]))


def pack(x):
    h = x.shape[0] // 2
    return jnp.concatenate([x[:h], x[h:]], 1)


def unpack(x):
    h = x.shape[1] // 2
    return jnp.concatenate([x[:, :h], x[:, h:]], 0)


def loop(n, fn):
    if n <= 16:
        for i in range(n):
            fn(i)
    else:
        lax.fori_loop(0, n, lambda i, c: (fn(i), c)[1], 0)


def kernel(
    dims, owners,
    field, drive, relax, offs, u_hbm, ut_hbm, v_hbm, vt_hbm, small_hbm,
    out, modes,
    fvm, fbuf, gbuf, fin, start, par, cbuf, sib, obuf, lead, glead, mbuf, tx,
    u_t, ut_t, v_t, vt_t, small,
    load_sem, a_send, a_recv, c_send, c_recv, o_sem, g_sem, f_send, f_recv, m_send, m_recv,
):
    nests, PY, PX, L, cx, cy, m, W = dims
    G, nx, ny = PY * PX, cx * PX, cy * PY
    k, py, px = lax.axis_index("nest"), lax.axis_index("py"), lax.axis_index("px")
    me = px * PY + py
    mine = [me == o for o in owners]
    level = sum(jnp.where(c, l, 0) for l, c in enumerate(mine))
    is_owner = functools.reduce(jnp.logical_or, mine)

    def at(g):
        return (k, g % PY, g // PY)

    def plain(g):
        return functools.reduce(jnp.logical_and, [g != o for o in owners])

    odd = k % 2 == 1
    hops = [
        (-1, k > 0),
        (1, k < nests - 1),
        (-2, jnp.logical_and(odd, k > 2)),
        (2, jnp.logical_and(odd, k < nests - 2)),
    ]
    barrier = pltpu.get_barrier_semaphore()
    for l, o in enumerate(owners):
        @pl.when(me != o)
        def _():
            pl.semaphore_signal(barrier, inc=1, device_id=at(o), device_id_type=MESH)

    @pl.when(is_owner)
    def _():
        def greet(g):
            @pl.when(plain(g))
            def _():
                pl.semaphore_signal(barrier, inc=1, device_id=at(g), device_id_type=MESH)
        loop(G, greet)

        for hop, cond in hops:
            @pl.when(cond)
            def _():
                pl.semaphore_signal(
                    barrier, inc=1, device_id=(k + hop, py, px), device_id_type=MESH
                )

    def hop_copy(src, dst, send_sem, recv_sem, hop):
        return pltpu.make_async_remote_copy(
            src_ref=src, dst_ref=dst, send_sem=send_sem, recv_sem=recv_sem,
            device_id=(k + hop, py, px), device_id_type=MESH,
        )

    gain_out = hop_copy(lead, glead, g_sem.at[0], g_sem.at[1], 1)
    gain_in = hop_copy(lead, glead, g_sem.at[0], g_sem.at[1], -1)
    own_out_copy = hop_copy(obuf, sib, o_sem.at[0], o_sem.at[1], 1)
    own_in = hop_copy(obuf, sib, o_sem.at[0], o_sem.at[1], -1)
    chain_out = [hop_copy(cbuf, par, c_send.at[h - 1], c_recv, h) for h in (1, 2)]
    chain_in = hop_copy(cbuf, par, c_send.at[0], c_recv, -1)

    loads = [pltpu.make_async_copy(field.at[0, l], fvm.at[l], load_sem.at[l]) for l in range(L)]
    for c in loads:
        c.start()
    tables = [
        pltpu.make_async_copy(src, dst, load_sem.at[L + i])
        for i, (src, dst) in enumerate(
            [(v_hbm, v_t), (ut_hbm, ut_t), (small_hbm, small), (u_hbm, u_t), (vt_hbm, vt_t)]
        )
    ]
    get_drive = pltpu.make_async_copy(drive.at[:, level], start, load_sem.at[L + 5])

    @pl.when(is_owner)
    def _():
        for c in tables:
            c.start()

        @pl.when(k < 2)
        def _():
            get_drive.start()

        pl.semaphore_wait(barrier, G - 1 + sum(jnp.where(c, 1, 0) for _, c in hops))

    @pl.when(jnp.logical_not(is_owner))
    def _():
        pl.semaphore_wait(barrier, L)

    def patch(ref, g, shift):
        return ref.at[
            pl.ds(pl.multiple_of((g // PY) * cx + shift, 8), cx),
            pl.ds(pl.multiple_of((g % PY) * cy, 128), cy),
        ]

    def gather(l):
        return pltpu.make_async_remote_copy(
            src_ref=fvm.at[l], dst_ref=patch(fbuf, me, 8), send_sem=a_send.at[l],
            recv_sem=a_recv.at[me], device_id=at(owners[l]), device_id_type=MESH,
        )

    def keep(l):
        return pltpu.make_async_copy(fvm.at[l], patch(fbuf, me, 8), a_send.at[l])

    for l, o in enumerate(owners):
        loads[l].wait()

        @pl.when(me != o)
        def _():
            gather(l).start()

        @pl.when(me == o)
        def _():
            keep(l).start()

    @pl.when(is_owner)
    def _():
        edge = jnp.zeros((8, ny), F32)
        for ref in (fbuf, gbuf):
            ref[0:8, :] = edge
            ref[nx + 8 : nx + 16, :] = edge
        gain = relax[0, level]
        lead[...] = jnp.full(lead.shape, gain, F32)

        @pl.when(jnp.logical_and(jnp.logical_not(odd), k < nests - 1))
        def _():
            gain_out.start()

        tables[2].wait()

        def turn(kk, cells, dim, axis):
            number = lax.broadcasted_iota(jnp.int32, (m, m), dim).astype(F32)
            product = number * (2 * RATIO * offs[axis, kk]).astype(F32)
            period = float(4 * RATIO * cells)
            product = product - period * jnp.floor(product * (1.0 / period))
            angle = product * (math.pi / (2.0 * RATIO * cells))
            return jnp.cos(angle), jnp.sin(angle)

        def flat(kk):
            eye = jnp.where(
                lax.broadcasted_iota(jnp.int32, (m, m), 0)
                == lax.broadcasted_iota(jnp.int32, (m, m), 1),
                1.0, 0.0,
            ).astype(F32)
            cos_x, sin_x = turn(kk, nx, 1, 0)
            cos_y, sin_y = turn(kk, ny, 0, 1)
            row = jnp.where(kk == 0, eye, small[0] * cos_x - small[1] * sin_x)
            col = jnp.where(kk == 0, eye, small[2] * cos_y - small[3] * sin_y)
            return split(row), split(col)

        a1, b1 = split(small[4]), split(small[7])

        def curved(rate):
            return split(small[5] - rate * small[6]), split(small[8] - rate * small[9])

        def maps(kk, rate):
            a2, b2 = curved(rate)
            f0, g0 = flat(kk)
            f1, f2 = split(dot3(a1, f0)), split(dot3(a2, f0))
            g1, g2 = split(dot3(g0, b1)), split(dot3(g0, b2))
            return f0, f1, f2, g0, g1, g2, 2.0 * (1.0 - rate)

        def follow(cs, ms):
            f0, f1, f2, g0, g1, g2, rest = ms
            c1, c2, c3 = (split(c) for c in cs)
            y10, y20, y30 = dot3(c1, g0), dot3(c2, g0), dot3(c3, g0)
            y11, y21, y12 = dot3(c1, g1), dot3(c2, g1), dot3(c1, g2)
            y10s = split(y10)
            return (
                dot3(f0, y10s),
                dot3(f0, y20),
                dot3(f0, y30),
                dot3(f1, y10s) + dot3(f0, y11),
                dot3(f0, y21 + y12) + dot3(f1, y20 + rest * y11) + dot3(f2, y10s),
            )

        def nudge(own, moved, rate):
            own2, own3 = own[1] + rate * moved[3], own[2] + rate * moved[4]
            d1, d2, d3 = rate * (moved[0] - own[0]), rate * (moved[1] - own2), rate * (moved[2] - own3)
            return (d1, d2, d3), (own[0] + d1, own2 + d2, own3 + d3)

        own_maps = maps(k, gain)

        @pl.when(odd)
        def _():
            gain_in.wait_recv()
            lead[...] = glead[...]

        lead_gain = lead[0:1, 0:m]
        lead_maps = maps(k - k % 2, lead_gain)

        def first(cs):
            for i, x in enumerate(follow(cs, lead_maps)):
                tx[i] = x

        @pl.when(k < 2)
        def _():
            get_drive.wait()
            first([start[w] for w in range(W)])

        tables[0].wait()
        tables[1].wait()

        def arrive(g):
            @pl.when(g == me)
            def _():
                keep(level).wait()

            @pl.when(g != me)
            def _():
                pltpu.make_async_remote_copy(
                    src_ref=fvm.at[0], dst_ref=patch(fbuf, g, 8), send_sem=a_send.at[0],
                    recv_sem=a_recv.at[g], device_id=at(me), device_id_type=MESH,
                ).wait_recv()
        loop(G, arrive)

        step = min(nx, 256)
        both = jnp.zeros(((W + 1) * m, (W + 1) * m), F32)
        for r in range(0, nx, step):
            part = dot3(fbuf[8 + r : 8 + r + step, :], (v_t[0], v_t[1]))
            both = both + dot3((ut_t[0, :, r : r + step], ut_t[1, :, r : r + step]), part)

        def block(i, j):
            return both[i * m : (i + 1) * m, j * m : (j + 1) * m]

        s1, s2, s3 = (
            sum(float(math.comb(w, i)) * block(i, w - i) for i in range(w + 1)) for w in (1, 2, 3)
        )
        a2, b2 = curved(gain)
        s1s, s2s = split(s1), split(s2)
        z11 = dot3(s1s, b1)
        x2 = dot3(a1, s1s) + z11
        x3 = dot3(s2s, b1) + dot3(s1s, b2) + dot3(a1, s2 + 2.0 * (1.0 - gain) * z11) + dot3(a2, s1s)
        own = (s1, s2 - gain * x2, s3 - gain * x3)

        @pl.when(jnp.logical_and(jnp.logical_not(odd), k < nests - 1))
        def _():
            for w in range(W):
                obuf[w] = pack(own[w])
            own_out_copy.start()

        rows = min(64, nx)

        def free():
            col_id = lax.broadcasted_iota(jnp.int32, (rows, ny), 1)

            def sweep(src, dst):
                def some(r, carry):
                    at_row = pl.multiple_of(r * rows, 8)
                    wide = src[pl.ds(at_row, rows + 16), :]
                    mid = wide[8 : rows + 8]
                    near = wide[7 : rows + 7] + wide[9 : rows + 9]
                    near = near + jnp.where(col_id == 0, 0.0, pltpu.roll(mid, 1, 1))
                    near = near + jnp.where(col_id == ny - 1, 0.0, pltpu.roll(mid, ny - 1, 1))
                    dst[pl.ds(pl.multiple_of(at_row + 8, 8), rows), :] = mid + RATE * (near - 4.0 * mid)
                    return carry
                lax.fori_loop(0, nx // rows, some, 0, unroll=nx // rows <= 4)
            sweep(fbuf, gbuf)
            sweep(gbuf, fbuf)
            sweep(fbuf, gbuf)

        @pl.when(k > 0)
        def _():
            free()

        @pl.when(k > 1)
        def _():
            chain_in.wait_recv()
            first([unpack(par[w]) for w in range(W)])

        @pl.when(odd)
        def _():
            own_in.wait_recv()
            _, above = nudge(
                [unpack(sib[w]) for w in range(W)], [tx[i] for i in range(5)], lead_gain
            )
            for i, x in enumerate(follow(above, own_maps)):
                tx[i] = x

        (d1, d2, d3), now = nudge(own, [tx[i] for i in range(5)], gain)
        for w in range(W):
            cbuf[w] = pack(now[w])
        for h in (1, 2):
            @pl.when(jnp.logical_and(odd, k < nests - h))
            def _():
                chain_out[h - 1].start()

        def tell(g):
            return pltpu.make_async_remote_copy(
                src_ref=cbuf.at[W - 1], dst_ref=mbuf.at[level], send_sem=m_send.at[g],
                recv_sem=m_recv.at[level], device_id=at(g), device_id_type=MESH,
            )

        def tell_start(g):
            @pl.when(g != me)
            def _():
                tell(g).start()
        loop(G, tell_start)
        own_modes = pltpu.make_async_copy(cbuf.at[W - 1], mbuf.at[level], m_recv.at[level])
        own_modes.start()

        @pl.when(k == 0)
        def _():
            free()

        tables[3].wait()
        tables[4].wait()
        e1, e2, e3 = split(d1), split(d2), split(d3)
        vt = [(vt_t[0, i * m : (i + 1) * m, :], vt_t[1, i * m : (i + 1) * m, :]) for i in range(W)]
        w0 = dot3(e3, vt[0]) + dot3(e2, vt[1]) + dot3(e1, vt[2])
        w1 = dot3(e2, vt[0]) + 2.0 * dot3(e1, vt[1])
        w2 = dot3(e1, vt[0])
        mixed = split(jnp.concatenate([w0, w1, w2], 0))

        def send_back(g):
            return pltpu.make_async_remote_copy(
                src_ref=patch(fin, g, 0), dst_ref=out.at[0, level], send_sem=f_send.at[g],
                recv_sem=f_recv.at[level], device_id=at(g), device_id_type=MESH,
            )

        own_out = pltpu.make_async_copy(patch(fin, me, 0), out.at[0, level], f_recv.at[level])

        def finish(i):
            r = jnp.where(2 * px < PX, PX - 1 - i, i)
            here = pl.ds(pl.multiple_of(r * cx, 8), cx)
            there = pl.ds(pl.multiple_of(r * cx + 8, 8), cx)
            fin[here, :] = gbuf[there, :] + dot3((u_t[0, here, :], u_t[1, here, :]), mixed)

            def give(j):
                g = r * PY + j

                @pl.when(g != me)
                def _():
                    send_back(g).start()

                @pl.when(g == me)
                def _():
                    own_out.start()
            loop(PY, give)
        loop(PX, finish)

        own_out.wait()
        own_modes.wait()

        def drain(g):
            @pl.when(g != me)
            def _():
                tell(g).wait_send()
                send_back(g).wait_send()
        loop(G, drain)

        for h in (1, 2):
            @pl.when(jnp.logical_and(odd, k < nests - h))
            def _():
                chain_out[h - 1].wait_send()

        @pl.when(jnp.logical_and(jnp.logical_not(odd), k < nests - 1))
        def _():
            gain_out.wait_send()
            own_out_copy.wait_send()

    for l, o in enumerate(owners):
        @pl.when(me != o)
        def _():
            pltpu.make_async_remote_copy(
                src_ref=cbuf.at[W - 1], dst_ref=mbuf.at[l], send_sem=m_send.at[0],
                recv_sem=m_recv.at[l], device_id=at(o), device_id_type=MESH,
            ).wait_recv()
            pltpu.make_async_remote_copy(
                src_ref=patch(fin, 0, 0), dst_ref=out.at[0, l], send_sem=f_send.at[0],
                recv_sem=f_recv.at[l], device_id=at(o), device_id_type=MESH,
            ).wait_recv()
            gather(l).wait_send()
    for l in range(L):
        modes[0, l] = unpack(mbuf[l])


def body(dims, owners, initial_state, drive_modes, relax_rates, nest_offsets):
    nests, PY, PX, L, cx, cy, m, W = dims
    G, nx, ny = PY * PX, cx * PX, cy * PY
    rp, cp = powers(basis(nx, m, 1), W), powers(basis(ny, m, 1), W)
    u, v = np.concatenate(rp, 1), np.concatenate(cp, 1)
    a = [rp[0].T @ t for t in rp]
    b = [cp[0].T @ t for t in cp]
    even_x, odd_x = (rp[0].T @ basis(nx, m, RATIO, f) for f in (np.cos, np.sin))
    even_y, odd_y = ((cp[0].T @ basis(ny, m, RATIO, f)).T for f in (np.cos, np.sin))
    small = np.stack(
        [even_x, odd_x, even_y, odd_y, a[1], a[2], a[1] @ a[1], b[1], b[2], b[1] @ b[1]]
    ).astype(np.float32)
    wide, deep = W * m, (W + 1) * m
    tables = (halves(u[:, :wide]), halves(u.T), halves(v), halves(v.T[:wide]))
    any_space = pl.BlockSpec(memory_space=pl.ANY)
    vmem = pl.BlockSpec(memory_space=pltpu.VMEM)
    smem = pl.BlockSpec(memory_space=pltpu.SMEM)
    dma = pltpu.SemaphoreType.DMA
    return pl.pallas_call(
        functools.partial(kernel, dims, owners),
        out_shape=(
            pltpu.VMEM((1, L, cx, cy), F32),
            pltpu.VMEM((1, L, m, m), F32),
        ),
        in_specs=[any_space, any_space, smem, smem] + [any_space] * 5,
        out_specs=(any_space, vmem),
        scratch_shapes=[
            pltpu.VMEM((L, cx, cy), F32),
            pltpu.VMEM((nx + 16, ny), F32),
            pltpu.VMEM((nx + 16, ny), F32),
            pltpu.VMEM((nx, ny), F32),
            pltpu.VMEM((W, m, m), F32),
            pltpu.VMEM((W, m // 2, 2 * m), F32),
            pltpu.VMEM((W, m // 2, 2 * m), F32),
            pltpu.VMEM((W, m // 2, 2 * m), F32),
            pltpu.VMEM((W, m // 2, 2 * m), F32),
            pltpu.VMEM((8, 128), F32),
            pltpu.VMEM((8, 128), F32),
            pltpu.VMEM((L, m // 2, 2 * m), F32),
            pltpu.VMEM((5, m, m), F32),
            pltpu.VMEM((2, nx, wide), BF16),
            pltpu.VMEM((2, deep, nx), BF16),
            pltpu.VMEM((2, ny, deep), BF16),
            pltpu.VMEM((2, wide, ny), BF16),
            pltpu.VMEM((10, m, m), F32),
            dma((L + 6,)),
            dma((L,)),
            dma((G,)),
            dma((2,)),
            dma,
            dma((2,)),
            dma((2,)),
            dma((G,)),
            dma((L,)),
            dma((G,)),
            dma((L,)),
        ],
        compiler_params=pltpu.CompilerParams(collective_id=0, has_side_effects=True),
    )(initial_state, drive_modes, relax_rates, nest_offsets.T,
      *(jnp.asarray(t) for t in tables), jnp.asarray(small))


def solution(mesh):
    nests, PY, PX = (mesh.shape[n] for n in ("nest", "py", "px"))
    spec = P("nest", None, "px", "py")

    def local(initial_state, drive_modes, relax_rates, nest_offsets):
        _, L, cx, cy = initial_state.shape
        W, _, m, _ = drive_modes.shape
        places = sorted(
            range(PY * PX),
            key=lambda g: (abs(2 * (g // PY) - PX + 1) + abs(2 * (g % PY) - PY + 1), g),
        )
        dims = (nests, PY, PX, L, cx, cy, m, W)
        return body(dims, tuple(places[:L]), initial_state, drive_modes, relax_rates, nest_offsets)

    return jax.shard_map(
        local,
        mesh=mesh,
        in_specs=(spec, P(), P("nest", None), P()),
        out_specs=(spec, P("nest", None, None, None)),
        check_vma=False,
    )
```

```python
import functools
import math

import jax
import jax.numpy as jnp
import numpy as np
from jax import lax
from jax.experimental import pallas as pl
from jax.experimental.pallas import tpu as pltpu
from jax.sharding import PartitionSpec as P

RATIO = 3
RATE = 0.2
MESH = pl.DeviceIdType.MESH
F32, BF16 = jnp.float32, jnp.bfloat16


def basis(cells, modes, refine, fn=np.cos):
    j = np.arange(modes, dtype=np.int64)
    q = 2 * np.arange(cells, dtype=np.int64) + 1
    product = (j[None, :] * q[:, None]) % (4 * refine * cells)
    weight = np.where(j == 0, 1.0, 2.0) / cells
    return np.sqrt(weight)[None, :] * fn(np.pi * product / (2.0 * refine * cells))


def half_step(table):
    pad = np.pad(table, ((1, 1), (0, 0)))
    return (0.5 - 2 * RATE) * table + RATE * (pad[2:] + pad[:-2])


def powers(table, count):
    out = [table]
    for _ in range(count):
        out.append(half_step(out[-1]))
    return out


def halves(table):
    high = np.asarray(table, np.float32).astype(BF16)
    low = (np.asarray(table, np.float64) - high.astype(np.float64)).astype(np.float32)
    return np.stack([high, low.astype(BF16)])


def split(x):
    high = x.astype(BF16)
    return high, (x - high.astype(F32)).astype(BF16)


def mm(a, b):
    return lax.dot_general(a, b, (((1,), (0,)), ((), ())), preferred_element_type=F32)


def dot3(a, b):
    a = a if isinstance(a, tuple) else split(a)
    b = b if isinstance(b, tuple) else split(b)
    return mm(a[0], b[0]) + (mm(a[0], b[1]) + mm(a[1], b[0]))


def pack(x):
    h = x.shape[0] // 2
    return jnp.concatenate([x[:h], x[h:]], 1)


def unpack(x):
    h = x.shape[1] // 2
    return jnp.concatenate([x[:, :h], x[:, h:]], 0)


def loop(n, fn):
    if n <= 16:
        for i in range(n):
            fn(i)
    else:
        lax.fori_loop(0, n, lambda i, c: (fn(i), c)[1], 0)


def kernel(
    dims, owners,
    field, drive, relax_hbm, offs_hbm, u_hbm, ut_hbm, v_hbm, vt_hbm, small_hbm,
    out, modes,
    fvm, fbuf, gbuf, fin, start, par, cbuf, sib, obuf, lead, glead, mbuf, tx,
    u_t, ut_t, v_t, vt_t, small, relax, offs,
    load_sem, a_send, a_recv, c_send, c_recv, o_sem, g_sem, f_send, f_recv, m_send, m_recv,
):
    nests, PY, PX, L, cx, cy, m, W = dims
    G, nx, ny = PY * PX, cx * PX, cy * PY
    k, py, px = lax.axis_index("nest"), lax.axis_index("py"), lax.axis_index("px")
    me = px * PY + py
    mine = [me == o for o in owners]
    level = sum(jnp.where(c, l, 0) for l, c in enumerate(mine))
    is_owner = functools.reduce(jnp.logical_or, mine)

    def at(g):
        return (k, g % PY, g // PY)

    def plain(g):
        return functools.reduce(jnp.logical_and, [g != o for o in owners])

    odd = k % 2 == 1
    hops = [
        (-1, k > 0),
        (1, k < nests - 1),
        (-2, jnp.logical_and(odd, k > 2)),
        (2, jnp.logical_and(odd, k < nests - 2)),
    ]
    barrier = pltpu.get_barrier_semaphore()
    for l, o in enumerate(owners):
        @pl.when(me != o)
        def _():
            pl.semaphore_signal(barrier, inc=1, device_id=at(o), device_id_type=MESH)

    @pl.when(is_owner)
    def _():
        def greet(g):
            @pl.when(plain(g))
            def _():
                pl.semaphore_signal(barrier, inc=1, device_id=at(g), device_id_type=MESH)
        loop(G, greet)

        for hop, cond in hops:
            @pl.when(cond)
            def _():
                pl.semaphore_signal(
                    barrier, inc=1, device_id=(k + hop, py, px), device_id_type=MESH
                )

    def hop_copy(src, dst, send_sem, recv_sem, hop):
        return pltpu.make_async_remote_copy(
            src_ref=src, dst_ref=dst, send_sem=send_sem, recv_sem=recv_sem,
            device_id=(k + hop, py, px), device_id_type=MESH,
        )

    gain_out = hop_copy(lead, glead, g_sem.at[0], g_sem.at[1], 1)
    gain_in = hop_copy(lead, glead, g_sem.at[0], g_sem.at[1], -1)
    own_out_copy = hop_copy(obuf, sib, o_sem.at[0], o_sem.at[1], 1)
    own_in = hop_copy(obuf, sib, o_sem.at[0], o_sem.at[1], -1)
    chain_out = [hop_copy(cbuf, par, c_send.at[h - 1], c_recv, h) for h in (1, 2)]
    chain_in = hop_copy(cbuf, par, c_send.at[0], c_recv, -1)

    loads = [pltpu.make_async_copy(field.at[0, l], fvm.at[l], load_sem.at[l]) for l in range(L)]
    for c in loads:
        c.start()
    tables = [
        pltpu.make_async_copy(src, dst, load_sem.at[L + i])
        for i, (src, dst) in enumerate(
            [
                (v_hbm, v_t), (ut_hbm, ut_t), (small_hbm, small), (u_hbm, u_t), (vt_hbm, vt_t),
                (relax_hbm, relax), (offs_hbm, offs),
            ]
        )
    ]
    get_drive = pltpu.make_async_copy(drive.at[:, level], start, load_sem.at[L + 7])

    @pl.when(is_owner)
    def _():
        for c in tables:
            c.start()

        @pl.when(k < 2)
        def _():
            get_drive.start()

        pl.semaphore_wait(barrier, G - 1 + sum(jnp.where(c, 1, 0) for _, c in hops))

    @pl.when(jnp.logical_not(is_owner))
    def _():
        pl.semaphore_wait(barrier, L)

    def patch(ref, g, shift):
        return ref.at[
            pl.ds(pl.multiple_of((g // PY) * cx + shift, 8), cx),
            pl.ds(pl.multiple_of((g % PY) * cy, 128), cy),
        ]

    def gather(l):
        return pltpu.make_async_remote_copy(
            src_ref=fvm.at[l], dst_ref=patch(fbuf, me, 8), send_sem=a_send.at[l],
            recv_sem=a_recv.at[me], device_id=at(owners[l]), device_id_type=MESH,
        )

    def keep(l):
        return pltpu.make_async_copy(fvm.at[l], patch(fbuf, me, 8), a_send.at[l])

    for l, o in enumerate(owners):
        loads[l].wait()

        @pl.when(me != o)
        def _():
            gather(l).start()

        @pl.when(me == o)
        def _():
            keep(l).start()

    @pl.when(is_owner)
    def _():
        edge = jnp.zeros((8, ny), F32)
        for ref in (fbuf, gbuf):
            ref[0:8, :] = edge
            ref[nx + 8 : nx + 16, :] = edge
        tables[5].wait()
        tables[6].wait()
        gain = relax[0, level]
        lead[...] = jnp.full(lead.shape, gain, F32)

        @pl.when(jnp.logical_and(jnp.logical_not(odd), k < nests - 1))
        def _():
            gain_out.start()

        tables[2].wait()

        def turn(kk, cells, dim, axis):
            number = lax.broadcasted_iota(jnp.int32, (m, m), dim).astype(F32)
            product = number * (2 * RATIO * offs[axis, kk]).astype(F32)
            period = float(4 * RATIO * cells)
            product = product - period * jnp.floor(product * (1.0 / period))
            angle = product * (math.pi / (2.0 * RATIO * cells))
            return jnp.cos(angle), jnp.sin(angle)

        def flat(kk):
            eye = jnp.where(
                lax.broadcasted_iota(jnp.int32, (m, m), 0)
                == lax.broadcasted_iota(jnp.int32, (m, m), 1),
                1.0, 0.0,
            ).astype(F32)
            cos_x, sin_x = turn(kk, nx, 1, 0)
            cos_y, sin_y = turn(kk, ny, 0, 1)
            row = jnp.where(kk == 0, eye, small[0] * cos_x - small[1] * sin_x)
            col = jnp.where(kk == 0, eye, small[2] * cos_y - small[3] * sin_y)
            return split(row), split(col)

        a1, b1 = split(small[4]), split(small[7])

        def curved(rate):
            return split(small[5] - rate * small[6]), split(small[8] - rate * small[9])

        def maps(kk, rate):
            a2, b2 = curved(rate)
            f0, g0 = flat(kk)
            f1, f2 = split(dot3(a1, f0)), split(dot3(a2, f0))
            g1, g2 = split(dot3(g0, b1)), split(dot3(g0, b2))
            return f0, f1, f2, g0, g1, g2, 2.0 * (1.0 - rate)

        def follow(cs, ms):
            f0, f1, f2, g0, g1, g2, rest = ms
            c1, c2, c3 = (split(c) for c in cs)
            y10, y20, y30 = dot3(c1, g0), dot3(c2, g0), dot3(c3, g0)
            y11, y21, y12 = dot3(c1, g1), dot3(c2, g1), dot3(c1, g2)
            y10s = split(y10)
            return (
                dot3(f0, y10s),
                dot3(f0, y20),
                dot3(f0, y30),
                dot3(f1, y10s) + dot3(f0, y11),
                dot3(f0, y21 + y12) + dot3(f1, y20 + rest * y11) + dot3(f2, y10s),
            )

        def nudge(own, moved, rate):
            own2, own3 = own[1] + rate * moved[3], own[2] + rate * moved[4]
            d1, d2, d3 = rate * (moved[0] - own[0]), rate * (moved[1] - own2), rate * (moved[2] - own3)
            return (d1, d2, d3), (own[0] + d1, own2 + d2, own3 + d3)

        own_maps = maps(k, gain)

        @pl.when(odd)
        def _():
            gain_in.wait_recv()
            lead[...] = glead[...]

        lead_gain = lead[0:1, 0:m]
        lead_maps = maps(k - k % 2, lead_gain)

        def first(cs):
            for i, x in enumerate(follow(cs, lead_maps)):
                tx[i] = x

        @pl.when(k < 2)
        def _():
            get_drive.wait()
            first([start[w] for w in range(W)])

        tables[0].wait()
        tables[1].wait()

        def arrive(g):
            @pl.when(g == me)
            def _():
                keep(level).wait()

            @pl.when(g != me)
            def _():
                pltpu.make_async_remote_copy(
                    src_ref=fvm.at[0], dst_ref=patch(fbuf, g, 8), send_sem=a_send.at[0],
                    recv_sem=a_recv.at[g], device_id=at(me), device_id_type=MESH,
                ).wait_recv()
        loop(G, arrive)

        step = min(nx, 256)
        both = jnp.zeros(((W + 1) * m, (W + 1) * m), F32)
        for r in range(0, nx, step):
            part = dot3(fbuf[8 + r : 8 + r + step, :], (v_t[0], v_t[1]))
            both = both + dot3((ut_t[0, :, r : r + step], ut_t[1, :, r : r + step]), part)

        def block(i, j):
            return both[i * m : (i + 1) * m, j * m : (j + 1) * m]

        s1, s2, s3 = (
            sum(float(math.comb(w, i)) * block(i, w - i) for i in range(w + 1)) for w in (1, 2, 3)
        )
        a2, b2 = curved(gain)
        s1s, s2s = split(s1), split(s2)
        z11 = dot3(s1s, b1)
        x2 = dot3(a1, s1s) + z11
        x3 = dot3(s2s, b1) + dot3(s1s, b2) + dot3(a1, s2 + 2.0 * (1.0 - gain) * z11) + dot3(a2, s1s)
        own = (s1, s2 - gain * x2, s3 - gain * x3)

        @pl.when(jnp.logical_and(jnp.logical_not(odd), k < nests - 1))
        def _():
            for w in range(W):
                obuf[w] = pack(own[w])
            own_out_copy.start()

        rows = min(64, nx)

        def free():
            col_id = lax.broadcasted_iota(jnp.int32, (rows, ny), 1)

            def sweep(src, dst):
                def some(r, carry):
                    at_row = pl.multiple_of(r * rows, 8)
                    wide = src[pl.ds(at_row, rows + 16), :]
                    mid = wide[8 : rows + 8]
                    near = wide[7 : rows + 7] + wide[9 : rows + 9]
                    near = near + jnp.where(col_id == 0, 0.0, pltpu.roll(mid, 1, 1))
                    near = near + jnp.where(col_id == ny - 1, 0.0, pltpu.roll(mid, ny - 1, 1))
                    dst[pl.ds(pl.multiple_of(at_row + 8, 8), rows), :] = mid + RATE * (near - 4.0 * mid)
                    return carry
                lax.fori_loop(0, nx // rows, some, 0, unroll=nx // rows <= 4)
            sweep(fbuf, gbuf)
            sweep(gbuf, fbuf)
            sweep(fbuf, gbuf)

        @pl.when(k > 0)
        def _():
            free()

        @pl.when(k > 1)
        def _():
            chain_in.wait_recv()
            first([unpack(par[w]) for w in range(W)])

        @pl.when(odd)
        def _():
            own_in.wait_recv()
            _, above = nudge(
                [unpack(sib[w]) for w in range(W)], [tx[i] for i in range(5)], lead_gain
            )
            for i, x in enumerate(follow(above, own_maps)):
                tx[i] = x

        (d1, d2, d3), now = nudge(own, [tx[i] for i in range(5)], gain)
        for w in range(W):
            cbuf[w] = pack(now[w])
        for h in (2, 1):
            @pl.when(jnp.logical_and(odd, k < nests - h))
            def _():
                chain_out[h - 1].start()

        def tell(g):
            return pltpu.make_async_remote_copy(
                src_ref=cbuf.at[W - 1], dst_ref=mbuf.at[level], send_sem=m_send.at[g],
                recv_sem=m_recv.at[level], device_id=at(g), device_id_type=MESH,
            )

        def tell_start(g):
            @pl.when(g != me)
            def _():
                tell(g).start()
        loop(G, tell_start)
        own_modes = pltpu.make_async_copy(cbuf.at[W - 1], mbuf.at[level], m_recv.at[level])
        own_modes.start()

        @pl.when(k == 0)
        def _():
            free()

        tables[3].wait()
        tables[4].wait()
        e1, e2, e3 = split(d1), split(d2), split(d3)
        vt = [(vt_t[0, i * m : (i + 1) * m, :], vt_t[1, i * m : (i + 1) * m, :]) for i in range(W)]
        w0 = dot3(e3, vt[0]) + dot3(e2, vt[1]) + dot3(e1, vt[2])
        w1 = dot3(e2, vt[0]) + 2.0 * dot3(e1, vt[1])
        w2 = dot3(e1, vt[0])
        mixed = split(jnp.concatenate([w0, w1, w2], 0))

        def send_back(g):
            return pltpu.make_async_remote_copy(
                src_ref=patch(fin, g, 0), dst_ref=out.at[0, level], send_sem=f_send.at[g],
                recv_sem=f_recv.at[level], device_id=at(g), device_id_type=MESH,
            )

        own_out = pltpu.make_async_copy(patch(fin, me, 0), out.at[0, level], f_recv.at[level])

        def finish(i):
            r = jnp.where(2 * px < PX, PX - 1 - i, i)
            here = pl.ds(pl.multiple_of(r * cx, 8), cx)
            there = pl.ds(pl.multiple_of(r * cx + 8, 8), cx)
            fin[here, :] = gbuf[there, :] + dot3((u_t[0, here, :], u_t[1, here, :]), mixed)

            def give(j):
                g = r * PY + j

                @pl.when(g != me)
                def _():
                    send_back(g).start()

                @pl.when(g == me)
                def _():
                    own_out.start()
            loop(PY, give)
        loop(PX, finish)

        own_out.wait()
        own_modes.wait()

        def drain(g):
            @pl.when(g != me)
            def _():
                tell(g).wait_send()
                send_back(g).wait_send()
        loop(G, drain)

        for h in (1, 2):
            @pl.when(jnp.logical_and(odd, k < nests - h))
            def _():
                chain_out[h - 1].wait_send()

        @pl.when(jnp.logical_and(jnp.logical_not(odd), k < nests - 1))
        def _():
            gain_out.wait_send()
            own_out_copy.wait_send()

    for l, o in enumerate(owners):
        @pl.when(me != o)
        def _():
            pltpu.make_async_remote_copy(
                src_ref=cbuf.at[W - 1], dst_ref=mbuf.at[l], send_sem=m_send.at[0],
                recv_sem=m_recv.at[l], device_id=at(o), device_id_type=MESH,
            ).wait_recv()
            pltpu.make_async_remote_copy(
                src_ref=patch(fin, 0, 0), dst_ref=out.at[0, l], send_sem=f_send.at[0],
                recv_sem=f_recv.at[l], device_id=at(o), device_id_type=MESH,
            ).wait_recv()
            gather(l).wait_send()
    for l in range(L):
        modes[0, l] = unpack(mbuf[l])


def store(state, modes, state_out, modes_out, sem):
    copies = [
        pltpu.make_async_copy(state, state_out, sem.at[0]),
        pltpu.make_async_copy(modes, modes_out, sem.at[1]),
    ]
    for c in copies:
        c.start()
    for c in copies:
        c.wait()


def body(dims, owners, initial_state, drive_modes, relax_rates, nest_offsets):
    nests, PY, PX, L, cx, cy, m, W = dims
    G, nx, ny = PY * PX, cx * PX, cy * PY
    rp, cp = powers(basis(nx, m, 1), W), powers(basis(ny, m, 1), W)
    u, v = np.concatenate(rp, 1), np.concatenate(cp, 1)
    a = [rp[0].T @ t for t in rp]
    b = [cp[0].T @ t for t in cp]
    even_x, odd_x = (rp[0].T @ basis(nx, m, RATIO, f) for f in (np.cos, np.sin))
    even_y, odd_y = ((cp[0].T @ basis(ny, m, RATIO, f)).T for f in (np.cos, np.sin))
    small = np.stack(
        [even_x, odd_x, even_y, odd_y, a[1], a[2], a[1] @ a[1], b[1], b[2], b[1] @ b[1]]
    ).astype(np.float32)
    wide, deep = W * m, (W + 1) * m
    tables = (halves(u[:, :wide]), halves(u.T), halves(v), halves(v.T[:wide]))
    any_space = pl.BlockSpec(memory_space=pl.ANY)
    vmem = pl.BlockSpec(memory_space=pltpu.VMEM)
    dma = pltpu.SemaphoreType.DMA
    held = pl.pallas_call(
        functools.partial(kernel, dims, owners),
        out_shape=(
            pltpu.VMEM((1, L, cx, cy), F32),
            pltpu.VMEM((1, L, m, m), F32),
        ),
        in_specs=[any_space] * 9,
        out_specs=(any_space, vmem),
        scratch_shapes=[
            pltpu.VMEM((L, cx, cy), F32),
            pltpu.VMEM((nx + 16, ny), F32),
            pltpu.VMEM((nx + 16, ny), F32),
            pltpu.VMEM((nx, ny), F32),
            pltpu.VMEM((W, m, m), F32),
            pltpu.VMEM((W, m // 2, 2 * m), F32),
            pltpu.VMEM((W, m // 2, 2 * m), F32),
            pltpu.VMEM((W, m // 2, 2 * m), F32),
            pltpu.VMEM((W, m // 2, 2 * m), F32),
            pltpu.VMEM((8, 128), F32),
            pltpu.VMEM((8, 128), F32),
            pltpu.VMEM((L, m // 2, 2 * m), F32),
            pltpu.VMEM((5, m, m), F32),
            pltpu.VMEM((2, nx, wide), BF16),
            pltpu.VMEM((2, deep, nx), BF16),
            pltpu.VMEM((2, ny, deep), BF16),
            pltpu.VMEM((2, wide, ny), BF16),
            pltpu.VMEM((10, m, m), F32),
            pltpu.SMEM(relax_rates.shape, F32),
            pltpu.SMEM(nest_offsets.shape[::-1], jnp.int32),
            dma((L + 8,)),
            dma((L,)),
            dma((G,)),
            dma((2,)),
            dma,
            dma((2,)),
            dma((2,)),
            dma((G,)),
            dma((L,)),
            dma((G,)),
            dma((L,)),
        ],
        compiler_params=pltpu.CompilerParams(collective_id=0, has_side_effects=True),
    )(initial_state, drive_modes, relax_rates, nest_offsets.T,
      *(jnp.asarray(t) for t in tables), jnp.asarray(small))
    return pl.pallas_call(
        store,
        out_shape=[jax.ShapeDtypeStruct(x.shape, F32) for x in held],
        in_specs=[any_space] * 2,
        out_specs=[any_space] * 2,
        scratch_shapes=[dma((2,))],
    )(*(pltpu.with_memory_space_constraint(x, pltpu.VMEM) for x in held))


def solution(mesh):
    nests, PY, PX = (mesh.shape[n] for n in ("nest", "py", "px"))
    spec = P("nest", None, "px", "py")

    def local(initial_state, drive_modes, relax_rates, nest_offsets):
        _, L, cx, cy = initial_state.shape
        W, _, m, _ = drive_modes.shape
        places = sorted(
            range(PY * PX),
            key=lambda g: (abs(2 * (g // PY) - PX + 1) + abs(2 * (g % PY) - PY + 1), g),
        )
        dims = (nests, PY, PX, L, cx, cy, m, W)
        return body(dims, tuple(places[:L]), initial_state, drive_modes, relax_rates, nest_offsets)

    return jax.shard_map(
        local,
        mesh=mesh,
        in_specs=(spec, P(), P("nest", None), P()),
        out_specs=(spec, P("nest", None, None, None)),
        check_vma=False,
    )
```

```python
import functools
import math

import jax
import jax.numpy as jnp
import numpy as np
from jax import lax
from jax.experimental import pallas as pl
from jax.experimental.pallas import tpu as pltpu
from jax.sharding import PartitionSpec as P

RATIO = 3
RATE = 0.2
MESH = pl.DeviceIdType.MESH
F32, BF16 = jnp.float32, jnp.bfloat16


def basis(cells, modes, refine, fn=np.cos):
    j = np.arange(modes, dtype=np.int64)
    q = 2 * np.arange(cells, dtype=np.int64) + 1
    product = (j[None, :] * q[:, None]) % (4 * refine * cells)
    weight = np.where(j == 0, 1.0, 2.0) / cells
    return np.sqrt(weight)[None, :] * fn(np.pi * product / (2.0 * refine * cells))


def half_step(table):
    pad = np.pad(table, ((1, 1), (0, 0)))
    return (0.5 - 2 * RATE) * table + RATE * (pad[2:] + pad[:-2])


def powers(table, count):
    out = [table]
    for _ in range(count):
        out.append(half_step(out[-1]))
    return out


def halves(table):
    high = np.asarray(table, np.float32).astype(BF16)
    low = (np.asarray(table, np.float64) - high.astype(np.float64)).astype(np.float32)
    return np.stack([high, low.astype(BF16)])


def split(x):
    high = x.astype(BF16)
    return high, (x - high.astype(F32)).astype(BF16)


def mm(a, b):
    return lax.dot_general(a, b, (((1,), (0,)), ((), ())), preferred_element_type=F32)


def dot3(a, b):
    a = a if isinstance(a, tuple) else split(a)
    b = b if isinstance(b, tuple) else split(b)
    return mm(a[0], b[0]) + (mm(a[0], b[1]) + mm(a[1], b[0]))


def dot3t(a, b):
    b = b if isinstance(b, tuple) else split(b)

    def nt(x, y):
        return lax.dot_general(x, y, (((1,), (1,)), ((), ())), preferred_element_type=F32)

    return nt(a[0], b[0]) + (nt(a[0], b[1]) + nt(a[1], b[0]))


def pack(x):
    h = x.shape[0] // 2
    return jnp.concatenate([x[:h], x[h:]], 1)


def unpack(x):
    h = x.shape[1] // 2
    return jnp.concatenate([x[:, :h], x[:, h:]], 0)


def pack_wide(x, m):
    low = x[:m].T[m : m + 8]
    return jnp.concatenate(
        [pack(x[:m, :m]), x[m : m + 8], jnp.concatenate([low, jnp.zeros_like(low)], 1)], 0
    )


def unpack_fix(x, m):
    tile = x[m // 2 :]
    low = jnp.concatenate([tile[:, :m], jnp.zeros((m - 8, m), F32)], 0).T
    top = jnp.concatenate([unpack(x[: m // 2]), low], 1)
    return jnp.concatenate([top, tile, jnp.zeros((8, 2 * m), F32)], 0)[:, : m + 16]


def unpack_wide(x, m):
    low = jnp.concatenate([x[m // 2 + 8 :, :m], jnp.zeros((m - 8, m), F32)], 0).T
    top = jnp.concatenate([unpack(x[: m // 2]), low], 1)
    return jnp.concatenate([top, x[m // 2 : m // 2 + 8], jnp.zeros((8, 2 * m), F32)], 0)


def loop(n, fn):
    if n <= 16:
        for i in range(n):
            fn(i)
    else:
        lax.fori_loop(0, n, lambda i, c: (fn(i), c)[1], 0)


def kernel(
    dims, owners,
    field, drive, relax_hbm, offs_hbm,
    u_hbm, ut_hbm, v_hbm, vt_hbm, left_hbm, right_hbm, up_hbm, down_hbm, small_hbm,
    out, modes,
    fvm, pbuf, abuf, strip, near, wide, calm, state, fix, u_t, vt_t, zbuf, mail, start, par, cbuf, lead, glead, tx,
    ut_t, v_t, left, right, up, down, small, relax, offs,
    load_sem, a_send, a_recv, h_send, h_recv, c_sem, g_sem, out_sem, f_send, f_recv, m_send, m_recv,
):
    nests, PY, PX, L, cx, cy, m, W = dims
    G, nx, ny = PY * PX, cx * PX, cy * PY
    k, py, px = lax.axis_index("nest"), lax.axis_index("py"), lax.axis_index("px")
    me = px * PY + py
    odd = k % 2 == 1
    leader = k + 1 - k % 2
    placed = [me == o for o in owners]
    level = sum(jnp.where(c, l, 0) for l, c in enumerate(placed))
    in_place = functools.reduce(jnp.logical_or, placed)
    is_owner = jnp.logical_and(odd, in_place)
    is_spare = jnp.logical_and(jnp.logical_not(odd), in_place)
    owns = [jnp.logical_and(odd, c) for c in placed]

    def at(g, nest):
        return (nest, g % PY, g // PY)

    def plain(g):
        return functools.reduce(jnp.logical_and, [g != o for o in owners])

    hops = [(-2, k > 2), (2, k < nests - 2)]
    sides = [
        (px > 0, (k, py, px - 1)), (px < PX - 1, (k, py, px + 1)),
        (py > 0, (k, py - 1, px)), (py < PY - 1, (k, py + 1, px)),
    ]
    beside = sum(jnp.where(c, 1, 0) for c, _ in sides)
    barrier = pltpu.get_barrier_semaphore()
    for l, o in enumerate(owners):
        @pl.when(jnp.logical_not(owns[l]))
        def _():
            pl.semaphore_signal(barrier, inc=1, device_id=at(o, leader), device_id_type=MESH)

    for cond, device in sides:
        @pl.when(cond)
        def _():
            pl.semaphore_signal(barrier, inc=1, device_id=device, device_id_type=MESH)

    @pl.when(is_owner)
    def _():
        def greet(g):
            pl.semaphore_signal(barrier, inc=1, device_id=at(g, k - 1), device_id_type=MESH)

            @pl.when(plain(g))
            def _():
                pl.semaphore_signal(barrier, inc=1, device_id=at(g, k), device_id_type=MESH)
        loop(G, greet)

        for hop, cond in hops:
            @pl.when(cond)
            def _():
                pl.semaphore_signal(
                    barrier, inc=1, device_id=(k + hop, py, px), device_id_type=MESH
                )

    def hop_copy(src, dst, send_sem, recv_sem, hop):
        return pltpu.make_async_remote_copy(
            src_ref=src, dst_ref=dst, send_sem=send_sem, recv_sem=recv_sem,
            device_id=(k + hop, py, px), device_id_type=MESH,
        )

    gain_out = hop_copy(lead, glead, g_sem.at[0], g_sem.at[1], 1)
    gain_in = hop_copy(lead, glead, g_sem.at[0], g_sem.at[1], -1)
    chain_out = hop_copy(cbuf, par, c_sem.at[0], c_sem.at[1], 2)
    chain_in = hop_copy(cbuf, par, c_sem.at[0], c_sem.at[1], -2)

    loads = [pltpu.make_async_copy(field.at[0, l], fvm.at[l], load_sem.at[l]) for l in range(L)]
    for c in loads:
        c.start()
    rows_here = pl.ds(pl.multiple_of(px * cx, 8), cx)
    cols_here = pl.ds(pl.multiple_of(py * cy, 128), cy)
    pairs = [
        (v_hbm.at[:, cols_here], v_t), (ut_hbm.at[:, px], ut_t),
        (u_hbm.at[:, rows_here], u_t), (vt_hbm.at[:, :, cols_here], vt_t),
        (relax_hbm, relax), (offs_hbm, offs), (small_hbm, small),
        (left_hbm, left), (right_hbm, right), (up_hbm, up), (down_hbm, down),
    ]
    tables = [
        pltpu.make_async_copy(src, dst, load_sem.at[L + 1 + i]) for i, (src, dst) in enumerate(pairs)
    ]
    for c in tables[:4]:
        c.start()
    get_drive = pltpu.make_async_copy(drive.at[:, level], start, load_sem.at[L])

    @pl.when(in_place)
    def _():
        tables[4].start()

    @pl.when(is_owner)
    def _():
        for c in tables[5:]:
            c.start()

        @pl.when(k < 2)
        def _():
            get_drive.start()

    tables[0].wait()
    tables[1].wait()
    for c in loads:
        c.wait()
    half = dot3(fvm[...].reshape(L * cx, cy), (v_t[0], v_t[1]))
    for l in range(L):
        pbuf[l] = pack_wide(dot3((ut_t[0], ut_t[1]), half[l * cx : (l + 1) * cx]), m)

    lane = lax.broadcasted_iota(jnp.int32, (cx, 128), 1)
    edge = jnp.zeros((cx, 128), F32)
    for l in range(L):
        ends = jnp.where(lane < 64, fvm[l, :, 0:128], fvm[l, :, cy - 128 : cy])
        turned = pltpu.roll(ends, 8 * l, 1) if l else ends
        shift = (lane - 8 * l + 4) % 128
        edge = jnp.where(shift < 8, turned, edge)
        wide[l, 8 : cx + 8, 0:cy] = fvm[l]
    folds = 128 // (8 * L)
    thin = cx // folds
    short = lax.broadcasted_iota(jnp.int32, (thin, 128), 1)
    folded = edge[:thin]
    for i in range(1, folds):
        moved = pltpu.roll(edge[i * thin : (i + 1) * thin], 8 * L * i, 1)
        folded = jnp.where((short + 4) % 128 < 8 * L * i, folded, moved)
    strip[...] = folded
    bare = jnp.zeros((8, cy + 128), F32)

    @pl.when(px == 0)
    def _():
        for l in range(L):
            wide[l, 0:8, :] = bare

    @pl.when(px == PX - 1)
    def _():
        for l in range(L):
            wide[l, cx + 8 : cx + 16, :] = bare

    @pl.when(py == 0)
    def _():
        near[0] = jnp.zeros(near.shape[1:], F32)

    @pl.when(py == PY - 1)
    def _():
        near[1] = jnp.zeros(near.shape[1:], F32)

    @pl.when(is_owner)
    def _():
        abuf[1, me] = pbuf[level]
        pl.semaphore_wait(barrier, beside + 2 * G - 1 + sum(jnp.where(c, 1, 0) for _, c in hops))

    @pl.when(jnp.logical_not(is_owner))
    def _():
        pl.semaphore_wait(barrier, beside + L)

    def remote(src, dst, send_sem, recv_sem, g, nest):
        return pltpu.make_async_remote_copy(
            src_ref=src, dst_ref=dst, send_sem=send_sem, recv_sem=recv_sem,
            device_id=at(g, nest), device_id_type=MESH,
        )

    def share(l):
        return remote(
            pbuf.at[l], abuf.at[k % 2, me], a_send.at[l], a_recv.at[k % 2, me], owners[l], leader
        )

    keep_modes = pltpu.make_async_copy(mail.at[1], modes.at[level], m_recv.at[level])

    def beam(src, dst, i, device):
        return pltpu.make_async_remote_copy(
            src_ref=src, dst_ref=dst, send_sem=h_send.at[i], recv_sem=h_recv.at[i],
            device_id=device, device_id_type=MESH,
        )

    top, bottom = pl.ds(0, 8), pl.ds(cx + 8, 8)
    first_rows, last_rows = pl.ds(8, 8), pl.ds(cx, 8)
    halo = [
        beam(wide.at[:, first_rows], wide.at[:, bottom], 0, sides[0][1]),
        beam(wide.at[:, last_rows], wide.at[:, top], 1, sides[1][1]),
        beam(strip, near.at[1], 2, sides[2][1]),
        beam(strip, near.at[0], 3, sides[3][1]),
    ]

    def start_halo(i):
        @pl.when(sides[i][0])
        def _():
            halo[i].start()

    def land_halo(i):
        @pl.when(sides[i ^ 1][0])
        def _():
            halo[i].wait_recv()

    for l, o in enumerate(owners):
        @pl.when(jnp.logical_not(owns[l]))
        def _():
            share(l).start()

    @pl.when(is_spare)
    def _():
        tables[4].wait()
        lead[...] = jnp.full(lead.shape, relax[0, level], F32)
        gain_out.start()

    start_halo(2)
    start_halo(3)

    def widen_patch():
        land_halo(2)
        land_halo(3)
        after, before = near[1], near[0]
        for l in range(L):
            for i in range(folds):
                back = (128 - 8 * l - 8 * L * i) % 128
                right, left_side = after, before
                if back:
                    right, left_side = pltpu.roll(after, back, 1), pltpu.roll(before, back, 1)
                wide[l, 8 + i * thin : 8 + (i + 1) * thin, cy:] = jnp.where(
                    short < 64, right, left_side
                )
        start_halo(0)
        start_halo(1)

    def run_free():
        land_halo(0)
        land_halo(1)
        shape = (cx + 16, cy + 128)
        row = lax.broadcasted_iota(jnp.int32, shape, 0) + (px * cx - 8)
        col = lax.broadcasted_iota(jnp.int32, shape, 1)
        col = jnp.where(col < cy + 64, col, col - (cy + 128)) + py * cy
        inside = (row >= 0) & (row < nx) & (col >= 0) & (col < ny)
        for l in range(L):
            now = wide[l]
            for _ in range(W):
                side = pltpu.roll(now, 1, 0) + pltpu.roll(now, cx + 15, 0)
                side = side + pltpu.roll(now, 1, 1) + pltpu.roll(now, cy + 127, 1)
                now = jnp.where(inside, now + RATE * (side - 4.0 * now), 0.0)
            calm[l] = now[8 : cx + 8, 0:cy]

    @pl.when(is_owner)
    def _():
        tables[4].wait()
        tables[5].wait()
        tables[6].wait()
        gain = relax[0, level]

        def turn(kk, cells, dim, axis):
            number = lax.broadcasted_iota(jnp.int32, (m, m), dim).astype(F32)
            product = number * (2 * RATIO * offs[axis, kk]).astype(F32)
            period = float(4 * RATIO * cells)
            product = product - period * jnp.floor(product * (1.0 / period))
            angle = product * (math.pi / (2.0 * RATIO * cells))
            return jnp.cos(angle), jnp.sin(angle)

        def flat(kk):
            eye = jnp.where(
                lax.broadcasted_iota(jnp.int32, (m, m), 0)
                == lax.broadcasted_iota(jnp.int32, (m, m), 1),
                1.0, 0.0,
            ).astype(F32)
            cos_x, sin_x = turn(kk, nx, 1, 0)
            cos_y, sin_y = turn(kk, ny, 0, 1)
            row = jnp.where(kk == 0, eye, small[0] * cos_x - small[1] * sin_x)
            col = jnp.where(kk == 0, eye, small[2] * cos_y - small[3] * sin_y)
            return split(row), split(col)

        a1, b1 = split(small[4]), split(small[7])

        def curved(rate):
            return split(small[5] - rate * small[6]), split(small[8] - rate * small[9])

        def maps(kk, rate):
            a2, b2 = curved(rate)
            f0, g0 = flat(kk)
            f1, f2 = split(dot3(a1, f0)), split(dot3(a2, f0))
            g1, g2 = split(dot3(g0, b1)), split(dot3(g0, b2))
            return f0, f1, f2, g0, g1, g2, 2.0 * (1.0 - rate)

        def follow(cs, ms):
            f0, f1, f2, g0, g1, g2, rest = ms
            c1, c2, c3 = (split(c) for c in cs)
            y10, y20, y30 = dot3(c1, g0), dot3(c2, g0), dot3(c3, g0)
            y11, y21, y12 = dot3(c1, g1), dot3(c2, g1), dot3(c1, g2)
            y10s = split(y10)
            return (
                dot3(f0, y10s),
                dot3(f0, y20),
                dot3(f0, y30),
                dot3(f1, y10s) + dot3(f0, y11),
                dot3(f0, y21 + y12) + dot3(f1, y20 + rest * y11) + dot3(f2, y10s),
            )

        def nudge(own, moved, rate):
            own2, own3 = own[1] + rate * moved[3], own[2] + rate * moved[4]
            d1, d2, d3 = rate * (moved[0] - own[0]), rate * (moved[1] - own2), rate * (moved[2] - own3)
            return (d1, d2, d3), (own[0] + d1, own2 + d2, own3 + d3)

        own_maps = maps(k, gain)
        gain_in.wait_recv()
        lead_gain = glead[0:1, 0:m]
        lead_maps = maps(k - 1, lead_gain)

        def first(cs):
            for i, x in enumerate(follow(cs, lead_maps)):
                tx[i] = x

        @pl.when(k < 2)
        def _():
            get_drive.wait()
            first([start[w] for w in range(W)])

        tables[7].wait()
        tables[8].wait()

        def arrive(g):
            remote(pbuf.at[0], abuf.at[0, g], a_send.at[0], a_recv.at[0, g], g, k - 1).wait_recv()

            @pl.when(g != me)
            def _():
                remote(pbuf.at[0], abuf.at[1, g], a_send.at[0], a_recv.at[1, g], g, k).wait_recv()
        loop(G, arrive)

        def project(i):
            total = abuf[i, 0]
            if G <= 16:
                for g in range(1, G):
                    total = total + abuf[i, g]
            else:
                total = lax.fori_loop(1, G, lambda g, c: c + abuf[i, g], total)
            both = dot3((left[0], left[1]), dot3(unpack_wide(total, m), (right[0], right[1])))

            def block(i, j):
                return both[i * m : (i + 1) * m, j * m : (j + 1) * m]

            return [
                sum(float(math.comb(w, i)) * block(i, w - i) for i in range(w + 1))
                for w in (1, 2, 3)
            ]

        def settle(s, rate):
            s1, s2, s3 = s
            a2, b2 = curved(rate)
            s1s, s2s = split(s1), split(s2)
            z11 = dot3(s1s, b1)
            x2 = dot3(a1, s1s) + z11
            x3 = dot3(s2s, b1) + dot3(s1s, b2) + dot3(a2, s1s)
            x3 = x3 + dot3(a1, s2 + 2.0 * (1.0 - rate) * z11)
            return s1, s2 - rate * x2, s3 - rate * x3

        before, after = project(0), project(1)
        before, after = settle(before, lead_gain), settle(after, gain)

        @pl.when(k > 1)
        def _():
            widen_patch()
            chain_in.wait_recv()
            first([unpack(par[w]) for w in range(W)])

        d_lead, c_lead = nudge(before, [tx[i] for i in range(5)], lead_gain)
        d_own, c_own = nudge(after, follow(c_lead, own_maps), gain)
        for w in range(W):
            cbuf[w] = pack(c_own[w])

        @pl.when(k < nests - 2)
        def _():
            chain_out.start()

        @pl.when(k < 2)
        def _():
            widen_patch()

        tables[9].wait()
        tables[10].wait()
        def widen(x):
            return jnp.concatenate([x, jnp.zeros_like(x)], 1)

        def table(i):
            return up[0, 16 * i : 16 * (i + 1)], up[1, 16 * i : 16 * (i + 1)]

        def correct(d):
            d1, d2, d3 = d
            e1 = split(d1)
            main = d3 + small[10] * d2 + small[11] * d1
            rows = dot3(table(0), d2 + small[12] * d1) + dot3(table(1), e1)
            cols = dot3t(table(2), d2 + small[13] * d1) + dot3t(table(3), e1)
            corner = dot3(dot3(table(0), e1), (down[0], down[1]))
            return jnp.concatenate([pack(main), (widen(rows + cols) + corner)[:8]], 0)

        zbuf[0] = correct(d_lead)
        mail[0] = pack(c_lead[W - 1])
        zbuf[1] = correct(d_own)
        mail[1] = pack(c_own[W - 1])

        def mend(i, g):
            return remote(
                zbuf.at[i], fix.at[level], f_send.at[i, g], f_recv.at[level], g, k - 1 + i
            )

        def tell(i, g):
            return remote(
                mail.at[i], modes.at[level], m_send.at[i, g], m_recv.at[level], g, k - 1 + i
            )

        for copy in (mend, tell):
            for i in range(2):
                def one(j):
                    g = jnp.where(2 * px < PX, G - 1 - j, j)

                    @pl.when(jnp.logical_or(i == 0, g != me))
                    def _():
                        copy(i, g).start()
                loop(G, one)
        fix[level] = zbuf[1]
        keep_modes.start()
        run_free()

    @pl.when(jnp.logical_not(is_owner))
    def _():
        widen_patch()
        run_free()

    tables[2].wait()
    tables[3].wait()

    puts = [pltpu.make_async_copy(state.at[l], out.at[l], out_sem.at[l]) for l in range(L)]

    def finish(some):
        for l in some:
            @pl.when(jnp.logical_not(owns[l]))
            def _():
                remote(
                    zbuf.at[0], fix.at[l], f_send.at[0, 0], f_recv.at[l], owners[l], leader
                ).wait_recv()
        half = [dot3(unpack_fix(fix[l], m), (vt_t[0], vt_t[1])) for l in some]
        for l, x in zip(some, half):
            state[l] = calm[l] + dot3((u_t[0], u_t[1]), x)
            puts[l].start()

    finish(range(L // 2))
    finish(range(L // 2, L))
    for l, o in enumerate(owners):
        @pl.when(jnp.logical_not(owns[l]))
        def _():
            remote(
                mail.at[0], modes.at[l], m_send.at[0, 0], m_recv.at[l], o, leader
            ).wait_recv()
            share(l).wait_send()

    @pl.when(is_owner)
    def _():
        keep_modes.wait()

        def drain(g):
            for i in range(2):
                @pl.when(jnp.logical_or(i == 0, g != me))
                def _():
                    remote(
                        mail.at[i], modes.at[0], m_send.at[i, g], m_recv.at[0], g, k - 1 + i
                    ).wait_send()
                    remote(
                        zbuf.at[i], fix.at[0], f_send.at[i, g], f_recv.at[0], g, k - 1 + i
                    ).wait_send()
        loop(G, drain)

        @pl.when(k < nests - 2)
        def _():
            chain_out.wait_send()

    @pl.when(is_spare)
    def _():
        gain_out.wait_send()

    for i in range(4):
        @pl.when(sides[i][0])
        def _():
            halo[i].wait_send()
    for c in puts:
        c.wait()


def store(state, packed, state_out, modes_out, modes, sem):
    first = pltpu.make_async_copy(state, state_out.at[0], sem.at[0])
    second = pltpu.make_async_copy(modes, modes_out.at[0], sem.at[1])
    first.start()
    for l in range(packed.shape[0]):
        modes[l] = unpack(packed[l])
    second.start()
    first.wait()
    second.wait()


def wide_tables(cells, modes, windows):
    stages = powers(basis(cells, modes, 1), windows)
    edges = np.zeros((cells, modes))
    for e in range(windows):
        edges[e, 2 * e] = 1.0
        edges[cells - 1 - e, 2 * e + 1] = 1.0
    full = np.concatenate([stages[0], edges], 1)
    rate = 0.5 - 2 * RATE + 2 * RATE * np.cos(np.pi * np.arange(modes) / cells)
    turns = []
    for i, t in enumerate(stages):
        top = np.diag(rate**i)
        turns.append(np.concatenate([top, edges.T @ (t - stages[0] @ top)], 0))
    return stages, full, turns, rate


def body(dims, owners, initial_state, drive_modes, relax_rates, nest_offsets):
    nests, PY, PX, L, cx, cy, m, W = dims
    G, nx, ny = PY * PX, cx * PX, cy * PY
    assert nests % 2 == 0 and W == 3
    tall, lanes = m + 16, 2 * m
    rp, u, tu, rate_x = wide_tables(nx, m, W)
    cp, v, tv, rate_y = wide_tables(ny, m, W)
    few = 2 * (W - 1)
    u_few, v_few = u[:, :tall].copy(), np.zeros((ny, tall))
    u_few[:, m + few :] = 0.0
    v_few[:, :m] = v[:, :m]
    v_few[:, m + 4 : m + 4 + few] = v[:, m : m + few]
    both = rate_x[:, None] + rate_y[None, :]
    ends = np.zeros((4, 16, m))
    ends[0, :few], ends[1, :few] = tu[1][m : m + few], tu[2][m : m + few]
    ends[2, 4 : 4 + few], ends[3, 4 : 4 + few] = tv[1][m : m + few], tv[2][m : m + few]
    corner = np.zeros((m, lanes))
    corner[:, m + 4 : m + 4 + few] = 2.0 * tv[1][m : m + few].T
    a = [rp[0].T @ t for t in rp]
    b = [cp[0].T @ t for t in cp]
    even_x, odd_x = (rp[0].T @ basis(nx, m, RATIO, f) for f in (np.cos, np.sin))
    even_y, odd_y = ((cp[0].T @ basis(ny, m, RATIO, f)).T for f in (np.cos, np.sin))
    small = np.stack(
        [even_x, odd_x, even_y, odd_y, a[1], a[2], a[1] @ a[1], b[1], b[2], b[1] @ b[1],
         both, both**2, np.tile(2.0 * rate_y[None, :], (m, 1)), np.tile(2.0 * rate_x[:, None], (1, m))]
    ).astype(np.float32)
    deep = (W + 1) * m
    tables = [
        halves(u_few),
        halves(np.swapaxes(u[:, :tall].reshape(PX, cx, tall), 1, 2)),
        halves(v),
        halves(v_few.T),
        halves(np.concatenate([t[:tall] for t in tu], 1).T),
        halves(np.concatenate(tv, 1)),
        halves(ends.reshape(64, m)),
        halves(corner),
    ]
    any_space = pl.BlockSpec(memory_space=pl.ANY)
    vmem = pl.BlockSpec(memory_space=pltpu.VMEM)
    dma = pltpu.SemaphoreType.DMA
    coeffs = pltpu.VMEM((W, m // 2, lanes), F32)
    thin = m // 2 + 16
    held = pl.pallas_call(
        functools.partial(kernel, dims, owners),
        out_shape=(
            pltpu.VMEM((L, cx, cy), F32),
            pltpu.VMEM((L, m // 2, lanes), F32),
        ),
        in_specs=[any_space] * 13,
        out_specs=(any_space, any_space),
        scratch_shapes=[
            pltpu.VMEM((L, cx, cy), F32),
            pltpu.VMEM((L, thin, lanes), F32),
            pltpu.VMEM((2, G, thin, lanes), F32),
            pltpu.VMEM((cx * L // 16, 128), F32),
            pltpu.VMEM((2, cx * L // 16, 128), F32),
            pltpu.VMEM((L, cx + 16, cy + 128), F32),
            pltpu.VMEM((L, cx, cy), F32),
            pltpu.VMEM((L, cx, cy), F32),
            pltpu.VMEM((L, m // 2 + 8, lanes), F32),
            pltpu.VMEM((2, cx, tall), BF16),
            pltpu.VMEM((2, tall, cy), BF16),
            pltpu.VMEM((2, m // 2 + 8, lanes), F32),
            pltpu.VMEM((2, m // 2, lanes), F32),
            pltpu.VMEM((W, m, m), F32),
            coeffs,
            coeffs,
            pltpu.VMEM((8, 128), F32),
            pltpu.VMEM((8, 128), F32),
            pltpu.VMEM((5, m, m), F32),
            pltpu.VMEM((2, tall, cx), BF16),
            pltpu.VMEM((2, cy, lanes), BF16),
            pltpu.VMEM((2, deep, tall), BF16),
            pltpu.VMEM((2, lanes, deep), BF16),
            pltpu.VMEM((2, 64, m), BF16),
            pltpu.VMEM((2, m, lanes), BF16),
            pltpu.VMEM((14, m, m), F32),
            pltpu.SMEM(relax_rates.shape, F32),
            pltpu.SMEM(nest_offsets.shape[::-1], jnp.int32),
            dma((L + 12,)),
            dma((L,)),
            dma((2, G)),
            dma((4,)),
            dma((4,)),
            dma((2,)),
            dma((2,)),
            dma((L,)),
            dma((2, G)),
            dma((L,)),
            dma((2, G)),
            dma((L,)),
        ],
        compiler_params=pltpu.CompilerParams(collective_id=0, has_side_effects=True),
    )(initial_state, drive_modes, relax_rates, nest_offsets.T,
      *(jnp.asarray(t) for t in tables), jnp.asarray(small))
    return pl.pallas_call(
        store,
        out_shape=[
            jax.ShapeDtypeStruct((1, L, cx, cy), F32),
            jax.ShapeDtypeStruct((1, L, m, m), F32),
        ],
        in_specs=[any_space, vmem],
        out_specs=[any_space] * 2,
        scratch_shapes=[pltpu.VMEM((L, m, m), F32), dma((2,))],
    )(*(pltpu.with_memory_space_constraint(x, pltpu.VMEM) for x in held))


def solution(mesh):
    nests, PY, PX = (mesh.shape[n] for n in ("nest", "py", "px"))
    spec = P("nest", None, "px", "py")

    def local(initial_state, drive_modes, relax_rates, nest_offsets):
        _, L, cx, cy = initial_state.shape
        W, _, m, _ = drive_modes.shape
        places = sorted(
            range(PY * PX),
            key=lambda g: (abs(2 * (g // PY) - PX + 1) + abs(2 * (g % PY) - PY + 1), g),
        )
        dims = (nests, PY, PX, L, cx, cy, m, W)
        return body(dims, tuple(places[:L]), initial_state, drive_modes, relax_rates, nest_offsets)

    return jax.shard_map(
        local,
        mesh=mesh,
        in_specs=(spec, P(), P("nest", None), P()),
        out_specs=(spec, P("nest", None, None, None)),
        check_vma=False,
    )
```

```python
import functools
import math

import jax
import jax.numpy as jnp
import numpy as np
from jax import lax
from jax.experimental import pallas as pl
from jax.experimental.pallas import tpu as pltpu
from jax.sharding import PartitionSpec as P

RATIO = 3
RATE = 0.2
MESH = pl.DeviceIdType.MESH
F32, BF16 = jnp.float32, jnp.bfloat16


def basis(cells, modes, refine, fn=np.cos):
    j = np.arange(modes, dtype=np.int64)
    q = 2 * np.arange(cells, dtype=np.int64) + 1
    product = (j[None, :] * q[:, None]) % (4 * refine * cells)
    weight = np.where(j == 0, 1.0, 2.0) / cells
    return np.sqrt(weight)[None, :] * fn(np.pi * product / (2.0 * refine * cells))


def half_step(table):
    pad = np.pad(table, ((1, 1), (0, 0)))
    return (0.5 - 2 * RATE) * table + RATE * (pad[2:] + pad[:-2])


def powers(table, count):
    out = [table]
    for _ in range(count):
        out.append(half_step(out[-1]))
    return out


def halves(table):
    high = np.asarray(table, np.float32).astype(BF16)
    low = (np.asarray(table, np.float64) - high.astype(np.float64)).astype(np.float32)
    return np.stack([high, low.astype(BF16)])


def split(x):
    high = x.astype(BF16)
    return high, (x - high.astype(F32)).astype(BF16)


def mm(a, b):
    return lax.dot_general(a, b, (((1,), (0,)), ((), ())), preferred_element_type=F32)


def dot3(a, b):
    a = a if isinstance(a, tuple) else split(a)
    b = b if isinstance(b, tuple) else split(b)
    return mm(a[0], b[0]) + (mm(a[0], b[1]) + mm(a[1], b[0]))


def dot3t(a, b):
    b = b if isinstance(b, tuple) else split(b)

    def nt(x, y):
        return lax.dot_general(x, y, (((1,), (1,)), ((), ())), preferred_element_type=F32)

    return nt(a[0], b[0]) + (nt(a[0], b[1]) + nt(a[1], b[0]))


def pack(x):
    h = x.shape[0] // 2
    return jnp.concatenate([x[:h], x[h:]], 1)


def unpack(x):
    h = x.shape[1] // 2
    return jnp.concatenate([x[:, :h], x[:, h:]], 0)


def pack_wide(x, m):
    low = x[:m].T[m : m + 8]
    return jnp.concatenate(
        [pack(x[:m, :m]), x[m : m + 8], jnp.concatenate([low, jnp.zeros_like(low)], 1)], 0
    )


def unpack_fix(x, m):
    tile = x[m // 2 :]
    low = jnp.concatenate([tile[:, :m], jnp.zeros((m - 8, m), F32)], 0).T
    top = jnp.concatenate([unpack(x[: m // 2]), low], 1)
    return jnp.concatenate([top, tile, jnp.zeros((8, 2 * m), F32)], 0)[:, : m + 16]


def unpack_wide(x, m):
    low = jnp.concatenate([x[m // 2 + 8 :, :m], jnp.zeros((m - 8, m), F32)], 0).T
    top = jnp.concatenate([unpack(x[: m // 2]), low], 1)
    return jnp.concatenate([top, x[m // 2 : m // 2 + 8], jnp.zeros((8, 2 * m), F32)], 0)


def loop(n, fn):
    if n <= 16:
        for i in range(n):
            fn(i)
    else:
        lax.fori_loop(0, n, lambda i, c: (fn(i), c)[1], 0)


def kernel(
    dims, owners,
    field, drive, relax_hbm, offs_hbm,
    u_hbm, ut_hbm, v_hbm, vt_hbm, left_hbm, right_hbm, up_hbm, small_hbm,
    out, modes,
    fvm, pbuf, abuf, strip, near, wide, calm, state, fix, tally, u_t, vt_t, zbuf, mail, start, par, cbuf, lead, glead, tx,
    ut_t, v_t, left, right, up, small, relax, offs,
    load_sem, a_send, a_recv, h_send, h_recv, c_sem, g_sem, out_sem, b_send, f_recv, m_recv,
):
    nests, PY, PX, L, cx, cy, m, W = dims
    G, nx, ny = PY * PX, cx * PX, cy * PY
    k, py, px = lax.axis_index("nest"), lax.axis_index("py"), lax.axis_index("px")
    me = px * PY + py
    odd = k % 2 == 1
    leader = k + 1 - k % 2
    placed = [me == o for o in owners]
    level = sum(jnp.where(c, l, 0) for l, c in enumerate(placed))
    in_place = functools.reduce(jnp.logical_or, placed)
    is_owner = jnp.logical_and(odd, in_place)
    is_spare = jnp.logical_and(jnp.logical_not(odd), in_place)
    owns = [jnp.logical_and(odd, c) for c in placed]

    def at(g, nest):
        return (nest, g % PY, g // PY)

    def plain(g):
        return functools.reduce(jnp.logical_and, [g != o for o in owners])

    hops = [(-2, k > 2), (2, k < nests - 2)]
    sides = [
        (px > 0, (k, py, px - 1)), (px < PX - 1, (k, py, px + 1)),
        (py > 0, (k, py - 1, px)), (py < PY - 1, (k, py + 1, px)),
    ]
    beside = sum(jnp.where(c, 1, 0) for c, _ in sides)
    barrier = pltpu.get_barrier_semaphore()
    for l, o in enumerate(owners):
        @pl.when(jnp.logical_not(owns[l]))
        def _():
            pl.semaphore_signal(barrier, inc=1, device_id=at(o, leader), device_id_type=MESH)

    for cond, device in sides:
        @pl.when(cond)
        def _():
            pl.semaphore_signal(barrier, inc=1, device_id=device, device_id_type=MESH)

    @pl.when(is_owner)
    def _():
        def greet(g):
            pl.semaphore_signal(barrier, inc=1, device_id=at(g, k - 1), device_id_type=MESH)

            @pl.when(plain(g))
            def _():
                pl.semaphore_signal(barrier, inc=1, device_id=at(g, k), device_id_type=MESH)
        loop(G, greet)

        for hop, cond in hops:
            @pl.when(cond)
            def _():
                pl.semaphore_signal(
                    barrier, inc=1, device_id=(k + hop, py, px), device_id_type=MESH
                )

    def hop_copy(src, dst, send_sem, recv_sem, hop):
        return pltpu.make_async_remote_copy(
            src_ref=src, dst_ref=dst, send_sem=send_sem, recv_sem=recv_sem,
            device_id=(k + hop, py, px), device_id_type=MESH,
        )

    gain_out = hop_copy(lead, glead, g_sem.at[0], g_sem.at[1], 1)
    gain_in = hop_copy(lead, glead, g_sem.at[0], g_sem.at[1], -1)
    chain_out = hop_copy(cbuf, par, c_sem.at[0], c_sem.at[1], 2)
    chain_in = hop_copy(cbuf, par, c_sem.at[0], c_sem.at[1], -2)

    load = pltpu.make_async_copy(field.at[0], fvm, load_sem.at[0])
    load.start()
    rows_here = pl.ds(pl.multiple_of(px * cx, 8), cx)
    cols_here = pl.ds(pl.multiple_of(py * cy, 128), cy)
    pairs = [
        (v_hbm.at[:, cols_here], v_t), (ut_hbm.at[:, px], ut_t),
        (u_hbm.at[:, rows_here], u_t), (vt_hbm.at[:, :, cols_here], vt_t),
        (relax_hbm, relax), (offs_hbm, offs), (small_hbm, small),
        (left_hbm, left), (right_hbm, right), (up_hbm, up),
    ]
    tables = [
        pltpu.make_async_copy(src, dst, load_sem.at[2 + i]) for i, (src, dst) in enumerate(pairs)
    ]
    for c in tables[:4]:
        c.start()
    get_drive = pltpu.make_async_copy(drive.at[:, level], start, load_sem.at[1])

    @pl.when(in_place)
    def _():
        tables[4].start()

    @pl.when(is_owner)
    def _():
        for c in tables[5:]:
            c.start()

        @pl.when(k < 2)
        def _():
            get_drive.start()

    tables[0].wait()
    tables[1].wait()
    load.wait()
    half = dot3(fvm[...].reshape(L * cx, cy), (v_t[0], v_t[1]))
    for l in range(L):
        pbuf[l] = pack_wide(dot3((ut_t[0], ut_t[1]), half[l * cx : (l + 1) * cx]), m)

    lane = lax.broadcasted_iota(jnp.int32, (cx, 128), 1)
    edge = jnp.zeros((cx, 128), F32)
    for l in range(L):
        ends = jnp.where(lane < 64, fvm[l, :, 0:128], fvm[l, :, cy - 128 : cy])
        turned = pltpu.roll(ends, 8 * l, 1) if l else ends
        shift = (lane - 8 * l + 4) % 128
        edge = jnp.where(shift < 8, turned, edge)
        wide[l, 8 : cx + 8, 0:cy] = fvm[l]
    folds = 128 // (8 * L)
    thin = cx // folds
    short = lax.broadcasted_iota(jnp.int32, (thin, 128), 1)
    folded = edge[:thin]
    for i in range(1, folds):
        moved = pltpu.roll(edge[i * thin : (i + 1) * thin], 8 * L * i, 1)
        folded = jnp.where((short + 4) % 128 < 8 * L * i, folded, moved)
    strip[...] = folded
    bare = jnp.zeros((8, cy + 128), F32)

    @pl.when(px == 0)
    def _():
        for l in range(L):
            wide[l, 0:8, :] = bare

    @pl.when(px == PX - 1)
    def _():
        for l in range(L):
            wide[l, cx + 8 : cx + 16, :] = bare

    @pl.when(py == 0)
    def _():
        near[0] = jnp.zeros(near.shape[1:], F32)

    @pl.when(py == PY - 1)
    def _():
        near[1] = jnp.zeros(near.shape[1:], F32)

    @pl.when(is_owner)
    def _():
        abuf[G + me] = pbuf[level]
        pl.semaphore_wait(barrier, beside + 2 * G - 1 + sum(jnp.where(c, 1, 0) for _, c in hops))

    @pl.when(jnp.logical_not(is_owner))
    def _():
        pl.semaphore_wait(barrier, beside + L)

    def remote(src, dst, send_sem, recv_sem, g, nest):
        return pltpu.make_async_remote_copy(
            src_ref=src, dst_ref=dst, send_sem=send_sem, recv_sem=recv_sem,
            device_id=at(g, nest), device_id_type=MESH,
        )

    def share(l):
        return remote(
            pbuf.at[l], abuf.at[(k % 2) * G + me], a_send, a_recv, owners[l], leader
        )

    def settled(ref, sem):
        pltpu.make_async_copy(ref, ref, sem).wait()

    part = jnp.where(level < L // 2, 0, 1)
    keep_modes = pltpu.make_async_copy(mail.at[1], modes.at[level], m_recv)
    keep_fix = pltpu.make_async_copy(zbuf.at[1], fix.at[level], f_recv.at[part])

    def beam(src, dst, i, device):
        return pltpu.make_async_remote_copy(
            src_ref=src, dst_ref=dst, send_sem=h_send.at[i], recv_sem=h_recv.at[i],
            device_id=device, device_id_type=MESH,
        )

    top, bottom = pl.ds(0, 8), pl.ds(cx + 8, 8)
    first_rows, last_rows = pl.ds(8, 8), pl.ds(cx, 8)
    halo = [
        beam(wide.at[:, first_rows], wide.at[:, bottom], 0, sides[0][1]),
        beam(wide.at[:, last_rows], wide.at[:, top], 1, sides[1][1]),
        beam(strip, near.at[1], 2, sides[2][1]),
        beam(strip, near.at[0], 3, sides[3][1]),
    ]

    def start_halo(i):
        @pl.when(sides[i][0])
        def _():
            halo[i].start()

    def land_halo(i):
        @pl.when(sides[i ^ 1][0])
        def _():
            halo[i].wait_recv()

    for l, o in enumerate(owners):
        @pl.when(jnp.logical_not(owns[l]))
        def _():
            share(l).start()

    @pl.when(is_spare)
    def _():
        tables[4].wait()
        lead[...] = jnp.full(lead.shape, relax[0, level], F32)
        gain_out.start()

    start_halo(2)
    start_halo(3)

    def widen_patch():
        land_halo(2)
        land_halo(3)
        after, before = near[1], near[0]
        for l in range(L):
            for i in range(folds):
                back = (128 - 8 * l - 8 * L * i) % 128
                right, left_side = after, before
                if back:
                    right, left_side = pltpu.roll(after, back, 1), pltpu.roll(before, back, 1)
                wide[l, 8 + i * thin : 8 + (i + 1) * thin, cy:] = jnp.where(
                    short < 64, right, left_side
                )
        start_halo(0)
        start_halo(1)

    def run_free():
        land_halo(0)
        land_halo(1)
        shape = (cx + 16, cy + 128)
        row = lax.broadcasted_iota(jnp.int32, shape, 0) + (px * cx - 8)
        col = lax.broadcasted_iota(jnp.int32, shape, 1)
        col = jnp.where(col < cy + 64, col, col - (cy + 128)) + py * cy
        inside = (row >= 0) & (row < nx) & (col >= 0) & (col < ny)
        for l in range(L):
            now = wide[l]
            for _ in range(W):
                side = pltpu.roll(now, 1, 0) + pltpu.roll(now, cx + 15, 0)
                side = side + pltpu.roll(now, 1, 1) + pltpu.roll(now, cy + 127, 1)
                now = jnp.where(inside, now + RATE * (side - 4.0 * now), 0.0)
            calm[l] = now[8 : cx + 8, 0:cy]

    @pl.when(is_owner)
    def _():
        tables[4].wait()
        tables[5].wait()
        tables[6].wait()
        gain = relax[0, level]

        def turn(kk, cells, dim, axis):
            number = lax.broadcasted_iota(jnp.int32, (m, m), dim).astype(F32)
            product = number * (2 * RATIO * offs[axis, kk]).astype(F32)
            period = float(4 * RATIO * cells)
            product = product - period * jnp.floor(product * (1.0 / period))
            angle = product * (math.pi / (2.0 * RATIO * cells))
            return jnp.cos(angle), jnp.sin(angle)

        def flat(kk):
            eye = jnp.where(
                lax.broadcasted_iota(jnp.int32, (m, m), 0)
                == lax.broadcasted_iota(jnp.int32, (m, m), 1),
                1.0, 0.0,
            ).astype(F32)
            cos_x, sin_x = turn(kk, nx, 1, 0)
            cos_y, sin_y = turn(kk, ny, 0, 1)
            row = jnp.where(kk == 0, eye, small[0] * cos_x - small[1] * sin_x)
            col = jnp.where(kk == 0, eye, small[2] * cos_y - small[3] * sin_y)
            return split(row), split(col)

        a1, b1 = split(small[4]), split(small[7])

        def curved(rate):
            return split(small[5] - rate * small[6]), split(small[8] - rate * small[9])

        def maps(kk, rate):
            a2, b2 = curved(rate)
            f0, g0 = flat(kk)
            f1, f2 = split(dot3(a1, f0)), split(dot3(a2, f0))
            g1, g2 = split(dot3(g0, b1)), split(dot3(g0, b2))
            return f0, f1, f2, g0, g1, g2, 2.0 * (1.0 - rate)

        def follow(cs, ms):
            f0, f1, f2, g0, g1, g2, rest = ms
            c1, c2, c3 = (split(c) for c in cs)
            y10, y20, y30 = dot3(c1, g0), dot3(c2, g0), dot3(c3, g0)
            y11, y21, y12 = dot3(c1, g1), dot3(c2, g1), dot3(c1, g2)
            y10s = split(y10)
            return (
                dot3(f0, y10s),
                dot3(f0, y20),
                dot3(f0, y30),
                dot3(f1, y10s) + dot3(f0, y11),
                dot3(f0, y21 + y12) + dot3(f1, y20 + rest * y11) + dot3(f2, y10s),
            )

        def nudge(own, moved, rate):
            own2, own3 = own[1] + rate * moved[3], own[2] + rate * moved[4]
            d1, d2, d3 = rate * (moved[0] - own[0]), rate * (moved[1] - own2), rate * (moved[2] - own3)
            return (d1, d2, d3), (own[0] + d1, own2 + d2, own3 + d3)

        own_maps = maps(k, gain)
        gain_in.wait_recv()
        lead_gain = glead[0:1, 0:m]
        lead_maps = maps(k - 1, lead_gain)

        def first(cs):
            for i, x in enumerate(follow(cs, lead_maps)):
                tx[i] = x

        @pl.when(k < 2)
        def _():
            get_drive.wait()
            first([start[w] for w in range(W)])

        tables[7].wait()
        tables[8].wait()

        settled(abuf.at[pl.ds(0, 2 * G - 1)], a_recv)

        def project(i):
            total = abuf[i * G]
            if G <= 16:
                for g in range(1, G):
                    total = total + abuf[i * G + g]
            else:
                total = lax.fori_loop(1, G, lambda g, c: c + abuf[i * G + g], total)
            both = dot3((left[0], left[1]), dot3(unpack_wide(total, m), (right[0], right[1])))

            def block(i, j):
                return both[i * m : (i + 1) * m, j * m : (j + 1) * m]

            return [
                sum(float(math.comb(w, i)) * block(i, w - i) for i in range(w + 1))
                for w in (1, 2, 3)
            ]

        def settle(s, rate):
            s1, s2, s3 = s
            a2, b2 = curved(rate)
            s1s, s2s = split(s1), split(s2)
            z11 = dot3(s1s, b1)
            x2 = dot3(a1, s1s) + z11
            x3 = dot3(s2s, b1) + dot3(s1s, b2) + dot3(a2, s1s)
            x3 = x3 + dot3(a1, s2 + 2.0 * (1.0 - rate) * z11)
            return s1, s2 - rate * x2, s3 - rate * x3

        before, after = project(0), project(1)
        before, after = settle(before, lead_gain), settle(after, gain)

        @pl.when(k > 1)
        def _():
            widen_patch()
            chain_in.wait_recv()
            first([unpack(par[w]) for w in range(W)])

        d_lead, c_lead = nudge(before, [tx[i] for i in range(5)], lead_gain)
        tables[9].wait()
        def widen(x):
            return jnp.concatenate([x, jnp.zeros_like(x)], 1)

        def table(i):
            return up[0, 16 * i : 16 * (i + 1), :m], up[1, 16 * i : 16 * (i + 1), :m]

        def correct(d):
            d1, d2, d3 = d
            e1 = split(d1)
            main = d3 + small[10] * d2 + small[11] * d1
            rows = dot3(table(0), d2 + small[12] * d1) + dot3(table(1), e1)
            cols = dot3t(table(2), d2 + small[13] * d1) + dot3t(table(3), e1)
            corner = dot3(dot3(table(0), e1), (up[0, 64:], up[1, 64:]))
            return jnp.concatenate([pack(main), (widen(rows + cols) + corner)[:8]], 0)

        def mend(i, g):
            return remote(
                zbuf.at[i], fix.at[level], b_send, f_recv.at[part], g, k - 1 + i
            )

        def tell(i, g):
            return remote(
                mail.at[i], modes.at[level], b_send, m_recv, g, k - 1 + i
            )

        def give(i):
            for copy in (mend, tell):
                def one(j):
                    g = jnp.where(2 * px < PX, G - 1 - j, j)
                    if i == 0:
                        copy(i, g).start()
                    else:
                        @pl.when(g != me)
                        def _():
                            copy(i, g).start()
                loop(G, one)

        def advance():
            zbuf[0] = correct(d_lead)
            mail[0] = pack(c_lead[W - 1])
            give(0)

        @pl.when(k >= nests - 2)
        def _():
            advance()

        d_own, c_own = nudge(after, follow(c_lead, own_maps), gain)
        for w in range(W):
            cbuf[w] = pack(c_own[w])

        @pl.when(k < nests - 2)
        def _():
            chain_out.start()

        @pl.when(k < 2)
        def _():
            widen_patch()

        @pl.when(k < nests - 2)
        def _():
            advance()

        zbuf[1] = correct(d_own)
        mail[1] = pack(c_own[W - 1])
        give(1)
        keep_fix.start()
        keep_modes.start()
        run_free()

    @pl.when(jnp.logical_not(is_owner))
    def _():
        widen_patch()
        run_free()

    tables[2].wait()
    tables[3].wait()

    puts = [pltpu.make_async_copy(state.at[l], out.at[l], out_sem) for l in range(L)]

    def finish(i, some):
        settled(fix.at[pl.ds(some[0], len(some))], f_recv.at[i])
        half = [dot3(unpack_fix(fix[l], m), (vt_t[0], vt_t[1])) for l in some]
        for l, x in zip(some, half):
            state[l] = calm[l] + dot3((u_t[0], u_t[1]), x)
            puts[l].start()

    finish(0, range(L // 2))
    finish(1, range(L // 2, L))
    settled(modes, m_recv)

    @pl.when(jnp.logical_not(is_owner))
    def _():
        settled(pbuf, a_send)

    @pl.when(is_owner)
    def _():
        settled(pbuf.at[pl.ds(0, L - 1)], a_send)
        settled(tally, b_send)

        @pl.when(k < nests - 2)
        def _():
            chain_out.wait_send()

    @pl.when(is_spare)
    def _():
        gain_out.wait_send()

    for i in range(4):
        @pl.when(sides[i][0])
        def _():
            halo[i].wait_send()
    settled(state, out_sem)


def store(state, packed, state_out, modes_out, modes, sem):
    first = pltpu.make_async_copy(state, state_out.at[0], sem.at[0])
    second = pltpu.make_async_copy(modes, modes_out.at[0], sem.at[1])
    first.start()
    for l in range(packed.shape[0]):
        modes[l] = unpack(packed[l])
    second.start()
    first.wait()
    second.wait()


def wide_tables(cells, modes, windows):
    stages = powers(basis(cells, modes, 1), windows)
    edges = np.zeros((cells, modes))
    for e in range(windows):
        edges[e, 2 * e] = 1.0
        edges[cells - 1 - e, 2 * e + 1] = 1.0
    full = np.concatenate([stages[0], edges], 1)
    rate = 0.5 - 2 * RATE + 2 * RATE * np.cos(np.pi * np.arange(modes) / cells)
    turns = []
    for i, t in enumerate(stages):
        top = np.diag(rate**i)
        turns.append(np.concatenate([top, edges.T @ (t - stages[0] @ top)], 0))
    return stages, full, turns, rate


def body(dims, owners, initial_state, drive_modes, relax_rates, nest_offsets):
    nests, PY, PX, L, cx, cy, m, W = dims
    G, nx, ny = PY * PX, cx * PX, cy * PY
    assert nests % 2 == 0 and W == 3
    tall, lanes = m + 16, 2 * m
    rp, u, tu, rate_x = wide_tables(nx, m, W)
    cp, v, tv, rate_y = wide_tables(ny, m, W)
    few = 2 * (W - 1)
    u_few, v_few = u[:, :tall].copy(), np.zeros((ny, tall))
    u_few[:, m + few :] = 0.0
    v_few[:, :m] = v[:, :m]
    v_few[:, m + 4 : m + 4 + few] = v[:, m : m + few]
    both = rate_x[:, None] + rate_y[None, :]
    ends = np.zeros((4, 16, m))
    ends[0, :few], ends[1, :few] = tu[1][m : m + few], tu[2][m : m + few]
    ends[2, 4 : 4 + few], ends[3, 4 : 4 + few] = tv[1][m : m + few], tv[2][m : m + few]
    corner = np.zeros((m, lanes))
    corner[:, m + 4 : m + 4 + few] = 2.0 * tv[1][m : m + few].T
    a = [rp[0].T @ t for t in rp]
    b = [cp[0].T @ t for t in cp]
    even_x, odd_x = (rp[0].T @ basis(nx, m, RATIO, f) for f in (np.cos, np.sin))
    even_y, odd_y = ((cp[0].T @ basis(ny, m, RATIO, f)).T for f in (np.cos, np.sin))
    small = np.stack(
        [even_x, odd_x, even_y, odd_y, a[1], a[2], a[1] @ a[1], b[1], b[2], b[1] @ b[1],
         both, both**2, np.tile(2.0 * rate_y[None, :], (m, 1)), np.tile(2.0 * rate_x[:, None], (1, m))]
    ).astype(np.float32)
    deep = (W + 1) * m
    tables = [
        halves(u_few),
        halves(np.swapaxes(u[:, :tall].reshape(PX, cx, tall), 1, 2)),
        halves(v),
        halves(v_few.T),
        halves(np.concatenate([t[:tall] for t in tu], 1).T),
        halves(np.concatenate(tv, 1)),
        halves(np.concatenate([np.pad(ends.reshape(64, m), ((0, 0), (0, m))), corner], 0)),
    ]
    any_space = pl.BlockSpec(memory_space=pl.ANY)
    vmem = pl.BlockSpec(memory_space=pltpu.VMEM)
    dma = pltpu.SemaphoreType.DMA
    coeffs = pltpu.VMEM((W, m // 2, lanes), F32)
    thin = m // 2 + 16
    held = pl.pallas_call(
        functools.partial(kernel, dims, owners),
        out_shape=(
            pltpu.VMEM((L, cx, cy), F32),
            pltpu.VMEM((L, m // 2, lanes), F32),
        ),
        in_specs=[any_space] * 12,
        out_specs=(any_space, any_space),
        scratch_shapes=[
            pltpu.VMEM((L, cx, cy), F32),
            pltpu.VMEM((L, thin, lanes), F32),
            pltpu.VMEM((2 * G, thin, lanes), F32),
            pltpu.VMEM((cx * L // 16, 128), F32),
            pltpu.VMEM((2, cx * L // 16, 128), F32),
            pltpu.VMEM((L, cx + 16, cy + 128), F32),
            pltpu.VMEM((L, cx, cy), F32),
            pltpu.VMEM((L, cx, cy), F32),
            pltpu.VMEM((L, m // 2 + 8, lanes), F32),
            pltpu.VMEM((2 * G - 1, m + 8, lanes), F32),
            pltpu.VMEM((2, cx, tall), BF16),
            pltpu.VMEM((2, tall, cy), BF16),
            pltpu.VMEM((2, m // 2 + 8, lanes), F32),
            pltpu.VMEM((2, m // 2, lanes), F32),
            pltpu.VMEM((W, m, m), F32),
            coeffs,
            coeffs,
            pltpu.VMEM((8, 128), F32),
            pltpu.VMEM((8, 128), F32),
            pltpu.VMEM((5, m, m), F32),
            pltpu.VMEM((2, tall, cx), BF16),
            pltpu.VMEM((2, cy, lanes), BF16),
            pltpu.VMEM((2, deep, tall), BF16),
            pltpu.VMEM((2, lanes, deep), BF16),
            pltpu.VMEM((2, 64 + m, lanes), BF16),
            pltpu.VMEM((14, m, m), F32),
            pltpu.SMEM(relax_rates.shape, F32),
            pltpu.SMEM(nest_offsets.shape[::-1], jnp.int32),
            dma((12,)),
            dma,
            dma,
            dma((4,)),
            dma((4,)),
            dma((2,)),
            dma((2,)),
            dma,
            dma,
            dma((2,)),
            dma,
        ],
        compiler_params=pltpu.CompilerParams(collective_id=0, has_side_effects=True),
    )(initial_state, drive_modes, relax_rates, nest_offsets.T,
      *(jnp.asarray(t) for t in tables), jnp.asarray(small))
    return pl.pallas_call(
        store,
        out_shape=[
            jax.ShapeDtypeStruct((1, L, cx, cy), F32),
            jax.ShapeDtypeStruct((1, L, m, m), F32),
        ],
        in_specs=[any_space, vmem],
        out_specs=[any_space] * 2,
        scratch_shapes=[pltpu.VMEM((L, m, m), F32), dma((2,))],
    )(*(pltpu.with_memory_space_constraint(x, pltpu.VMEM) for x in held))


def solution(mesh):
    nests, PY, PX = (mesh.shape[n] for n in ("nest", "py", "px"))
    spec = P("nest", None, "px", "py")

    def local(initial_state, drive_modes, relax_rates, nest_offsets):
        _, L, cx, cy = initial_state.shape
        W, _, m, _ = drive_modes.shape
        places = sorted(
            range(PY * PX),
            key=lambda g: (abs(2 * (g // PY) - PX + 1) + abs(2 * (g % PY) - PY + 1), g),
        )
        dims = (nests, PY, PX, L, cx, cy, m, W)
        return body(dims, tuple(places[:L]), initial_state, drive_modes, relax_rates, nest_offsets)

    return jax.shard_map(
        local,
        mesh=mesh,
        in_specs=(spec, P(), P("nest", None), P()),
        out_specs=(spec, P("nest", None, None, None)),
        check_vma=False,
    )
```

```python
import functools
import math

import jax
import jax.numpy as jnp
import numpy as np
from jax import lax
from jax.experimental import pallas as pl
from jax.experimental.pallas import tpu as pltpu
from jax.sharding import PartitionSpec as P

RATIO = 3
RATE = 0.2
MESH = pl.DeviceIdType.MESH
F32, BF16 = jnp.float32, jnp.bfloat16


def basis(cells, modes, refine, fn=np.cos):
    j = np.arange(modes, dtype=np.int64)
    q = 2 * np.arange(cells, dtype=np.int64) + 1
    product = (j[None, :] * q[:, None]) % (4 * refine * cells)
    weight = np.where(j == 0, 1.0, 2.0) / cells
    return np.sqrt(weight)[None, :] * fn(np.pi * product / (2.0 * refine * cells))


def half_step(table):
    pad = np.pad(table, ((1, 1), (0, 0)))
    return (0.5 - 2 * RATE) * table + RATE * (pad[2:] + pad[:-2])


def powers(table, count):
    out = [table]
    for _ in range(count):
        out.append(half_step(out[-1]))
    return out


def halves(table):
    high = np.asarray(table, np.float32).astype(BF16)
    low = (np.asarray(table, np.float64) - high.astype(np.float64)).astype(np.float32)
    return np.stack([high, low.astype(BF16)])


def split(x):
    high = x.astype(BF16)
    return high, (x - high.astype(F32)).astype(BF16)


def mm(a, b):
    return lax.dot_general(a, b, (((1,), (0,)), ((), ())), preferred_element_type=F32)


def dot3(a, b):
    a = a if isinstance(a, tuple) else split(a)
    b = b if isinstance(b, tuple) else split(b)
    return mm(a[0], b[0]) + (mm(a[0], b[1]) + mm(a[1], b[0]))


def dot3t(a, b):
    b = b if isinstance(b, tuple) else split(b)

    def nt(x, y):
        return lax.dot_general(x, y, (((1,), (1,)), ((), ())), preferred_element_type=F32)

    return nt(a[0], b[0]) + (nt(a[0], b[1]) + nt(a[1], b[0]))


def pack(x):
    h = x.shape[0] // 2
    return jnp.concatenate([x[:h], x[h:]], 1)


def unpack(x):
    h = x.shape[1] // 2
    return jnp.concatenate([x[:, :h], x[:, h:]], 0)


def pack_wide(x, m):
    low = x[:m].T[m : m + 8]
    return jnp.concatenate(
        [pack(x[:m, :m]), x[m : m + 8], jnp.concatenate([low, jnp.zeros_like(low)], 1)], 0
    )


def unpack_fix(x, m):
    tile = x[m // 2 :]
    low = jnp.concatenate([tile[:, :m], jnp.zeros((m - 8, m), F32)], 0).T
    top = jnp.concatenate([unpack(x[: m // 2]), low], 1)
    return jnp.concatenate([top, tile, jnp.zeros((8, 2 * m), F32)], 0)[:, : m + 16]


def unpack_wide(x, m):
    low = jnp.concatenate([x[m // 2 + 8 :, :m], jnp.zeros((m - 8, m), F32)], 0).T
    top = jnp.concatenate([unpack(x[: m // 2]), low], 1)
    return jnp.concatenate([top, x[m // 2 : m // 2 + 8], jnp.zeros((8, 2 * m), F32)], 0)


def loop(n, fn):
    if n <= 16:
        for i in range(n):
            fn(i)
    else:
        lax.fori_loop(0, n, lambda i, c: (fn(i), c)[1], 0)


def kernel(
    dims, owners,
    field, drive, relax_hbm, offs_hbm,
    u_hbm, ut_hbm, v_hbm, vt_hbm, left_hbm, right_hbm, up_hbm, small_hbm,
    out, modes,
    fvm, pbuf, abuf, strip, near, wide, calm, state, fix, tally, u_t, vt_t, zbuf, mail, start, par, cbuf, lead, glead, tx,
    ut_t, v_t, left, right, up, small, relax, offs,
    load_sem, a_send, a_recv, h_send, h_recv, c_sem, g_sem, out_sem, b_send, f_recv, m_recv,
):
    nests, PY, PX, L, cx, cy, m, W = dims
    G, nx, ny = PY * PX, cx * PX, cy * PY
    k, py, px = lax.axis_index("nest"), lax.axis_index("py"), lax.axis_index("px")
    me = px * PY + py
    odd = k % 2 == 1
    leader = k + 1 - k % 2
    placed = [me == o for o in owners]
    level = sum(jnp.where(c, l, 0) for l, c in enumerate(placed))
    in_place = functools.reduce(jnp.logical_or, placed)
    is_owner = jnp.logical_and(odd, in_place)
    is_spare = jnp.logical_and(jnp.logical_not(odd), in_place)
    owns = [jnp.logical_and(odd, c) for c in placed]

    def at(g, nest):
        return (nest, g % PY, g // PY)

    def plain(g):
        return functools.reduce(jnp.logical_and, [g != o for o in owners])

    hops = [(-2, k > 2), (2, k < nests - 2)]
    sides = [
        (px > 0, (k, py, px - 1)), (px < PX - 1, (k, py, px + 1)),
        (py > 0, (k, py - 1, px)), (py < PY - 1, (k, py + 1, px)),
    ]
    beside = sum(jnp.where(c, 1, 0) for c, _ in sides)
    load = pltpu.make_async_copy(field.at[0], fvm, load_sem.at[0])
    load.start()
    rows_here = pl.ds(pl.multiple_of(px * cx, 8), cx)
    cols_here = pl.ds(pl.multiple_of(py * cy, 128), cy)
    pairs = [
        (v_hbm.at[:, cols_here], v_t), (ut_hbm.at[:, px], ut_t),
        (u_hbm.at[:, rows_here], u_t), (vt_hbm.at[:, :, cols_here], vt_t),
        (relax_hbm, relax), (offs_hbm, offs), (small_hbm, small),
        (left_hbm, left), (right_hbm, right), (up_hbm, up),
    ]
    tables = [
        pltpu.make_async_copy(src, dst, load_sem.at[2 + i]) for i, (src, dst) in enumerate(pairs)
    ]
    for c in tables[:4]:
        c.start()
    barrier = pltpu.get_barrier_semaphore()
    for l, o in enumerate(owners):
        @pl.when(jnp.logical_not(owns[l]))
        def _():
            pl.semaphore_signal(barrier, inc=1, device_id=at(o, leader), device_id_type=MESH)

    for cond, device in sides:
        @pl.when(cond)
        def _():
            pl.semaphore_signal(barrier, inc=1, device_id=device, device_id_type=MESH)

    @pl.when(is_owner)
    def _():
        def greet(g):
            pl.semaphore_signal(barrier, inc=1, device_id=at(g, k - 1), device_id_type=MESH)

            @pl.when(plain(g))
            def _():
                pl.semaphore_signal(barrier, inc=1, device_id=at(g, k), device_id_type=MESH)
        loop(G, greet)

        for hop, cond in hops:
            @pl.when(cond)
            def _():
                pl.semaphore_signal(
                    barrier, inc=1, device_id=(k + hop, py, px), device_id_type=MESH
                )

    def hop_copy(src, dst, send_sem, recv_sem, hop):
        return pltpu.make_async_remote_copy(
            src_ref=src, dst_ref=dst, send_sem=send_sem, recv_sem=recv_sem,
            device_id=(k + hop, py, px), device_id_type=MESH,
        )

    gain_out = hop_copy(lead, glead, g_sem.at[0], g_sem.at[1], 1)
    gain_in = hop_copy(lead, glead, g_sem.at[0], g_sem.at[1], -1)
    chain_out = hop_copy(cbuf, par, c_sem.at[0], c_sem.at[1], 2)
    chain_in = hop_copy(cbuf, par, c_sem.at[0], c_sem.at[1], -2)

    get_drive = pltpu.make_async_copy(drive.at[:, level], start, load_sem.at[1])

    @pl.when(in_place)
    def _():
        tables[4].start()

    @pl.when(is_owner)
    def _():
        for c in tables[5:]:
            c.start()

        @pl.when(k < 2)
        def _():
            get_drive.start()

    tables[0].wait()
    tables[1].wait()
    load.wait()
    half = dot3(fvm[...].reshape(L * cx, cy), (v_t[0], v_t[1]))
    for l in range(L):
        pbuf[l] = pack_wide(dot3((ut_t[0], ut_t[1]), half[l * cx : (l + 1) * cx]), m)

    @pl.when(is_owner)
    def _():
        abuf[G + me] = pbuf[level]
        pl.semaphore_wait(barrier, beside + 2 * G - 1 + sum(jnp.where(c, 1, 0) for _, c in hops))

    @pl.when(jnp.logical_not(is_owner))
    def _():
        pl.semaphore_wait(barrier, beside + L)

    def remote(src, dst, send_sem, recv_sem, g, nest):
        return pltpu.make_async_remote_copy(
            src_ref=src, dst_ref=dst, send_sem=send_sem, recv_sem=recv_sem,
            device_id=at(g, nest), device_id_type=MESH,
        )

    def share(l):
        return remote(
            pbuf.at[l], abuf.at[(k % 2) * G + me], a_send, a_recv, owners[l], leader
        )

    def settled(ref, sem):
        pltpu.make_async_copy(ref, ref, sem).wait()

    part = jnp.where(level < L // 2, 0, 1)
    keep_modes = pltpu.make_async_copy(mail.at[1], modes.at[level], m_recv)
    keep_fix = pltpu.make_async_copy(zbuf.at[1], fix.at[level], f_recv.at[part])

    def beam(src, dst, i, device):
        return pltpu.make_async_remote_copy(
            src_ref=src, dst_ref=dst, send_sem=h_send.at[i], recv_sem=h_recv.at[i],
            device_id=device, device_id_type=MESH,
        )

    top, bottom = pl.ds(0, 8), pl.ds(cx + 8, 8)
    first_rows, last_rows = pl.ds(8, 8), pl.ds(cx, 8)
    halo = [
        beam(wide.at[:, first_rows], wide.at[:, bottom], 0, sides[0][1]),
        beam(wide.at[:, last_rows], wide.at[:, top], 1, sides[1][1]),
        beam(strip, near.at[1], 2, sides[2][1]),
        beam(strip, near.at[0], 3, sides[3][1]),
    ]

    def start_halo(i):
        @pl.when(sides[i][0])
        def _():
            halo[i].start()

    def land_halo(i):
        @pl.when(sides[i ^ 1][0])
        def _():
            halo[i].wait_recv()

    for l, o in enumerate(owners):
        @pl.when(jnp.logical_not(owns[l]))
        def _():
            share(l).start()

    @pl.when(is_spare)
    def _():
        tables[4].wait()
        lead[...] = jnp.full(lead.shape, relax[0, level], F32)
        gain_out.start()

    lane = lax.broadcasted_iota(jnp.int32, (cx, 128), 1)
    edge = jnp.zeros((cx, 128), F32)
    for l in range(L):
        ends = jnp.where(lane < 64, fvm[l, :, 0:128], fvm[l, :, cy - 128 : cy])
        turned = pltpu.roll(ends, 8 * l, 1) if l else ends
        shift = (lane - 8 * l + 4) % 128
        edge = jnp.where(shift < 8, turned, edge)
        wide[l, 8 : cx + 8, 0:cy] = fvm[l]
    folds = 128 // (8 * L)
    thin = cx // folds
    short = lax.broadcasted_iota(jnp.int32, (thin, 128), 1)
    folded = edge[:thin]
    for i in range(1, folds):
        moved = pltpu.roll(edge[i * thin : (i + 1) * thin], 8 * L * i, 1)
        folded = jnp.where((short + 4) % 128 < 8 * L * i, folded, moved)
    strip[...] = folded
    bare = jnp.zeros((8, cy + 128), F32)

    @pl.when(px == 0)
    def _():
        for l in range(L):
            wide[l, 0:8, :] = bare

    @pl.when(px == PX - 1)
    def _():
        for l in range(L):
            wide[l, cx + 8 : cx + 16, :] = bare

    @pl.when(py == 0)
    def _():
        near[0] = jnp.zeros(near.shape[1:], F32)

    @pl.when(py == PY - 1)
    def _():
        near[1] = jnp.zeros(near.shape[1:], F32)

    start_halo(2)
    start_halo(3)

    def widen_patch():
        land_halo(2)
        land_halo(3)
        after, before = near[1], near[0]
        for l in range(L):
            for i in range(folds):
                back = (128 - 8 * l - 8 * L * i) % 128
                right, left_side = after, before
                if back:
                    right, left_side = pltpu.roll(after, back, 1), pltpu.roll(before, back, 1)
                wide[l, 8 + i * thin : 8 + (i + 1) * thin, cy:] = jnp.where(
                    short < 64, right, left_side
                )
        start_halo(0)
        start_halo(1)

    def run_free():
        land_halo(0)
        land_halo(1)
        shape = (cx + 16, cy + 128)
        row = lax.broadcasted_iota(jnp.int32, shape, 0) + (px * cx - 8)
        col = lax.broadcasted_iota(jnp.int32, shape, 1)
        col = jnp.where(col < cy + 64, col, col - (cy + 128)) + py * cy
        inside = (row >= 0) & (row < nx) & (col >= 0) & (col < ny)
        for l in range(L):
            now = wide[l]
            for _ in range(W):
                side = pltpu.roll(now, 1, 0) + pltpu.roll(now, cx + 15, 0)
                side = side + pltpu.roll(now, 1, 1) + pltpu.roll(now, cy + 127, 1)
                now = jnp.where(inside, now + RATE * (side - 4.0 * now), 0.0)
            calm[l] = now[8 : cx + 8, 0:cy]

    @pl.when(is_owner)
    def _():
        tables[4].wait()
        tables[5].wait()
        tables[6].wait()
        gain = relax[0, level]

        def turn(kk, cells, dim, axis):
            number = lax.broadcasted_iota(jnp.int32, (m, m), dim).astype(F32)
            product = number * (2 * RATIO * offs[axis, kk]).astype(F32)
            period = float(4 * RATIO * cells)
            product = product - period * jnp.floor(product * (1.0 / period))
            angle = product * (math.pi / (2.0 * RATIO * cells))
            return jnp.cos(angle), jnp.sin(angle)

        def flat(kk):
            eye = jnp.where(
                lax.broadcasted_iota(jnp.int32, (m, m), 0)
                == lax.broadcasted_iota(jnp.int32, (m, m), 1),
                1.0, 0.0,
            ).astype(F32)
            cos_x, sin_x = turn(kk, nx, 1, 0)
            cos_y, sin_y = turn(kk, ny, 0, 1)
            row = jnp.where(kk == 0, eye, small[0] * cos_x - small[1] * sin_x)
            col = jnp.where(kk == 0, eye, small[2] * cos_y - small[3] * sin_y)
            return split(row), split(col)

        a1, b1 = split(small[4]), split(small[7])

        def curved(rate):
            return split(small[5] - rate * small[6]), split(small[8] - rate * small[9])

        def maps(kk, rate):
            a2, b2 = curved(rate)
            f0, g0 = flat(kk)
            f1, f2 = split(dot3(a1, f0)), split(dot3(a2, f0))
            g1, g2 = split(dot3(g0, b1)), split(dot3(g0, b2))
            return f0, f1, f2, g0, g1, g2, 2.0 * (1.0 - rate)

        def follow(cs, ms):
            f0, f1, f2, g0, g1, g2, rest = ms
            c1, c2, c3 = (split(c) for c in cs)
            y10, y20, y30 = dot3(c1, g0), dot3(c2, g0), dot3(c3, g0)
            y11, y21, y12 = dot3(c1, g1), dot3(c2, g1), dot3(c1, g2)
            y10s = split(y10)
            return (
                dot3(f0, y10s),
                dot3(f0, y20),
                dot3(f0, y30),
                dot3(f1, y10s) + dot3(f0, y11),
                dot3(f0, y21 + y12) + dot3(f1, y20 + rest * y11) + dot3(f2, y10s),
            )

        def nudge(own, moved, rate):
            own2, own3 = own[1] + rate * moved[3], own[2] + rate * moved[4]
            d1, d2, d3 = rate * (moved[0] - own[0]), rate * (moved[1] - own2), rate * (moved[2] - own3)
            return (d1, d2, d3), (own[0] + d1, own2 + d2, own3 + d3)

        own_maps = maps(k, gain)
        gain_in.wait_recv()
        lead_gain = glead[0:1, 0:m]
        lead_maps = maps(k - 1, lead_gain)

        def first(cs):
            for i, x in enumerate(follow(cs, lead_maps)):
                tx[i] = x

        @pl.when(k < 2)
        def _():
            get_drive.wait()
            first([start[w] for w in range(W)])

        tables[7].wait()
        tables[8].wait()

        settled(abuf.at[pl.ds(0, 2 * G - 1)], a_recv)

        def project(i):
            total = abuf[i * G]
            if G <= 16:
                for g in range(1, G):
                    total = total + abuf[i * G + g]
            else:
                total = lax.fori_loop(1, G, lambda g, c: c + abuf[i * G + g], total)
            main = unpack(total[: m // 2])
            edge = total[m // 2 : m // 2 + 8]
            low = jnp.concatenate([total[m // 2 + 8 :, :m], jnp.zeros((m - 8, m), F32)], 0).T
            low = split(low[:, :16])
            none = jnp.zeros_like(edge)
            row0 = jnp.concatenate([edge[:, :m], none[:, :m]], 0)
            edge = split(jnp.concatenate([edge, none], 0))

            def table(start, size):
                return right[0, start : start + size], right[1, start : start + size]

            row1, row2 = (dot3(edge, table(2 * m * j, 2 * m)) for j in range(2))
            q1, q2, q3 = (dot3(low, table(4 * m + 16 * j, 16)) for j in range(3))

            def rows(*parts):
                size = 16 * len(parts)
                return dot3((left[0, :, :size], left[1, :, :size]), jnp.concatenate(parts, 0))

            return [
                small[10] * main + (rows(row0) + q1),
                small[11] * main + (rows(2.0 * row1, row0) + small[13] * q1 + q2),
                small[14] * main
                + (rows(3.0 * row2, 3.0 * row1, row0) + small[15] * q1 + 1.5 * small[13] * q2 + q3),
            ]

        def settle(s, rate):
            s1, s2, s3 = s
            a2, b2 = curved(rate)
            s1s, s2s = split(s1), split(s2)
            z11 = dot3(s1s, b1)
            x2 = dot3(a1, s1s) + z11
            x3 = dot3(s2s, b1) + dot3(s1s, b2) + dot3(a2, s1s)
            x3 = x3 + dot3(a1, s2 + 2.0 * (1.0 - rate) * z11)
            return s1, s2 - rate * x2, s3 - rate * x3

        before, after = project(0), project(1)
        before, after = settle(before, lead_gain), settle(after, gain)

        @pl.when(k > 1)
        def _():
            widen_patch()
            chain_in.wait_recv()
            first([unpack(par[w]) for w in range(W)])

        d_lead, c_lead = nudge(before, [tx[i] for i in range(5)], lead_gain)
        tables[9].wait()
        def widen(x):
            return jnp.concatenate([x, jnp.zeros_like(x)], 1)

        def table(i):
            return up[0, 16 * i : 16 * (i + 1), :m], up[1, 16 * i : 16 * (i + 1), :m]

        def correct(d):
            d1, d2, d3 = d
            e1 = split(d1)
            main = d3 + small[10] * d2 + small[11] * d1
            rows = dot3(table(0), d2 + small[12] * d1) + dot3(table(1), e1)
            cols = dot3t(table(2), d2 + small[13] * d1) + dot3t(table(3), e1)
            corner = dot3(dot3(table(0), e1), (up[0, 64:], up[1, 64:]))
            return jnp.concatenate([pack(main), (widen(rows + cols) + corner)[:8]], 0)

        def mend(i, g):
            return remote(
                zbuf.at[i], fix.at[level], b_send, f_recv.at[part], g, k - 1 + i
            )

        def tell(i, g):
            return remote(
                mail.at[i], modes.at[level], b_send, m_recv, g, k - 1 + i
            )

        def give(copy, i):
            def one(j):
                g = jnp.where(2 * px < PX, G - 1 - j, j)
                if i == 0:
                    copy(i, g).start()
                else:
                    @pl.when(g != me)
                    def _():
                        copy(i, g).start()
            loop(G, one)

        def advance():
            mail[0] = pack(c_lead[W - 1])
            give(tell, 0)
            zbuf[0] = correct(d_lead)
            give(mend, 0)

        @pl.when(k >= nests - 2)
        def _():
            advance()

        d_own, c_own = nudge(after, follow(c_lead, own_maps), gain)
        for w in range(W):
            cbuf[w] = pack(c_own[w])

        @pl.when(k < nests - 2)
        def _():
            chain_out.start()

        @pl.when(k < 2)
        def _():
            widen_patch()

        @pl.when(k < nests - 2)
        def _():
            advance()

        zbuf[1] = correct(d_own)
        give(mend, 1)
        mail[1] = pack(c_own[W - 1])
        give(tell, 1)
        keep_fix.start()
        keep_modes.start()
        run_free()

    @pl.when(jnp.logical_not(is_owner))
    def _():
        widen_patch()
        run_free()

    tables[2].wait()
    tables[3].wait()

    most = L // 2
    far = jnp.where(2 * px < PX, 0, 1)
    for i in range(2):
        turn = (i + far) % 2
        first = turn * most
        some = pl.ds(first, most)
        settled(fix.at[some], f_recv.at[turn])
        half = [dot3(unpack_fix(fix[first + j], m), (vt_t[0], vt_t[1])) for j in range(most)]
        done = [calm[first + j] + dot3((u_t[0], u_t[1]), half[j]) for j in range(most)]
        for j in range(most):
            state[first + j] = done[j]
        pltpu.make_async_copy(state.at[some], out.at[some], out_sem).start()
    settled(modes, m_recv)

    @pl.when(jnp.logical_not(is_owner))
    def _():
        settled(pbuf, a_send)

    @pl.when(is_owner)
    def _():
        settled(pbuf.at[pl.ds(0, L - 1)], a_send)
        settled(tally, b_send)

        @pl.when(k < nests - 2)
        def _():
            chain_out.wait_send()

    @pl.when(is_spare)
    def _():
        gain_out.wait_send()

    for i in range(4):
        @pl.when(sides[i][0])
        def _():
            halo[i].wait_send()
    settled(state, out_sem)


def store(state, packed, state_out, modes_out, modes, sem):
    first = pltpu.make_async_copy(state, state_out.at[0], sem.at[0])
    second = pltpu.make_async_copy(modes, modes_out.at[0], sem.at[1])
    first.start()
    for l in range(packed.shape[0]):
        modes[l] = unpack(packed[l])
    second.start()
    first.wait()
    second.wait()


def wide_tables(cells, modes, windows):
    stages = powers(basis(cells, modes, 1), windows)
    edges = np.zeros((cells, modes))
    for e in range(windows):
        edges[e, 2 * e] = 1.0
        edges[cells - 1 - e, 2 * e + 1] = 1.0
    full = np.concatenate([stages[0], edges], 1)
    rate = 0.5 - 2 * RATE + 2 * RATE * np.cos(np.pi * np.arange(modes) / cells)
    turns = []
    for i, t in enumerate(stages):
        top = np.diag(rate**i)
        turns.append(np.concatenate([top, edges.T @ (t - stages[0] @ top)], 0))
    return stages, full, turns, rate


def body(dims, owners, initial_state, drive_modes, relax_rates, nest_offsets):
    nests, PY, PX, L, cx, cy, m, W = dims
    G, nx, ny = PY * PX, cx * PX, cy * PY
    assert nests % 2 == 0 and L % 2 == 0 and W == 3
    tall, lanes = m + 16, 2 * m
    rp, u, tu, rate_x = wide_tables(nx, m, W)
    cp, v, tv, rate_y = wide_tables(ny, m, W)
    few = 2 * (W - 1)
    u_few, v_few = u[:, :tall].copy(), np.zeros((ny, tall))
    u_few[:, m + few :] = 0.0
    v_few[:, :m] = v[:, :m]
    v_few[:, m + 4 : m + 4 + few] = v[:, m : m + few]
    both = rate_x[:, None] + rate_y[None, :]
    ends = np.zeros((4, 16, m))
    ends[0, :few], ends[1, :few] = tu[1][m : m + few], tu[2][m : m + few]
    ends[2, 4 : 4 + few], ends[3, 4 : 4 + few] = tv[1][m : m + few], tv[2][m : m + few]
    corner = np.zeros((m, lanes))
    corner[:, m + 4 : m + 4 + few] = 2.0 * tv[1][m : m + few].T
    a = [rp[0].T @ t for t in rp]
    b = [cp[0].T @ t for t in cp]
    even_x, odd_x = (rp[0].T @ basis(nx, m, RATIO, f) for f in (np.cos, np.sin))
    even_y, odd_y = ((cp[0].T @ basis(ny, m, RATIO, f)).T for f in (np.cos, np.sin))
    small = np.stack(
        [even_x, odd_x, even_y, odd_y, a[1], a[2], a[1] @ a[1], b[1], b[2], b[1] @ b[1],
         both, both**2, np.tile(2.0 * rate_y[None, :], (m, 1)), np.tile(2.0 * rate_x[:, None], (1, m)),
         both**3, np.tile(3.0 * rate_x[:, None] ** 2, (1, m))]
    ).astype(np.float32)
    deep = (W + 1) * m
    tables = [
        halves(u_few),
        halves(np.swapaxes(u[:, :tall].reshape(PX, cx, tall), 1, 2)),
        halves(v),
        halves(v_few.T),
        halves(np.concatenate([t[m:tall].T for t in tu[1:]], 1)),
        halves(np.concatenate(tv[1:3] + [t[m : m + 16] for t in tv[1:]], 0)),
        halves(np.concatenate([np.pad(ends.reshape(64, m), ((0, 0), (0, m))), corner], 0)),
    ]
    any_space = pl.BlockSpec(memory_space=pl.ANY)
    vmem = pl.BlockSpec(memory_space=pltpu.VMEM)
    dma = pltpu.SemaphoreType.DMA
    coeffs = pltpu.VMEM((W, m // 2, lanes), F32)
    thin = m // 2 + 16
    held = pl.pallas_call(
        functools.partial(kernel, dims, owners),
        out_shape=(
            pltpu.VMEM((L, cx, cy), F32),
            pltpu.VMEM((L, m // 2, lanes), F32),
        ),
        in_specs=[any_space] * 12,
        out_specs=(any_space, any_space),
        scratch_shapes=[
            pltpu.VMEM((L, cx, cy), F32),
            pltpu.VMEM((L, thin, lanes), F32),
            pltpu.VMEM((2 * G, thin, lanes), F32),
            pltpu.VMEM((cx * L // 16, 128), F32),
            pltpu.VMEM((2, cx * L // 16, 128), F32),
            pltpu.VMEM((L, cx + 16, cy + 128), F32),
            pltpu.VMEM((L, cx, cy), F32),
            pltpu.VMEM((L, cx, cy), F32),
            pltpu.VMEM((L, m // 2 + 8, lanes), F32),
            pltpu.VMEM((2 * G - 1, m + 8, lanes), F32),
            pltpu.VMEM((2, cx, tall), BF16),
            pltpu.VMEM((2, tall, cy), BF16),
            pltpu.VMEM((2, m // 2 + 8, lanes), F32),
            pltpu.VMEM((2, m // 2, lanes), F32),
            pltpu.VMEM((W, m, m), F32),
            coeffs,
            coeffs,
            pltpu.VMEM((8, 128), F32),
            pltpu.VMEM((8, 128), F32),
            pltpu.VMEM((5, m, m), F32),
            pltpu.VMEM((2, tall, cx), BF16),
            pltpu.VMEM((2, cy, lanes), BF16),
            pltpu.VMEM((2, m, 16 * W), BF16),
            pltpu.VMEM((2, 4 * m + 16 * W, m), BF16),
            pltpu.VMEM((2, 64 + m, lanes), BF16),
            pltpu.VMEM((16, m, m), F32),
            pltpu.SMEM(relax_rates.shape, F32),
            pltpu.SMEM(nest_offsets.shape[::-1], jnp.int32),
            dma((12,)),
            dma,
            dma,
            dma((4,)),
            dma((4,)),
            dma((2,)),
            dma((2,)),
            dma,
            dma,
            dma((2,)),
            dma,
        ],
        compiler_params=pltpu.CompilerParams(collective_id=0, has_side_effects=True),
    )(initial_state, drive_modes, relax_rates, nest_offsets.T,
      *(jnp.asarray(t) for t in tables), jnp.asarray(small))
    return pl.pallas_call(
        store,
        out_shape=[
            jax.ShapeDtypeStruct((1, L, cx, cy), F32),
            jax.ShapeDtypeStruct((1, L, m, m), F32),
        ],
        in_specs=[any_space, vmem],
        out_specs=[any_space] * 2,
        scratch_shapes=[pltpu.VMEM((L, m, m), F32), dma((2,))],
    )(*(pltpu.with_memory_space_constraint(x, pltpu.VMEM) for x in held))


def solution(mesh):
    nests, PY, PX = (mesh.shape[n] for n in ("nest", "py", "px"))
    spec = P("nest", None, "px", "py")

    def local(initial_state, drive_modes, relax_rates, nest_offsets):
        _, L, cx, cy = initial_state.shape
        W, _, m, _ = drive_modes.shape
        places = sorted(
            range(PY * PX),
            key=lambda g: (abs(2 * (g // PY) - PX + 1) + abs(2 * (g % PY) - PY + 1), g),
        )
        dims = (nests, PY, PX, L, cx, cy, m, W)
        return body(dims, tuple(places[:L]), initial_state, drive_modes, relax_rates, nest_offsets)

    return jax.shard_map(
        local,
        mesh=mesh,
        in_specs=(spec, P(), P("nest", None), P()),
        out_specs=(spec, P("nest", None, None, None)),
        check_vma=False,
    )
```

```python
import functools
import math

import jax
import jax.numpy as jnp
import numpy as np
from jax import lax
from jax.experimental import pallas as pl
from jax.experimental.pallas import tpu as pltpu
from jax.sharding import PartitionSpec as P

RATIO = 3
RATE = 0.2
MESH = pl.DeviceIdType.MESH
F32, BF16 = jnp.float32, jnp.bfloat16


def basis(cells, modes, refine, fn=np.cos):
    j = np.arange(modes, dtype=np.int64)
    q = 2 * np.arange(cells, dtype=np.int64) + 1
    product = (j[None, :] * q[:, None]) % (4 * refine * cells)
    weight = np.where(j == 0, 1.0, 2.0) / cells
    return np.sqrt(weight)[None, :] * fn(np.pi * product / (2.0 * refine * cells))


def half_step(table):
    pad = np.pad(table, ((1, 1), (0, 0)))
    return (0.5 - 2 * RATE) * table + RATE * (pad[2:] + pad[:-2])


def powers(table, count):
    out = [table]
    for _ in range(count):
        out.append(half_step(out[-1]))
    return out


def halves(table):
    high = np.asarray(table, np.float32).astype(BF16)
    low = (np.asarray(table, np.float64) - high.astype(np.float64)).astype(np.float32)
    return np.stack([high, low.astype(BF16)])


def split(x):
    high = x.astype(BF16)
    return high, (x - high.astype(F32)).astype(BF16)


def mm(a, b):
    return lax.dot_general(a, b, (((1,), (0,)), ((), ())), preferred_element_type=F32)


def dot3(a, b):
    a = a if isinstance(a, tuple) else split(a)
    b = b if isinstance(b, tuple) else split(b)
    return mm(a[0], b[0]) + (mm(a[0], b[1]) + mm(a[1], b[0]))


def dot3t(a, b):
    b = b if isinstance(b, tuple) else split(b)

    def nt(x, y):
        return lax.dot_general(x, y, (((1,), (1,)), ((), ())), preferred_element_type=F32)

    return nt(a[0], b[0]) + (nt(a[0], b[1]) + nt(a[1], b[0]))


def tri(a):
    return jnp.concatenate([a[0], a[0], a[1]], 1)


def dotk(a, b):
    b = b if isinstance(b, tuple) else split(b)
    return mm(a, jnp.concatenate([b[0], b[1], b[0]], 0))


def stack(*parts):
    if isinstance(parts[0], tuple):
        return tuple(jnp.concatenate(p, 0) for p in zip(*parts))
    return jnp.concatenate(parts, 0)


def pack(x):
    h = x.shape[0] // 2
    return jnp.concatenate([x[:h], x[h:]], 1)


def unpack(x):
    h = x.shape[1] // 2
    return jnp.concatenate([x[:, :h], x[:, h:]], 0)


def pack_wide(x, m):
    low = x[:m].T[m : m + 8]
    return jnp.concatenate(
        [pack(x[:m, :m]), x[m : m + 8], jnp.concatenate([low, jnp.zeros_like(low)], 1)], 0
    )


def unpack_fix(x, m):
    tile = x[m // 2 :]
    low = jnp.concatenate([tile[:, :m], jnp.zeros((m - 8, m), F32)], 0).T
    top = jnp.concatenate([unpack(x[: m // 2]), low], 1)
    return jnp.concatenate([top, tile, jnp.zeros((8, 2 * m), F32)], 0)[:, : m + 16]


def unpack_wide(x, m):
    low = jnp.concatenate([x[m // 2 + 8 :, :m], jnp.zeros((m - 8, m), F32)], 0).T
    top = jnp.concatenate([unpack(x[: m // 2]), low], 1)
    return jnp.concatenate([top, x[m // 2 : m // 2 + 8], jnp.zeros((8, 2 * m), F32)], 0)


def loop(n, fn):
    if n <= 16:
        for i in range(n):
            fn(i)
    else:
        lax.fori_loop(0, n, lambda i, c: (fn(i), c)[1], 0)


def kernel(
    dims, owners,
    field, drive, relax_hbm, offs_hbm,
    u_hbm, ut_hbm, v_hbm, vt_hbm, left_hbm, right_hbm, up_hbm, small_hbm,
    out, modes,
    fvm, pbuf, abuf, strip, near, wide, calm, state, fix, tally, u_t, vt_t, zbuf, mail, start, par, cbuf, lead, glead, tx,
    ut_t, v_t, left, right, up, small, relax, offs,
    load_sem, a_send, a_recv, h_send, h_recv, c_sem, g_sem, out_sem, b_send, f_recv, m_recv,
):
    nests, PY, PX, L, cx, cy, m, W = dims
    G, nx, ny = PY * PX, cx * PX, cy * PY
    k, py, px = lax.axis_index("nest"), lax.axis_index("py"), lax.axis_index("px")
    me = px * PY + py
    odd = k % 2 == 1
    leader = k + 1 - k % 2
    placed = [me == o for o in owners]
    level = sum(jnp.where(c, l, 0) for l, c in enumerate(placed))
    in_place = functools.reduce(jnp.logical_or, placed)
    is_owner = jnp.logical_and(odd, in_place)
    is_spare = jnp.logical_and(jnp.logical_not(odd), in_place)
    owns = [jnp.logical_and(odd, c) for c in placed]

    def at(g, nest):
        return (nest, g % PY, g // PY)

    def plain(g):
        return functools.reduce(jnp.logical_and, [g != o for o in owners])

    hops = [(-2, k > 2), (2, k < nests - 2)]
    sides = [
        (px > 0, (k, py, px - 1)), (px < PX - 1, (k, py, px + 1)),
        (py > 0, (k, py - 1, px)), (py < PY - 1, (k, py + 1, px)),
    ]
    beside = sum(jnp.where(c, 1, 0) for c, _ in sides)
    barrier = pltpu.get_barrier_semaphore()

    @pl.when(is_owner)
    def _():
        def greet(g):
            pl.semaphore_signal(barrier, inc=1, device_id=at(g, k - 1), device_id_type=MESH)

            @pl.when(plain(g))
            def _():
                pl.semaphore_signal(barrier, inc=1, device_id=at(g, k), device_id_type=MESH)
        loop(G, greet)

    load = pltpu.make_async_copy(field.at[0], fvm, load_sem.at[0])
    load.start()
    rows_here = pl.ds(pl.multiple_of(px * cx, 8), cx)
    cols_here = pl.ds(pl.multiple_of(py * cy, 128), cy)
    pairs = [
        (v_hbm.at[:, cols_here], v_t), (ut_hbm.at[px], ut_t),
        (u_hbm.at[:, rows_here], u_t), (vt_hbm.at[:, :, cols_here], vt_t),
        (relax_hbm, relax), (offs_hbm, offs), (small_hbm, small),
        (left_hbm, left), (right_hbm, right), (up_hbm, up),
    ]
    tables = [
        pltpu.make_async_copy(src, dst, load_sem.at[2 + i]) for i, (src, dst) in enumerate(pairs)
    ]
    for c in tables[:4]:
        c.start()
    for l, o in enumerate(owners):
        @pl.when(jnp.logical_not(owns[l]))
        def _():
            pl.semaphore_signal(barrier, inc=1, device_id=at(o, leader), device_id_type=MESH)

    for cond, device in sides:
        @pl.when(cond)
        def _():
            pl.semaphore_signal(barrier, inc=1, device_id=device, device_id_type=MESH)

    @pl.when(is_owner)
    def _():
        for hop, cond in hops:
            @pl.when(cond)
            def _():
                pl.semaphore_signal(
                    barrier, inc=1, device_id=(k + hop, py, px), device_id_type=MESH
                )

    def hop_copy(src, dst, send_sem, recv_sem, hop):
        return pltpu.make_async_remote_copy(
            src_ref=src, dst_ref=dst, send_sem=send_sem, recv_sem=recv_sem,
            device_id=(k + hop, py, px), device_id_type=MESH,
        )

    gain_out = hop_copy(lead, glead, g_sem.at[0], g_sem.at[1], 1)
    gain_in = hop_copy(lead, glead, g_sem.at[0], g_sem.at[1], -1)
    chain_out = hop_copy(cbuf, par, c_sem.at[0], c_sem.at[1], 2)
    chain_in = hop_copy(cbuf, par, c_sem.at[0], c_sem.at[1], -2)

    get_drive = pltpu.make_async_copy(drive.at[:, level], start, load_sem.at[1])

    @pl.when(in_place)
    def _():
        tables[4].start()

    @pl.when(is_owner)
    def _():
        for c in tables[5:]:
            c.start()

        @pl.when(k < 2)
        def _():
            get_drive.start()

    tables[0].wait()
    tables[1].wait()
    load.wait()
    half = dot3(fvm[...].reshape(L * cx, cy), (v_t[0], v_t[1]))
    for l in range(L):
        pbuf[l] = pack_wide(dotk(ut_t[...], half[l * cx : (l + 1) * cx]), m)

    @pl.when(is_owner)
    def _():
        abuf[G + me] = pbuf[level]
        pl.semaphore_wait(barrier, beside + 2 * G - 1 + sum(jnp.where(c, 1, 0) for _, c in hops))

    @pl.when(jnp.logical_not(is_owner))
    def _():
        pl.semaphore_wait(barrier, beside + L)

    def remote(src, dst, send_sem, recv_sem, g, nest):
        return pltpu.make_async_remote_copy(
            src_ref=src, dst_ref=dst, send_sem=send_sem, recv_sem=recv_sem,
            device_id=at(g, nest), device_id_type=MESH,
        )

    def share(l):
        return remote(
            pbuf.at[l], abuf.at[(k % 2) * G + me], a_send, a_recv, owners[l], leader
        )

    def settled(ref, sem):
        pltpu.make_async_copy(ref, ref, sem).wait()

    part = jnp.where(level < L // 2, 0, 1)
    keep_modes = pltpu.make_async_copy(mail.at[1], modes.at[level], m_recv)
    keep_fix = pltpu.make_async_copy(zbuf.at[1], fix.at[level], f_recv.at[part])

    def beam(src, dst, i, device):
        return pltpu.make_async_remote_copy(
            src_ref=src, dst_ref=dst, send_sem=h_send.at[i], recv_sem=h_recv.at[i],
            device_id=device, device_id_type=MESH,
        )

    top, bottom = pl.ds(0, 8), pl.ds(cx + 8, 8)
    first_rows, last_rows = pl.ds(8, 8), pl.ds(cx, 8)
    halo = [
        beam(wide.at[:, first_rows], wide.at[:, bottom], 0, sides[0][1]),
        beam(wide.at[:, last_rows], wide.at[:, top], 1, sides[1][1]),
        beam(strip, near.at[1], 2, sides[2][1]),
        beam(strip, near.at[0], 3, sides[3][1]),
    ]

    def start_halo(i):
        @pl.when(sides[i][0])
        def _():
            halo[i].start()

    def land_halo(i):
        @pl.when(sides[i ^ 1][0])
        def _():
            halo[i].wait_recv()

    for l, o in enumerate(owners):
        @pl.when(jnp.logical_not(owns[l]))
        def _():
            share(l).start()

    @pl.when(is_spare)
    def _():
        tables[4].wait()
        lead[...] = jnp.full(lead.shape, relax[0, level], F32)
        gain_out.start()

    lane = lax.broadcasted_iota(jnp.int32, (cx, 128), 1)
    edge = jnp.zeros((cx, 128), F32)
    for l in range(L):
        ends = jnp.where(lane < 64, fvm[l, :, 0:128], fvm[l, :, cy - 128 : cy])
        turned = pltpu.roll(ends, 8 * l, 1) if l else ends
        shift = (lane - 8 * l + 4) % 128
        edge = jnp.where(shift < 8, turned, edge)
        wide[l, 8 : cx + 8, 0:cy] = fvm[l]
    folds = 128 // (8 * L)
    thin = cx // folds
    short = lax.broadcasted_iota(jnp.int32, (thin, 128), 1)
    folded = edge[:thin]
    for i in range(1, folds):
        moved = pltpu.roll(edge[i * thin : (i + 1) * thin], 8 * L * i, 1)
        folded = jnp.where((short + 4) % 128 < 8 * L * i, folded, moved)
    strip[...] = folded
    bare = jnp.zeros((8, cy + 128), F32)

    @pl.when(px == 0)
    def _():
        for l in range(L):
            wide[l, 0:8, :] = bare

    @pl.when(px == PX - 1)
    def _():
        for l in range(L):
            wide[l, cx + 8 : cx + 16, :] = bare

    @pl.when(py == 0)
    def _():
        near[0] = jnp.zeros(near.shape[1:], F32)

    @pl.when(py == PY - 1)
    def _():
        near[1] = jnp.zeros(near.shape[1:], F32)

    start_halo(2)
    start_halo(3)

    def widen_patch():
        land_halo(2)
        land_halo(3)
        after, before = near[1], near[0]
        for l in range(L):
            for i in range(folds):
                back = (128 - 8 * l - 8 * L * i) % 128
                right, left_side = after, before
                if back:
                    right, left_side = pltpu.roll(after, back, 1), pltpu.roll(before, back, 1)
                wide[l, 8 + i * thin : 8 + (i + 1) * thin, cy:] = jnp.where(
                    short < 64, right, left_side
                )
        start_halo(0)
        start_halo(1)

    def run_free():
        land_halo(0)
        land_halo(1)
        shape = (cx + 16, cy + 128)
        row = lax.broadcasted_iota(jnp.int32, shape, 0) + (px * cx - 8)
        col = lax.broadcasted_iota(jnp.int32, shape, 1)
        col = jnp.where(col < cy + 64, col, col - (cy + 128)) + py * cy
        inside = (row >= 0) & (row < nx) & (col >= 0) & (col < ny)
        for l in range(L):
            now = wide[l]
            for _ in range(W):
                side = pltpu.roll(now, 1, 0) + pltpu.roll(now, cx + 15, 0)
                side = side + pltpu.roll(now, 1, 1) + pltpu.roll(now, cy + 127, 1)
                now = jnp.where(inside, now + RATE * (side - 4.0 * now), 0.0)
            calm[l] = now[8 : cx + 8, 0:cy]

    @pl.when(is_owner)
    def _():
        tables[4].wait()
        tables[5].wait()
        tables[6].wait()
        gain = relax[0, level]

        def turn(kk, cells, dim, axis):
            number = lax.broadcasted_iota(jnp.int32, (m, m), dim).astype(F32)
            product = number * (2 * RATIO * offs[axis, kk]).astype(F32)
            period = float(4 * RATIO * cells)
            product = product - period * jnp.floor(product * (1.0 / period))
            angle = product * (math.pi / (2.0 * RATIO * cells))
            return jnp.cos(angle), jnp.sin(angle)

        def flat(kk):
            eye = jnp.where(
                lax.broadcasted_iota(jnp.int32, (m, m), 0)
                == lax.broadcasted_iota(jnp.int32, (m, m), 1),
                1.0, 0.0,
            ).astype(F32)
            cos_x, sin_x = turn(kk, nx, 1, 0)
            cos_y, sin_y = turn(kk, ny, 0, 1)
            row = jnp.where(kk == 0, eye, small[0] * cos_x - small[1] * sin_x)
            col = jnp.where(kk == 0, eye, small[2] * cos_y - small[3] * sin_y)
            return split(row), split(col)

        a1, b1 = split(small[4]), split(small[7])

        def curved(rate):
            return split(small[5] - rate * small[6]), split(small[8] - rate * small[9])

        def maps(kk, rate):
            a2, b2 = curved(rate)
            f0, g0 = flat(kk)
            f1, f2 = split(dot3(a1, f0)), split(dot3(a2, f0))
            f01 = tuple(jnp.concatenate(p, 1) for p in zip(f0, f1))
            g1, g2 = split(dot3(g0, b1)), split(dot3(g0, b2))
            return tri(f0), tri(stack(f0, f1, f2)), tri(f01), g0, g1, g2, 2.0 * (1.0 - rate)

        def follow(cs, ms):
            f0, f012, f01, g0, g1, g2, rest = ms
            c1, c2, c3 = (split(c) for c in cs)
            y0 = dot3(stack(c1, c2, c3), g0)
            y1 = dot3(stack(c1, c2), g1)
            y12 = dot3(c1, g2)
            y10, y20, y30 = y0[:m], y0[m : 2 * m], y0[2 * m :]
            y11, y21 = y1[:m], y1[m:]
            z = dotk(f012, y10)
            return (
                z[:m],
                dotk(f0, y20),
                dotk(f0, y30),
                z[m : 2 * m] + dotk(f0, y11),
                z[2 * m :] + dotk(f01, stack(y21 + y12, y20 + rest * y11)),
            )

        def nudge(own, moved, rate):
            own2, own3 = own[1] + rate * moved[3], own[2] + rate * moved[4]
            d1, d2, d3 = rate * (moved[0] - own[0]), rate * (moved[1] - own2), rate * (moved[2] - own3)
            return (d1, d2, d3), (own[0] + d1, own2 + d2, own3 + d3)

        own_maps = maps(k, gain)
        gain_in.wait_recv()
        lead_gain = glead[0:1, 0:m]
        lead_maps = maps(k - 1, lead_gain)

        def both_sides(rate):
            a2, b2 = curved(rate)
            return tri(a1), tri(stack(a1, a2)), b2

        sides_lead, sides_own = both_sides(lead_gain), both_sides(gain)

        def first(cs):
            for i, x in enumerate(follow(cs, lead_maps)):
                tx[i] = x

        @pl.when(k < 2)
        def _():
            get_drive.wait()
            first([start[w] for w in range(W)])

        tables[7].wait()
        tables[8].wait()

        grown = [tri((left[0, :, : 16 * i], left[1, :, : 16 * i])) for i in (1, 2, 3)]
        tables[9].wait()
        ends = [tri((up[0, 16 * i : 16 * i + 16, :m], up[1, 16 * i : 16 * i + 16, :m])) for i in (0, 1)]
        settled(abuf.at[pl.ds(0, 2 * G - 1)], a_recv)

        def gathered(i):
            total = abuf[i * G]
            if G <= 16:
                for g in range(1, G):
                    total = total + abuf[i * G + g]
            else:
                total = lax.fori_loop(1, G, lambda g, c: c + abuf[i * G + g], total)
            return total

        def table(start, size):
            return right[0, start : start + size], right[1, start : start + size]

        def rows(*parts):
            return dotk(grown[len(parts) - 1], jnp.concatenate(parts, 0))

        totals = [gathered(i) for i in range(2)]
        lows, edges = [], []
        for t in totals:
            low = t[m // 2 + 8 :, :m]
            lows.append(jnp.concatenate([low, jnp.zeros((m - 8, m), F32)], 0).T[:, :16])
            edges.append(t[m // 2 : m // 2 + 8])
        lows, edges_s = split(stack(*lows)), split(stack(*edges))
        row1, row2 = (dot3(edges_s, table(2 * m * j, 2 * m)) for j in range(2))
        q1, q2, q3 = (dot3(lows, table(4 * m + 16 * j, 16)) for j in range(3))

        def project(i):
            main = unpack(totals[i][: m // 2])
            none = jnp.zeros((8, m), F32)
            r0 = stack(edges[i][:, :m], none)
            r1, r2 = (stack(r[8 * i : 8 * i + 8], none) for r in (row1, row2))
            p1, p2, p3 = (q[i * m : (i + 1) * m] for q in (q1, q2, q3))
            return [
                small[10] * main + (rows(r0) + p1),
                small[11] * main + (rows(2.0 * r1, r0) + small[13] * p1 + p2),
                small[14] * main
                + (rows(3.0 * r2, 3.0 * r1, r0) + small[15] * p1 + 1.5 * small[13] * p2 + p3),
            ]

        def settle(s, rate, sides):
            s1, s2, s3 = s
            a1, a12, b2 = sides
            s1s, s2s = split(s1), split(s2)
            by_b = dot3(stack(s1s, s2s), b1)
            by_a = dotk(a12, s1s)
            x2 = by_a[:m] + by_b[:m]
            x3 = by_b[m:] + dot3(s1s, b2) + by_a[m:]
            x3 = x3 + dotk(a1, s2 + 2.0 * (1.0 - rate) * by_b[:m])
            return s1, s2 - rate * x2, s3 - rate * x3

        before, after = project(0), project(1)
        before, after = settle(before, lead_gain, sides_lead), settle(after, gain, sides_own)

        @pl.when(k > 1)
        def _():
            widen_patch()
            chain_in.wait_recv()
            first([unpack(par[w]) for w in range(W)])

        d_lead, c_lead = nudge(before, [tx[i] for i in range(5)], lead_gain)
        def widen(x):
            return jnp.concatenate([x, jnp.zeros_like(x)], 1)

        def table(i):
            return up[0, 16 * i : 16 * (i + 1), :m], up[1, 16 * i : 16 * (i + 1), :m]

        def correct(d):
            d1, d2, d3 = d
            e1 = split(d1)
            main = d3 + small[10] * d2 + small[11] * d1
            rows = dotk(ends[0], d2 + small[12] * d1) + dotk(ends[1], e1)
            cols = dot3t(table(2), d2 + small[13] * d1) + dot3t(table(3), e1)
            corner = dot3(dotk(ends[0], e1), (up[0, 64:], up[1, 64:]))
            return jnp.concatenate([pack(main), (widen(rows + cols) + corner)[:8]], 0)

        def mend(i, g):
            return remote(
                zbuf.at[i], fix.at[level], b_send, f_recv.at[part], g, k - 1 + i
            )

        def tell(i, g):
            return remote(
                mail.at[i], modes.at[level], b_send, m_recv, g, k - 1 + i
            )

        def give(copy, i):
            def one(j):
                g = jnp.where(2 * px < PX, G - 1 - j, j)
                if i == 0:
                    copy(i, g).start()
                else:
                    @pl.when(g != me)
                    def _():
                        copy(i, g).start()
            loop(G, one)

        def advance():
            mail[0] = pack(c_lead[W - 1])
            give(tell, 0)
            zbuf[0] = correct(d_lead)
            give(mend, 0)

        @pl.when(k >= nests - 2)
        def _():
            advance()

        d_own, c_own = nudge(after, follow(c_lead, own_maps), gain)
        for w in range(W):
            cbuf[w] = pack(c_own[w])

        @pl.when(k < nests - 2)
        def _():
            chain_out.start()

        @pl.when(k < 2)
        def _():
            widen_patch()

        @pl.when(k < nests - 2)
        def _():
            advance()

        zbuf[1] = correct(d_own)
        give(mend, 1)
        mail[1] = pack(c_own[W - 1])
        give(tell, 1)
        keep_fix.start()
        keep_modes.start()
        run_free()

    @pl.when(jnp.logical_not(is_owner))
    def _():
        widen_patch()
        run_free()

    tables[2].wait()
    tables[3].wait()

    u_wide = tri((u_t[0], u_t[1]))
    most = L // 2
    far = jnp.where(2 * px < PX, 0, 1)
    for i in range(2):
        turn = (i + far) % 2
        first = turn * most
        some = pl.ds(first, most)
        settled(fix.at[some], f_recv.at[turn])
        half = [dot3(unpack_fix(fix[first + j], m), (vt_t[0], vt_t[1])) for j in range(most)]
        done = [calm[first + j] + dotk(u_wide, half[j]) for j in range(most)]
        for j in range(most):
            state[first + j] = done[j]
        pltpu.make_async_copy(state.at[some], out.at[some], out_sem).start()
    settled(modes, m_recv)

    @pl.when(jnp.logical_not(is_owner))
    def _():
        settled(pbuf, a_send)

    @pl.when(is_owner)
    def _():
        settled(pbuf.at[pl.ds(0, L - 1)], a_send)
        settled(tally, b_send)

        @pl.when(k < nests - 2)
        def _():
            chain_out.wait_send()

    @pl.when(is_spare)
    def _():
        gain_out.wait_send()

    for i in range(4):
        @pl.when(sides[i][0])
        def _():
            halo[i].wait_send()
    settled(state, out_sem)


def store(state, packed, state_out, modes_out, modes, sem):
    first = pltpu.make_async_copy(state, state_out.at[0], sem.at[0])
    second = pltpu.make_async_copy(modes, modes_out.at[0], sem.at[1])
    first.start()
    for l in range(packed.shape[0]):
        modes[l] = unpack(packed[l])
    second.start()
    first.wait()
    second.wait()


def wide_tables(cells, modes, windows):
    stages = powers(basis(cells, modes, 1), windows)
    edges = np.zeros((cells, modes))
    for e in range(windows):
        edges[e, 2 * e] = 1.0
        edges[cells - 1 - e, 2 * e + 1] = 1.0
    full = np.concatenate([stages[0], edges], 1)
    rate = 0.5 - 2 * RATE + 2 * RATE * np.cos(np.pi * np.arange(modes) / cells)
    turns = []
    for i, t in enumerate(stages):
        top = np.diag(rate**i)
        turns.append(np.concatenate([top, edges.T @ (t - stages[0] @ top)], 0))
    return stages, full, turns, rate


def body(dims, owners, initial_state, drive_modes, relax_rates, nest_offsets):
    nests, PY, PX, L, cx, cy, m, W = dims
    G, nx, ny = PY * PX, cx * PX, cy * PY
    assert nests % 2 == 0 and L % 2 == 0 and W == 3
    tall, lanes = m + 16, 2 * m
    rp, u, tu, rate_x = wide_tables(nx, m, W)
    cp, v, tv, rate_y = wide_tables(ny, m, W)
    few = 2 * (W - 1)
    u_few, v_few = u[:, :tall].copy(), np.zeros((ny, tall))
    u_few[:, m + few :] = 0.0
    v_few[:, :m] = v[:, :m]
    v_few[:, m + 4 : m + 4 + few] = v[:, m : m + few]
    both = rate_x[:, None] + rate_y[None, :]
    ends = np.zeros((4, 16, m))
    ends[0, :few], ends[1, :few] = tu[1][m : m + few], tu[2][m : m + few]
    ends[2, 4 : 4 + few], ends[3, 4 : 4 + few] = tv[1][m : m + few], tv[2][m : m + few]
    corner = np.zeros((m, lanes))
    corner[:, m + 4 : m + 4 + few] = 2.0 * tv[1][m : m + few].T
    a = [rp[0].T @ t for t in rp]
    b = [cp[0].T @ t for t in cp]
    even_x, odd_x = (rp[0].T @ basis(nx, m, RATIO, f) for f in (np.cos, np.sin))
    even_y, odd_y = ((cp[0].T @ basis(ny, m, RATIO, f)).T for f in (np.cos, np.sin))
    small = np.stack(
        [even_x, odd_x, even_y, odd_y, a[1], a[2], a[1] @ a[1], b[1], b[2], b[1] @ b[1],
         both, both**2, np.tile(2.0 * rate_y[None, :], (m, 1)), np.tile(2.0 * rate_x[:, None], (1, m)),
         both**3, np.tile(3.0 * rate_x[:, None] ** 2, (1, m))]
    ).astype(np.float32)
    here = halves(np.swapaxes(u[:, :tall].reshape(PX, cx, tall), 1, 2))
    tables = [
        halves(u_few),
        np.concatenate([here[0], here[0], here[1]], -1),
        halves(v),
        halves(v_few.T),
        halves(np.concatenate([t[m:tall].T for t in tu[1:]], 1)),
        halves(np.concatenate(tv[1:3] + [t[m : m + 16] for t in tv[1:]], 0)),
        halves(np.concatenate([np.pad(ends.reshape(64, m), ((0, 0), (0, m))), corner], 0)),
    ]
    any_space = pl.BlockSpec(memory_space=pl.ANY)
    vmem = pl.BlockSpec(memory_space=pltpu.VMEM)
    dma = pltpu.SemaphoreType.DMA
    coeffs = pltpu.VMEM((W, m // 2, lanes), F32)
    thin = m // 2 + 16
    held = pl.pallas_call(
        functools.partial(kernel, dims, owners),
        out_shape=(
            pltpu.VMEM((L, cx, cy), F32),
            pltpu.VMEM((L, m // 2, lanes), F32),
        ),
        in_specs=[any_space] * 12,
        out_specs=(any_space, any_space),
        scratch_shapes=[
            pltpu.VMEM((L, cx, cy), F32),
            pltpu.VMEM((L, thin, lanes), F32),
            pltpu.VMEM((2 * G, thin, lanes), F32),
            pltpu.VMEM((cx * L // 16, 128), F32),
            pltpu.VMEM((2, cx * L // 16, 128), F32),
            pltpu.VMEM((L, cx + 16, cy + 128), F32),
            pltpu.VMEM((L, cx, cy), F32),
            pltpu.VMEM((L, cx, cy), F32),
            pltpu.VMEM((L, m // 2 + 8, lanes), F32),
            pltpu.VMEM((2 * G - 1, m + 8, lanes), F32),
            pltpu.VMEM((2, cx, tall), BF16),
            pltpu.VMEM((2, tall, cy), BF16),
            pltpu.VMEM((2, m // 2 + 8, lanes), F32),
            pltpu.VMEM((2, m // 2, lanes), F32),
            pltpu.VMEM((W, m, m), F32),
            coeffs,
            coeffs,
            pltpu.VMEM((8, 128), F32),
            pltpu.VMEM((8, 128), F32),
            pltpu.VMEM((5, m, m), F32),
            pltpu.VMEM((tall, 3 * cx), BF16),
            pltpu.VMEM((2, cy, lanes), BF16),
            pltpu.VMEM((2, m, 16 * W), BF16),
            pltpu.VMEM((2, 4 * m + 16 * W, m), BF16),
            pltpu.VMEM((2, 64 + m, lanes), BF16),
            pltpu.VMEM((16, m, m), F32),
            pltpu.SMEM(relax_rates.shape, F32),
            pltpu.SMEM(nest_offsets.shape[::-1], jnp.int32),
            dma((12,)),
            dma,
            dma,
            dma((4,)),
            dma((4,)),
            dma((2,)),
            dma((2,)),
            dma,
            dma,
            dma((2,)),
            dma,
        ],
        compiler_params=pltpu.CompilerParams(collective_id=0, has_side_effects=True),
    )(initial_state, drive_modes, relax_rates, nest_offsets.T,
      *(jnp.asarray(t) for t in tables), jnp.asarray(small))
    return pl.pallas_call(
        store,
        out_shape=[
            jax.ShapeDtypeStruct((1, L, cx, cy), F32),
            jax.ShapeDtypeStruct((1, L, m, m), F32),
        ],
        in_specs=[any_space, vmem],
        out_specs=[any_space] * 2,
        scratch_shapes=[pltpu.VMEM((L, m, m), F32), dma((2,))],
    )(*(pltpu.with_memory_space_constraint(x, pltpu.VMEM) for x in held))


def solution(mesh):
    nests, PY, PX = (mesh.shape[n] for n in ("nest", "py", "px"))
    spec = P("nest", None, "px", "py")

    def local(initial_state, drive_modes, relax_rates, nest_offsets):
        _, L, cx, cy = initial_state.shape
        W, _, m, _ = drive_modes.shape
        places = sorted(
            range(PY * PX),
            key=lambda g: (abs(2 * (g // PY) - PX + 1) + abs(2 * (g % PY) - PY + 1), g),
        )
        dims = (nests, PY, PX, L, cx, cy, m, W)
        return body(dims, tuple(places[:L]), initial_state, drive_modes, relax_rates, nest_offsets)

    return jax.shard_map(
        local,
        mesh=mesh,
        in_specs=(spec, P(), P("nest", None), P()),
        out_specs=(spec, P("nest", None, None, None)),
        check_vma=False,
    )
```

```python
import functools
import math

import jax
import jax.numpy as jnp
import numpy as np
from jax import lax
from jax.experimental import pallas as pl
from jax.experimental.pallas import tpu as pltpu
from jax.sharding import PartitionSpec as P

RATIO = 3
RATE = 0.2
MESH = pl.DeviceIdType.MESH
F32, BF16 = jnp.float32, jnp.bfloat16


def basis(cells, modes, refine, fn=np.cos):
    j = np.arange(modes, dtype=np.int64)
    q = 2 * np.arange(cells, dtype=np.int64) + 1
    product = (j[None, :] * q[:, None]) % (4 * refine * cells)
    weight = np.where(j == 0, 1.0, 2.0) / cells
    return np.sqrt(weight)[None, :] * fn(np.pi * product / (2.0 * refine * cells))


def half_step(table):
    pad = np.pad(table, ((1, 1), (0, 0)))
    return (0.5 - 2 * RATE) * table + RATE * (pad[2:] + pad[:-2])


def powers(table, count):
    out = [table]
    for _ in range(count):
        out.append(half_step(out[-1]))
    return out


def halves(table):
    high = np.asarray(table, np.float32).astype(BF16)
    low = (np.asarray(table, np.float64) - high.astype(np.float64)).astype(np.float32)
    return np.stack([high, low.astype(BF16)])


def split(x):
    high = x.astype(BF16)
    return high, (x - high.astype(F32)).astype(BF16)


def mm(a, b):
    return lax.dot_general(a, b, (((1,), (0,)), ((), ())), preferred_element_type=F32)


def dot3(a, b):
    a = a if isinstance(a, tuple) else split(a)
    b = b if isinstance(b, tuple) else split(b)
    return mm(a[0], b[0]) + (mm(a[0], b[1]) + mm(a[1], b[0]))


def dot3t(a, b):
    b = b if isinstance(b, tuple) else split(b)

    def nt(x, y):
        return lax.dot_general(x, y, (((1,), (1,)), ((), ())), preferred_element_type=F32)

    return nt(a[0], b[0]) + (nt(a[0], b[1]) + nt(a[1], b[0]))


def tri(a):
    return jnp.concatenate([a[0], a[0], a[1]], 1)


def dotk(a, b):
    b = b if isinstance(b, tuple) else split(b)
    return mm(a, jnp.concatenate([b[0], b[1], b[0]], 0))


def stack(*parts):
    if isinstance(parts[0], tuple):
        return tuple(jnp.concatenate(p, 0) for p in zip(*parts))
    return jnp.concatenate(parts, 0)


def pack(x):
    h = x.shape[0] // 2
    return jnp.concatenate([x[:h], x[h:]], 1)


def unpack(x):
    h = x.shape[1] // 2
    return jnp.concatenate([x[:, :h], x[:, h:]], 0)


def pack_wide(x, m):
    low = x[:m].T[m : m + 8]
    return jnp.concatenate(
        [pack(x[:m, :m]), x[m : m + 8], jnp.concatenate([low, jnp.zeros_like(low)], 1)], 0
    )


def unpack_fix(x, m):
    tile = x[m // 2 :]
    low = jnp.concatenate([tile[:, :m], jnp.zeros((m - 8, m), F32)], 0).T
    top = jnp.concatenate([unpack(x[: m // 2]), low], 1)
    return jnp.concatenate([top, tile, jnp.zeros((8, 2 * m), F32)], 0)[:, : m + 16]


def unpack_wide(x, m):
    low = jnp.concatenate([x[m // 2 + 8 :, :m], jnp.zeros((m - 8, m), F32)], 0).T
    top = jnp.concatenate([unpack(x[: m // 2]), low], 1)
    return jnp.concatenate([top, x[m // 2 : m // 2 + 8], jnp.zeros((8, 2 * m), F32)], 0)


def loop(n, fn):
    if n <= 16:
        for i in range(n):
            fn(i)
    else:
        lax.fori_loop(0, n, lambda i, c: (fn(i), c)[1], 0)


def kernel(
    dims, owners,
    field, drive, relax_hbm, offs_hbm,
    u_hbm, ut_hbm, v_hbm, vt_hbm, left_hbm, right_hbm, up_hbm, small_hbm,
    out, modes,
    fvm, pbuf, abuf, strip, near, wide, calm, state, fix, tally, u_t, vt_t, zbuf, mail, start, par, cbuf, lead, glead, tx,
    ut_t, v_t, left, right, up, small, relax, offs,
    load_sem, a_send, a_recv, h_send, h_recv, c_sem, g_sem, out_sem, b_send, f_recv, m_recv,
):
    nests, PY, PX, L, cx, cy, m, W = dims
    G, nx, ny = PY * PX, cx * PX, cy * PY
    k, py, px = lax.axis_index("nest"), lax.axis_index("py"), lax.axis_index("px")
    me = px * PY + py
    odd = k % 2 == 1
    leader = k + 1 - k % 2
    placed = [me == o for o in owners]
    level = sum(jnp.where(c, l, 0) for l, c in enumerate(placed))
    in_place = functools.reduce(jnp.logical_or, placed)
    is_owner = jnp.logical_and(odd, in_place)
    is_spare = jnp.logical_and(jnp.logical_not(odd), in_place)
    owns = [jnp.logical_and(odd, c) for c in placed]

    def at(g, nest):
        return (nest, g % PY, g // PY)

    def plain(g):
        return functools.reduce(jnp.logical_and, [g != o for o in owners])

    hops = [(-2, k > 2), (2, k < nests - 2)]
    sides = [
        (px > 0, (k, py, px - 1)), (px < PX - 1, (k, py, px + 1)),
        (py > 0, (k, py - 1, px)), (py < PY - 1, (k, py + 1, px)),
    ]
    beside = sum(jnp.where(c, 1, 0) for c, _ in sides)
    barrier = pltpu.get_barrier_semaphore()

    @pl.when(is_owner)
    def _():
        def greet(g):
            pl.semaphore_signal(barrier, inc=1, device_id=at(g, k - 1), device_id_type=MESH)

            @pl.when(plain(g))
            def _():
                pl.semaphore_signal(barrier, inc=1, device_id=at(g, k), device_id_type=MESH)
        loop(G, greet)

    load = pltpu.make_async_copy(field.at[0], fvm, load_sem.at[0])
    load.start()
    rows_here = pl.ds(pl.multiple_of(px * cx, 8), cx)
    cols_here = pl.ds(pl.multiple_of(py * cy, 128), cy)
    pairs = [
        (v_hbm.at[:, cols_here], v_t), (ut_hbm.at[px], ut_t),
        (u_hbm.at[:, rows_here], u_t), (vt_hbm.at[:, :, cols_here], vt_t),
        (relax_hbm, relax), (offs_hbm, offs), (small_hbm, small),
        (left_hbm, left), (right_hbm, right), (up_hbm, up),
    ]
    tables = [
        pltpu.make_async_copy(src, dst, load_sem.at[2 + i]) for i, (src, dst) in enumerate(pairs)
    ]
    for c in tables[:4]:
        c.start()
    for l, o in enumerate(owners):
        @pl.when(jnp.logical_not(owns[l]))
        def _():
            pl.semaphore_signal(barrier, inc=1, device_id=at(o, leader), device_id_type=MESH)

    for cond, device in sides:
        @pl.when(cond)
        def _():
            pl.semaphore_signal(barrier, inc=1, device_id=device, device_id_type=MESH)

    @pl.when(is_owner)
    def _():
        for hop, cond in hops:
            @pl.when(cond)
            def _():
                pl.semaphore_signal(
                    barrier, inc=1, device_id=(k + hop, py, px), device_id_type=MESH
                )

    def hop_copy(src, dst, send_sem, recv_sem, hop):
        return pltpu.make_async_remote_copy(
            src_ref=src, dst_ref=dst, send_sem=send_sem, recv_sem=recv_sem,
            device_id=(k + hop, py, px), device_id_type=MESH,
        )

    gain_out = hop_copy(lead, glead, g_sem.at[0], g_sem.at[1], 1)
    gain_in = hop_copy(lead, glead, g_sem.at[0], g_sem.at[1], -1)
    chain_out = hop_copy(cbuf, par, c_sem.at[0], c_sem.at[1], 2)
    chain_in = hop_copy(cbuf, par, c_sem.at[0], c_sem.at[1], -2)

    get_drive = pltpu.make_async_copy(drive.at[:, level], start, load_sem.at[1])

    @pl.when(in_place)
    def _():
        tables[4].start()

    @pl.when(is_owner)
    def _():
        for c in tables[5:]:
            c.start()

        @pl.when(k < 2)
        def _():
            get_drive.start()

    tables[0].wait()
    tables[1].wait()
    load.wait()
    half = dot3(fvm[...].reshape(L * cx, cy), (v_t[0], v_t[1]))
    for l in range(L):
        pbuf[l] = pack_wide(dotk(ut_t[...], half[l * cx : (l + 1) * cx]), m)

    @pl.when(is_owner)
    def _():
        abuf[G + me] = pbuf[level]
        pl.semaphore_wait(barrier, beside + 2 * G - 1 + sum(jnp.where(c, 1, 0) for _, c in hops))

    @pl.when(jnp.logical_not(is_owner))
    def _():
        pl.semaphore_wait(barrier, beside + L)

    def remote(src, dst, send_sem, recv_sem, g, nest):
        return pltpu.make_async_remote_copy(
            src_ref=src, dst_ref=dst, send_sem=send_sem, recv_sem=recv_sem,
            device_id=at(g, nest), device_id_type=MESH,
        )

    def share(l):
        return remote(
            pbuf.at[l], abuf.at[(k % 2) * G + me], a_send, a_recv, owners[l], leader
        )

    def settled(ref, sem):
        pltpu.make_async_copy(ref, ref, sem).wait()

    part = jnp.where(level < L // 2, 0, 1)
    keep_modes = pltpu.make_async_copy(mail.at[1], modes.at[level], m_recv)
    keep_fix = pltpu.make_async_copy(zbuf.at[1], fix.at[level], f_recv.at[part])

    def beam(src, dst, i, device):
        return pltpu.make_async_remote_copy(
            src_ref=src, dst_ref=dst, send_sem=h_send.at[i // 2], recv_sem=h_recv.at[i // 2],
            device_id=device, device_id_type=MESH,
        )

    top, bottom = pl.ds(0, 8), pl.ds(cx + 8, 8)
    first_rows, last_rows = pl.ds(8, 8), pl.ds(cx, 8)
    halo = [
        beam(wide.at[:, first_rows], wide.at[:, bottom], 0, sides[0][1]),
        beam(wide.at[:, last_rows], wide.at[:, top], 1, sides[1][1]),
        beam(strip, near.at[1], 2, sides[2][1]),
        beam(strip, near.at[0], 3, sides[3][1]),
    ]

    def start_halo(i):
        @pl.when(sides[i][0])
        def _():
            halo[i].start()

    def settle_halo(i, sem):
        lower, upper = sides[2 * i][0], sides[2 * i + 1][0]
        two, one = (wide.at[:, pl.ds(0, 16)], wide.at[:, pl.ds(0, 8)]) if i == 0 else (near, near.at[0])

        @pl.when(jnp.logical_and(lower, upper))
        def _():
            settled(two, sem)

        @pl.when(lower != upper)
        def _():
            settled(one, sem)

    for l, o in enumerate(owners):
        @pl.when(jnp.logical_not(owns[l]))
        def _():
            share(l).start()

    @pl.when(is_spare)
    def _():
        tables[4].wait()
        lead[...] = jnp.full(lead.shape, relax[0, level], F32)
        gain_out.start()

    lane = lax.broadcasted_iota(jnp.int32, (cx, 128), 1)
    edge = jnp.zeros((cx, 128), F32)
    for l in range(L):
        ends = jnp.where(lane < 64, fvm[l, :, 0:128], fvm[l, :, cy - 128 : cy])
        turned = pltpu.roll(ends, 8 * l, 1) if l else ends
        shift = (lane - 8 * l + 4) % 128
        edge = jnp.where(shift < 8, turned, edge)
        wide[l, 8 : cx + 8, 0:cy] = fvm[l]
    folds = 128 // (8 * L)
    thin = cx // folds
    short = lax.broadcasted_iota(jnp.int32, (thin, 128), 1)
    folded = edge[:thin]
    for i in range(1, folds):
        moved = pltpu.roll(edge[i * thin : (i + 1) * thin], 8 * L * i, 1)
        folded = jnp.where((short + 4) % 128 < 8 * L * i, folded, moved)
    strip[...] = folded
    bare = jnp.zeros((8, cy + 128), F32)

    @pl.when(px == 0)
    def _():
        for l in range(L):
            wide[l, 0:8, :] = bare

    @pl.when(px == PX - 1)
    def _():
        for l in range(L):
            wide[l, cx + 8 : cx + 16, :] = bare

    @pl.when(py == 0)
    def _():
        near[0] = jnp.zeros(near.shape[1:], F32)

    @pl.when(py == PY - 1)
    def _():
        near[1] = jnp.zeros(near.shape[1:], F32)

    start_halo(2)
    start_halo(3)

    def widen_patch():
        settle_halo(1, h_recv.at[1])
        after, before = near[1], near[0]
        for l in range(L):
            for i in range(folds):
                back = (128 - 8 * l - 8 * L * i) % 128
                right, left_side = after, before
                if back:
                    right, left_side = pltpu.roll(after, back, 1), pltpu.roll(before, back, 1)
                wide[l, 8 + i * thin : 8 + (i + 1) * thin, cy:] = jnp.where(
                    short < 64, right, left_side
                )
        start_halo(0)
        start_halo(1)

    def run_free():
        settle_halo(0, h_recv.at[0])
        shape = (cx + 16, cy + 128)
        row = lax.broadcasted_iota(jnp.int32, shape, 0) + (px * cx - 8)
        col = lax.broadcasted_iota(jnp.int32, shape, 1)
        col = jnp.where(col < cy + 64, col, col - (cy + 128)) + py * cy
        inside = (row >= 0) & (row < nx) & (col >= 0) & (col < ny)
        for l in range(L):
            now = wide[l]
            for _ in range(W):
                side = pltpu.roll(now, 1, 0) + pltpu.roll(now, cx + 15, 0)
                side = side + pltpu.roll(now, 1, 1) + pltpu.roll(now, cy + 127, 1)
                now = jnp.where(inside, now + RATE * (side - 4.0 * now), 0.0)
            calm[l] = now[8 : cx + 8, 0:cy]

    @pl.when(is_owner)
    def _():
        tables[4].wait()
        tables[5].wait()
        tables[6].wait()
        gain = relax[0, level]

        def turn(kk, cells, dim, axis):
            number = lax.broadcasted_iota(jnp.int32, (m, m), dim).astype(F32)
            product = number * (2 * RATIO * offs[axis, kk]).astype(F32)
            period = float(4 * RATIO * cells)
            product = product - period * jnp.floor(product * (1.0 / period))
            angle = product * (math.pi / (2.0 * RATIO * cells))
            return jnp.cos(angle), jnp.sin(angle)

        def flat(kk):
            eye = jnp.where(
                lax.broadcasted_iota(jnp.int32, (m, m), 0)
                == lax.broadcasted_iota(jnp.int32, (m, m), 1),
                1.0, 0.0,
            ).astype(F32)
            cos_x, sin_x = turn(kk, nx, 1, 0)
            cos_y, sin_y = turn(kk, ny, 0, 1)
            row = jnp.where(kk == 0, eye, small[0] * cos_x - small[1] * sin_x)
            col = jnp.where(kk == 0, eye, small[2] * cos_y - small[3] * sin_y)
            return split(row), split(col)

        a1, b1 = split(small[4]), split(small[7])

        def curved(rate):
            return split(small[5] - rate * small[6]), split(small[8] - rate * small[9])

        def maps(kk, rate):
            a2, b2 = curved(rate)
            f0, g0 = flat(kk)
            f1, f2 = split(dot3(a1, f0)), split(dot3(a2, f0))
            f01 = tuple(jnp.concatenate(p, 1) for p in zip(f0, f1))
            g1, g2 = split(dot3(g0, b1)), split(dot3(g0, b2))
            return tri(f0), tri(stack(f0, f1, f2)), tri(f01), g0, g1, g2, 2.0 * (1.0 - rate)

        def follow(cs, ms):
            f0, f012, f01, g0, g1, g2, rest = ms
            c1, c2, c3 = (split(c) for c in cs)
            y0 = dot3(stack(c1, c2, c3), g0)
            y1 = dot3(stack(c1, c2), g1)
            y12 = dot3(c1, g2)
            y10, y20, y30 = y0[:m], y0[m : 2 * m], y0[2 * m :]
            y11, y21 = y1[:m], y1[m:]
            z = dotk(f012, y10)
            return (
                z[:m],
                dotk(f0, y20),
                dotk(f0, y30),
                z[m : 2 * m] + dotk(f0, y11),
                z[2 * m :] + dotk(f01, stack(y21 + y12, y20 + rest * y11)),
            )

        def nudge(own, moved, rate):
            own2, own3 = own[1] + rate * moved[3], own[2] + rate * moved[4]
            d1, d2, d3 = rate * (moved[0] - own[0]), rate * (moved[1] - own2), rate * (moved[2] - own3)
            return (d1, d2, d3), (own[0] + d1, own2 + d2, own3 + d3)

        own_maps = maps(k, gain)
        gain_in.wait_recv()
        lead_gain = glead[0:1, 0:m]
        lead_maps = maps(k - 1, lead_gain)

        def both_sides(rate):
            a2, b2 = curved(rate)
            return tri(a1), tri(stack(a1, a2)), b2

        sides_lead, sides_own = both_sides(lead_gain), both_sides(gain)

        def first(cs):
            for i, x in enumerate(follow(cs, lead_maps)):
                tx[i] = x

        @pl.when(k < 2)
        def _():
            get_drive.wait()
            first([start[w] for w in range(W)])

        tables[7].wait()
        tables[8].wait()

        grown = [tri((left[0, :, : 16 * i], left[1, :, : 16 * i])) for i in (1, 2, 3)]
        tables[9].wait()
        ends = [tri((up[0, 16 * i : 16 * i + 16, :m], up[1, 16 * i : 16 * i + 16, :m])) for i in (0, 1)]
        settled(abuf.at[pl.ds(0, 2 * G - 1)], a_recv)

        def gathered(i):
            total = abuf[i * G]
            if G <= 16:
                for g in range(1, G):
                    total = total + abuf[i * G + g]
            else:
                total = lax.fori_loop(1, G, lambda g, c: c + abuf[i * G + g], total)
            return total

        def table(start, size):
            return right[0, start : start + size], right[1, start : start + size]

        def rows(*parts):
            return dotk(grown[len(parts) - 1], jnp.concatenate(parts, 0))

        totals = [gathered(i) for i in range(2)]
        lows, edges = [], []
        for t in totals:
            low = t[m // 2 + 8 :, :m]
            lows.append(jnp.concatenate([low, jnp.zeros((m - 8, m), F32)], 0).T[:, :16])
            edges.append(t[m // 2 : m // 2 + 8])
        lows, edges_s = split(stack(*lows)), split(stack(*edges))
        row1, row2 = (dot3(edges_s, table(2 * m * j, 2 * m)) for j in range(2))
        q1, q2, q3 = (dot3(lows, table(4 * m + 16 * j, 16)) for j in range(3))

        def project(i):
            main = unpack(totals[i][: m // 2])
            none = jnp.zeros((8, m), F32)
            r0 = stack(edges[i][:, :m], none)
            r1, r2 = (stack(r[8 * i : 8 * i + 8], none) for r in (row1, row2))
            p1, p2, p3 = (q[i * m : (i + 1) * m] for q in (q1, q2, q3))
            return [
                small[10] * main + (rows(r0) + p1),
                small[11] * main + (rows(2.0 * r1, r0) + small[13] * p1 + p2),
                small[14] * main
                + (rows(3.0 * r2, 3.0 * r1, r0) + small[15] * p1 + 1.5 * small[13] * p2 + p3),
            ]

        def settle(s, rate, sides):
            s1, s2, s3 = s
            a1, a12, b2 = sides
            s1s, s2s = split(s1), split(s2)
            by_b = dot3(stack(s1s, s2s), b1)
            by_a = dotk(a12, s1s)
            x2 = by_a[:m] + by_b[:m]
            x3 = by_b[m:] + dot3(s1s, b2) + by_a[m:]
            x3 = x3 + dotk(a1, s2 + 2.0 * (1.0 - rate) * by_b[:m])
            return s1, s2 - rate * x2, s3 - rate * x3

        before, after = project(0), project(1)
        before, after = settle(before, lead_gain, sides_lead), settle(after, gain, sides_own)

        @pl.when(k > 1)
        def _():
            widen_patch()
            chain_in.wait_recv()
            first([unpack(par[w]) for w in range(W)])

        d_lead, c_lead = nudge(before, [tx[i] for i in range(5)], lead_gain)
        def widen(x):
            return jnp.concatenate([x, jnp.zeros_like(x)], 1)

        def table(i):
            return up[0, 16 * i : 16 * (i + 1), :m], up[1, 16 * i : 16 * (i + 1), :m]

        def correct(d):
            d1, d2, d3 = d
            e1 = split(d1)
            main = d3 + small[10] * d2 + small[11] * d1
            rows = dotk(ends[0], d2 + small[12] * d1) + dotk(ends[1], e1)
            cols = dot3t(table(2), d2 + small[13] * d1) + dot3t(table(3), e1)
            corner = dot3(dotk(ends[0], e1), (up[0, 64:], up[1, 64:]))
            return jnp.concatenate([pack(main), (widen(rows + cols) + corner)[:8]], 0)

        def mend(i, g):
            return remote(
                zbuf.at[i], fix.at[level], b_send, f_recv.at[part], g, k - 1 + i
            )

        def tell(i, g):
            return remote(
                mail.at[i], modes.at[level], b_send, m_recv, g, k - 1 + i
            )

        def give(copy, i):
            def one(j):
                g = jnp.where(2 * px < PX, G - 1 - j, j)
                if i == 0:
                    copy(i, g).start()
                else:
                    @pl.when(g != me)
                    def _():
                        copy(i, g).start()
            loop(G, one)

        def advance():
            mail[0] = pack(c_lead[W - 1])
            give(tell, 0)
            zbuf[0] = correct(d_lead)
            give(mend, 0)

        @pl.when(k >= nests - 2)
        def _():
            advance()

        d_own, c_own = nudge(after, follow(c_lead, own_maps), gain)
        for w in range(W):
            cbuf[w] = pack(c_own[w])

        @pl.when(k < nests - 2)
        def _():
            chain_out.start()

        @pl.when(k < 2)
        def _():
            widen_patch()

        @pl.when(k < nests - 2)
        def _():
            advance()

        zbuf[1] = correct(d_own)
        give(mend, 1)
        mail[1] = pack(c_own[W - 1])
        give(tell, 1)
        keep_fix.start()
        keep_modes.start()
        run_free()

    @pl.when(jnp.logical_not(is_owner))
    def _():
        widen_patch()
        run_free()

    tables[2].wait()
    tables[3].wait()

    u_wide = tri((u_t[0], u_t[1]))
    most = L // 2
    far = jnp.where(2 * px < PX, 0, 1)
    for i in range(2):
        turn = (i + far) % 2
        first = turn * most
        some = pl.ds(first, most)
        settled(fix.at[some], f_recv.at[turn])
        half = [dot3(unpack_fix(fix[first + j], m), (vt_t[0], vt_t[1])) for j in range(most)]
        done = [calm[first + j] + dotk(u_wide, half[j]) for j in range(most)]
        for j in range(most):
            state[first + j] = done[j]
        pltpu.make_async_copy(state.at[some], out.at[some], out_sem).start()
    settled(modes, m_recv)

    @pl.when(jnp.logical_not(is_owner))
    def _():
        settled(pbuf, a_send)

    @pl.when(is_owner)
    def _():
        settled(pbuf.at[pl.ds(0, L - 1)], a_send)
        settled(tally, b_send)

        @pl.when(k < nests - 2)
        def _():
            chain_out.wait_send()

    @pl.when(is_spare)
    def _():
        gain_out.wait_send()

    settle_halo(0, h_send.at[0])
    settle_halo(1, h_send.at[1])
    settled(state, out_sem)


def store(state, packed, state_out, modes_out, modes, sem):
    first = pltpu.make_async_copy(state, state_out.at[0], sem.at[0])
    second = pltpu.make_async_copy(modes, modes_out.at[0], sem.at[1])
    first.start()
    for l in range(packed.shape[0]):
        modes[l] = unpack(packed[l])
    second.start()
    first.wait()
    second.wait()


def wide_tables(cells, modes, windows):
    stages = powers(basis(cells, modes, 1), windows)
    edges = np.zeros((cells, modes))
    for e in range(windows):
        edges[e, 2 * e] = 1.0
        edges[cells - 1 - e, 2 * e + 1] = 1.0
    full = np.concatenate([stages[0], edges], 1)
    rate = 0.5 - 2 * RATE + 2 * RATE * np.cos(np.pi * np.arange(modes) / cells)
    turns = []
    for i, t in enumerate(stages):
        top = np.diag(rate**i)
        turns.append(np.concatenate([top, edges.T @ (t - stages[0] @ top)], 0))
    return stages, full, turns, rate


def body(dims, owners, initial_state, drive_modes, relax_rates, nest_offsets):
    nests, PY, PX, L, cx, cy, m, W = dims
    G, nx, ny = PY * PX, cx * PX, cy * PY
    assert nests % 2 == 0 and L % 2 == 0 and W == 3
    tall, lanes = m + 16, 2 * m
    rp, u, tu, rate_x = wide_tables(nx, m, W)
    cp, v, tv, rate_y = wide_tables(ny, m, W)
    few = 2 * (W - 1)
    u_few, v_few = u[:, :tall].copy(), np.zeros((ny, tall))
    u_few[:, m + few :] = 0.0
    v_few[:, :m] = v[:, :m]
    v_few[:, m + 4 : m + 4 + few] = v[:, m : m + few]
    both = rate_x[:, None] + rate_y[None, :]
    ends = np.zeros((4, 16, m))
    ends[0, :few], ends[1, :few] = tu[1][m : m + few], tu[2][m : m + few]
    ends[2, 4 : 4 + few], ends[3, 4 : 4 + few] = tv[1][m : m + few], tv[2][m : m + few]
    corner = np.zeros((m, lanes))
    corner[:, m + 4 : m + 4 + few] = 2.0 * tv[1][m : m + few].T
    a = [rp[0].T @ t for t in rp]
    b = [cp[0].T @ t for t in cp]
    even_x, odd_x = (rp[0].T @ basis(nx, m, RATIO, f) for f in (np.cos, np.sin))
    even_y, odd_y = ((cp[0].T @ basis(ny, m, RATIO, f)).T for f in (np.cos, np.sin))
    small = np.stack(
        [even_x, odd_x, even_y, odd_y, a[1], a[2], a[1] @ a[1], b[1], b[2], b[1] @ b[1],
         both, both**2, np.tile(2.0 * rate_y[None, :], (m, 1)), np.tile(2.0 * rate_x[:, None], (1, m)),
         both**3, np.tile(3.0 * rate_x[:, None] ** 2, (1, m))]
    ).astype(np.float32)
    here = halves(np.swapaxes(u[:, :tall].reshape(PX, cx, tall), 1, 2))
    tables = [
        halves(u_few),
        np.concatenate([here[0], here[0], here[1]], -1),
        halves(v),
        halves(v_few.T),
        halves(np.concatenate([t[m:tall].T for t in tu[1:]], 1)),
        halves(np.concatenate(tv[1:3] + [t[m : m + 16] for t in tv[1:]], 0)),
        halves(np.concatenate([np.pad(ends.reshape(64, m), ((0, 0), (0, m))), corner], 0)),
    ]
    any_space = pl.BlockSpec(memory_space=pl.ANY)
    vmem = pl.BlockSpec(memory_space=pltpu.VMEM)
    dma = pltpu.SemaphoreType.DMA
    coeffs = pltpu.VMEM((W, m // 2, lanes), F32)
    thin = m // 2 + 16
    held = pl.pallas_call(
        functools.partial(kernel, dims, owners),
        out_shape=(
            pltpu.VMEM((L, cx, cy), F32),
            pltpu.VMEM((L, m // 2, lanes), F32),
        ),
        in_specs=[any_space] * 12,
        out_specs=(any_space, any_space),
        scratch_shapes=[
            pltpu.VMEM((L, cx, cy), F32),
            pltpu.VMEM((L, thin, lanes), F32),
            pltpu.VMEM((2 * G, thin, lanes), F32),
            pltpu.VMEM((cx * L // 16, 128), F32),
            pltpu.VMEM((2, cx * L // 16, 128), F32),
            pltpu.VMEM((L, cx + 16, cy + 128), F32),
            pltpu.VMEM((L, cx, cy), F32),
            pltpu.VMEM((L, cx, cy), F32),
            pltpu.VMEM((L, m // 2 + 8, lanes), F32),
            pltpu.VMEM((2 * G - 1, m + 8, lanes), F32),
            pltpu.VMEM((2, cx, tall), BF16),
            pltpu.VMEM((2, tall, cy), BF16),
            pltpu.VMEM((2, m // 2 + 8, lanes), F32),
            pltpu.VMEM((2, m // 2, lanes), F32),
            pltpu.VMEM((W, m, m), F32),
            coeffs,
            coeffs,
            pltpu.VMEM((8, 128), F32),
            pltpu.VMEM((8, 128), F32),
            pltpu.VMEM((5, m, m), F32),
            pltpu.VMEM((tall, 3 * cx), BF16),
            pltpu.VMEM((2, cy, lanes), BF16),
            pltpu.VMEM((2, m, 16 * W), BF16),
            pltpu.VMEM((2, 4 * m + 16 * W, m), BF16),
            pltpu.VMEM((2, 64 + m, lanes), BF16),
            pltpu.VMEM((16, m, m), F32),
            pltpu.SMEM(relax_rates.shape, F32),
            pltpu.SMEM(nest_offsets.shape[::-1], jnp.int32),
            dma((12,)),
            dma,
            dma,
            dma((2,)),
            dma((2,)),
            dma((2,)),
            dma((2,)),
            dma,
            dma,
            dma((2,)),
            dma,
        ],
        compiler_params=pltpu.CompilerParams(collective_id=0, has_side_effects=True),
    )(initial_state, drive_modes, relax_rates, nest_offsets.T,
      *(jnp.asarray(t) for t in tables), jnp.asarray(small))
    return pl.pallas_call(
        store,
        out_shape=[
            jax.ShapeDtypeStruct((1, L, cx, cy), F32),
            jax.ShapeDtypeStruct((1, L, m, m), F32),
        ],
        in_specs=[any_space, vmem],
        out_specs=[any_space] * 2,
        scratch_shapes=[pltpu.VMEM((L, m, m), F32), dma((2,))],
    )(*(pltpu.with_memory_space_constraint(x, pltpu.VMEM) for x in held))


def solution(mesh):
    nests, PY, PX = (mesh.shape[n] for n in ("nest", "py", "px"))
    spec = P("nest", None, "px", "py")

    def local(initial_state, drive_modes, relax_rates, nest_offsets):
        _, L, cx, cy = initial_state.shape
        W, _, m, _ = drive_modes.shape
        places = sorted(
            range(PY * PX),
            key=lambda g: (abs(2 * (g // PY) - PX + 1) + abs(2 * (g % PY) - PY + 1), g),
        )
        dims = (nests, PY, PX, L, cx, cy, m, W)
        return body(dims, tuple(places[:L]), initial_state, drive_modes, relax_rates, nest_offsets)

    return jax.shard_map(
        local,
        mesh=mesh,
        in_specs=(spec, P(), P("nest", None), P()),
        out_specs=(spec, P("nest", None, None, None)),
        check_vma=False,
    )
```

```python
import functools
import math

import jax
import jax.numpy as jnp
import numpy as np
from jax import lax
from jax.experimental import pallas as pl
from jax.experimental.pallas import tpu as pltpu
from jax.sharding import PartitionSpec as P

RATIO = 3
RATE = 0.2
MESH = pl.DeviceIdType.MESH
F32, BF16 = jnp.float32, jnp.bfloat16


def basis(cells, modes, refine, fn=np.cos):
    j = np.arange(modes, dtype=np.int64)
    q = 2 * np.arange(cells, dtype=np.int64) + 1
    product = (j[None, :] * q[:, None]) % (4 * refine * cells)
    weight = np.where(j == 0, 1.0, 2.0) / cells
    return np.sqrt(weight)[None, :] * fn(np.pi * product / (2.0 * refine * cells))


def half_step(table):
    pad = np.pad(table, ((1, 1), (0, 0)))
    return (0.5 - 2 * RATE) * table + RATE * (pad[2:] + pad[:-2])


def powers(table, count):
    out = [table]
    for _ in range(count):
        out.append(half_step(out[-1]))
    return out


def halves(table):
    high = np.asarray(table, np.float32).astype(BF16)
    low = (np.asarray(table, np.float64) - high.astype(np.float64)).astype(np.float32)
    return np.stack([high, low.astype(BF16)])


def split(x):
    high = x.astype(BF16)
    return high, (x - high.astype(F32)).astype(BF16)


def mm(a, b):
    return lax.dot_general(a, b, (((1,), (0,)), ((), ())), preferred_element_type=F32)


def dot3(a, b):
    a = a if isinstance(a, tuple) else split(a)
    b = b if isinstance(b, tuple) else split(b)
    return mm(a[0], b[0]) + (mm(a[0], b[1]) + mm(a[1], b[0]))


def dot3t(a, b):
    b = b if isinstance(b, tuple) else split(b)

    def nt(x, y):
        return lax.dot_general(x, y, (((1,), (1,)), ((), ())), preferred_element_type=F32)

    return nt(a[0], b[0]) + (nt(a[0], b[1]) + nt(a[1], b[0]))


def tri(a):
    return jnp.concatenate([a[0], a[0], a[1]], 1)


def dotk(a, b):
    b = b if isinstance(b, tuple) else split(b)
    return mm(a, jnp.concatenate([b[0], b[1], b[0]], 0))


def stack(*parts):
    if isinstance(parts[0], tuple):
        return tuple(jnp.concatenate(p, 0) for p in zip(*parts))
    return jnp.concatenate(parts, 0)


def pack(x):
    h = x.shape[0] // 2
    return jnp.concatenate([x[:h], x[h:]], 1)


def unpack(x):
    h = x.shape[1] // 2
    return jnp.concatenate([x[:, :h], x[:, h:]], 0)


def pack_wide(x, m):
    low = x[:m].T[m : m + 8]
    return jnp.concatenate(
        [pack(x[:m, :m]), x[m : m + 8], jnp.concatenate([low, jnp.zeros_like(low)], 1)], 0
    )


def unpack_fix(x, m):
    tile = x[m // 2 :]
    low = jnp.concatenate([tile[:, :m], jnp.zeros((m - 8, m), F32)], 0).T
    top = jnp.concatenate([unpack(x[: m // 2]), low], 1)
    return jnp.concatenate([top, tile, jnp.zeros((8, 2 * m), F32)], 0)[:, : m + 16]


def unpack_wide(x, m):
    low = jnp.concatenate([x[m // 2 + 8 :, :m], jnp.zeros((m - 8, m), F32)], 0).T
    top = jnp.concatenate([unpack(x[: m // 2]), low], 1)
    return jnp.concatenate([top, x[m // 2 : m // 2 + 8], jnp.zeros((8, 2 * m), F32)], 0)


def loop(n, fn):
    if n <= 16:
        for i in range(n):
            fn(i)
    else:
        lax.fori_loop(0, n, lambda i, c: (fn(i), c)[1], 0)


def kernel(
    dims, owners,
    field, drive, relax_hbm, offs_hbm,
    u_hbm, ut_hbm, v_hbm, vt_hbm, up_hbm, small_hbm,
    out, modes,
    fvm, pbuf, abuf, strip, near, wide, calm, state, fix, tally, u_t, vt_t, zbuf, mail, start, par, cbuf, lead, glead, tx,
    ut_t, v_t, up, small, relax, offs,
    load_sem, a_send, a_recv, h_send, h_recv, c_sem, g_sem, out_sem, b_send, f_recv, m_recv,
):
    nests, PY, PX, L, cx, cy, m, W = dims
    G, nx, ny = PY * PX, cx * PX, cy * PY
    k, py, px = lax.axis_index("nest"), lax.axis_index("py"), lax.axis_index("px")
    me = px * PY + py
    odd = k % 2 == 1
    leader = k + 1 - k % 2
    placed = [me == o for o in owners]
    level = sum(jnp.where(c, l, 0) for l, c in enumerate(placed))
    in_place = functools.reduce(jnp.logical_or, placed)
    is_owner = jnp.logical_and(odd, in_place)
    is_spare = jnp.logical_and(jnp.logical_not(odd), in_place)
    owns = [jnp.logical_and(odd, c) for c in placed]

    def at(g, nest):
        return (nest, g % PY, g // PY)

    def plain(g):
        return functools.reduce(jnp.logical_and, [g != o for o in owners])

    hops = [(-2, k > 2), (2, k < nests - 2)]
    sides = [
        (px > 0, (k, py, px - 1)), (px < PX - 1, (k, py, px + 1)),
        (py > 0, (k, py - 1, px)), (py < PY - 1, (k, py + 1, px)),
    ]
    beside = sum(jnp.where(c, 1, 0) for c, _ in sides)
    barrier = pltpu.get_barrier_semaphore()

    @pl.when(is_owner)
    def _():
        def greet(g):
            pl.semaphore_signal(barrier, inc=1, device_id=at(g, k - 1), device_id_type=MESH)

            @pl.when(plain(g))
            def _():
                pl.semaphore_signal(barrier, inc=1, device_id=at(g, k), device_id_type=MESH)
        loop(G, greet)

    load = pltpu.make_async_copy(field.at[0], fvm, load_sem.at[0])
    load.start()
    rows_here = pl.ds(pl.multiple_of(px * cx, 8), cx)
    cols_here = pl.ds(pl.multiple_of(py * cy, 128), cy)
    pairs = [
        (v_hbm.at[:, cols_here], v_t), (ut_hbm.at[px], ut_t),
        (u_hbm.at[:, rows_here], u_t), (vt_hbm.at[:, :, cols_here], vt_t),
        (relax_hbm, relax), (offs_hbm, offs), (small_hbm, small),
        (up_hbm, up),
    ]
    tables = [
        pltpu.make_async_copy(src, dst, load_sem.at[2 + i]) for i, (src, dst) in enumerate(pairs)
    ]
    for c in tables[:4]:
        c.start()
    for l, o in enumerate(owners):
        @pl.when(jnp.logical_not(owns[l]))
        def _():
            pl.semaphore_signal(barrier, inc=1, device_id=at(o, leader), device_id_type=MESH)

    for cond, device in sides:
        @pl.when(cond)
        def _():
            pl.semaphore_signal(barrier, inc=1, device_id=device, device_id_type=MESH)

    @pl.when(is_owner)
    def _():
        for hop, cond in hops:
            @pl.when(cond)
            def _():
                pl.semaphore_signal(
                    barrier, inc=1, device_id=(k + hop, py, px), device_id_type=MESH
                )

    def hop_copy(src, dst, send_sem, recv_sem, hop):
        return pltpu.make_async_remote_copy(
            src_ref=src, dst_ref=dst, send_sem=send_sem, recv_sem=recv_sem,
            device_id=(k + hop, py, px), device_id_type=MESH,
        )

    gain_out = hop_copy(lead, glead, g_sem.at[0], g_sem.at[1], 1)
    gain_in = hop_copy(lead, glead, g_sem.at[0], g_sem.at[1], -1)
    chain_out = hop_copy(cbuf, par, c_sem.at[0], c_sem.at[1], 2)
    chain_in = hop_copy(cbuf, par, c_sem.at[0], c_sem.at[1], -2)

    get_drive = pltpu.make_async_copy(drive.at[:, level], start, load_sem.at[1])

    @pl.when(in_place)
    def _():
        tables[4].start()

    @pl.when(is_owner)
    def _():
        for c in tables[5:]:
            c.start()

        @pl.when(k < 2)
        def _():
            get_drive.start()

    tables[0].wait()
    tables[1].wait()
    load.wait()
    half = dot3(fvm[...].reshape(L * cx, cy), (v_t[0], v_t[1]))
    for l in range(L):
        pbuf[l] = pack_wide(dotk(ut_t[...], half[l * cx : (l + 1) * cx]), m)

    @pl.when(is_owner)
    def _():
        abuf[G + me] = pbuf[level]
        pl.semaphore_wait(barrier, beside + 2 * G - 1 + sum(jnp.where(c, 1, 0) for _, c in hops))

    @pl.when(jnp.logical_not(is_owner))
    def _():
        pl.semaphore_wait(barrier, beside + L)

    def remote(src, dst, send_sem, recv_sem, g, nest):
        return pltpu.make_async_remote_copy(
            src_ref=src, dst_ref=dst, send_sem=send_sem, recv_sem=recv_sem,
            device_id=at(g, nest), device_id_type=MESH,
        )

    def share(l):
        return remote(
            pbuf.at[l], abuf.at[(k % 2) * G + me], a_send, a_recv, owners[l], leader
        )

    def settled(ref, sem):
        pltpu.make_async_copy(ref, ref, sem).wait()

    part = jnp.where(level < L // 2, 0, 1)
    keep_modes = pltpu.make_async_copy(mail.at[1], modes.at[level], m_recv)
    keep_fix = pltpu.make_async_copy(zbuf.at[1], fix.at[level], f_recv.at[part])

    def beam(src, dst, i, device):
        return pltpu.make_async_remote_copy(
            src_ref=src, dst_ref=dst, send_sem=h_send.at[i // 2], recv_sem=h_recv.at[i // 2],
            device_id=device, device_id_type=MESH,
        )

    top, bottom = pl.ds(0, 8), pl.ds(cx + 8, 8)
    first_rows, last_rows = pl.ds(8, 8), pl.ds(cx, 8)
    halo = [
        beam(wide.at[:, first_rows], wide.at[:, bottom], 0, sides[0][1]),
        beam(wide.at[:, last_rows], wide.at[:, top], 1, sides[1][1]),
        beam(strip, near.at[1], 2, sides[2][1]),
        beam(strip, near.at[0], 3, sides[3][1]),
    ]

    def start_halo(i):
        @pl.when(sides[i][0])
        def _():
            halo[i].start()

    def settle_halo(i, sem):
        lower, upper = sides[2 * i][0], sides[2 * i + 1][0]
        two, one = (wide.at[:, pl.ds(0, 16)], wide.at[:, pl.ds(0, 8)]) if i == 0 else (near, near.at[0])

        @pl.when(jnp.logical_and(lower, upper))
        def _():
            settled(two, sem)

        @pl.when(lower != upper)
        def _():
            settled(one, sem)

    for l, o in enumerate(owners):
        @pl.when(jnp.logical_not(owns[l]))
        def _():
            share(l).start()

    @pl.when(is_spare)
    def _():
        tables[4].wait()
        lead[...] = jnp.full(lead.shape, relax[0, level], F32)
        gain_out.start()

    lane = lax.broadcasted_iota(jnp.int32, (cx, 128), 1)
    edge = jnp.zeros((cx, 128), F32)
    for l in range(L):
        ends = jnp.where(lane < 64, fvm[l, :, 0:128], fvm[l, :, cy - 128 : cy])
        turned = pltpu.roll(ends, 8 * l, 1) if l else ends
        shift = (lane - 8 * l + 4) % 128
        edge = jnp.where(shift < 8, turned, edge)
        wide[l, 8 : cx + 8, 0:cy] = fvm[l]
    folds = 128 // (8 * L)
    thin = cx // folds
    short = lax.broadcasted_iota(jnp.int32, (thin, 128), 1)
    folded = edge[:thin]
    for i in range(1, folds):
        moved = pltpu.roll(edge[i * thin : (i + 1) * thin], 8 * L * i, 1)
        folded = jnp.where((short + 4) % 128 < 8 * L * i, folded, moved)
    strip[...] = folded
    bare = jnp.zeros((8, cy + 128), F32)

    @pl.when(px == 0)
    def _():
        for l in range(L):
            wide[l, 0:8, :] = bare

    @pl.when(px == PX - 1)
    def _():
        for l in range(L):
            wide[l, cx + 8 : cx + 16, :] = bare

    @pl.when(py == 0)
    def _():
        near[0] = jnp.zeros(near.shape[1:], F32)

    @pl.when(py == PY - 1)
    def _():
        near[1] = jnp.zeros(near.shape[1:], F32)

    start_halo(2)
    start_halo(3)

    def widen_patch():
        settle_halo(1, h_recv.at[1])
        after, before = near[1], near[0]
        for l in range(L):
            for i in range(folds):
                back = (128 - 8 * l - 8 * L * i) % 128
                right, left_side = after, before
                if back:
                    right, left_side = pltpu.roll(after, back, 1), pltpu.roll(before, back, 1)
                wide[l, 8 + i * thin : 8 + (i + 1) * thin, cy:] = jnp.where(
                    short < 64, right, left_side
                )
        start_halo(0)
        start_halo(1)

    def run_free():
        settle_halo(0, h_recv.at[0])
        shape = (cx + 16, cy + 128)
        row = lax.broadcasted_iota(jnp.int32, shape, 0) + (px * cx - 8)
        col = lax.broadcasted_iota(jnp.int32, shape, 1)
        col = jnp.where(col < cy + 64, col, col - (cy + 128)) + py * cy
        inside = (row >= 0) & (row < nx) & (col >= 0) & (col < ny)
        for l in range(L):
            now = wide[l]
            for _ in range(W):
                side = pltpu.roll(now, 1, 0) + pltpu.roll(now, cx + 15, 0)
                side = side + pltpu.roll(now, 1, 1) + pltpu.roll(now, cy + 127, 1)
                now = jnp.where(inside, now + RATE * (side - 4.0 * now), 0.0)
            calm[l] = now[8 : cx + 8, 0:cy]

    @pl.when(is_owner)
    def _():
        tables[4].wait()
        tables[5].wait()
        tables[6].wait()
        gain = relax[0, level]

        def turn(kk, cells, dim, axis):
            number = lax.broadcasted_iota(jnp.int32, (m, m), dim).astype(F32)
            product = number * (2 * RATIO * offs[axis, kk]).astype(F32)
            period = float(4 * RATIO * cells)
            product = product - period * jnp.floor(product * (1.0 / period))
            angle = product * (math.pi / (2.0 * RATIO * cells))
            return jnp.cos(angle), jnp.sin(angle)

        def flat(kk):
            eye = jnp.where(
                lax.broadcasted_iota(jnp.int32, (m, m), 0)
                == lax.broadcasted_iota(jnp.int32, (m, m), 1),
                1.0, 0.0,
            ).astype(F32)
            cos_x, sin_x = turn(kk, nx, 1, 0)
            cos_y, sin_y = turn(kk, ny, 0, 1)
            row = jnp.where(kk == 0, eye, small[0] * cos_x - small[1] * sin_x)
            col = jnp.where(kk == 0, eye, small[2] * cos_y - small[3] * sin_y)
            return split(row), split(col)

        a1, b1 = split(small[4]), split(small[7])

        def curved(rate):
            return split(small[5] - rate * small[6]), split(small[8] - rate * small[9])

        def maps(kk, rate):
            a2, b2 = curved(rate)
            f0, g0 = flat(kk)
            f1, f2 = split(dot3(a1, f0)), split(dot3(a2, f0))
            f01 = tuple(jnp.concatenate(p, 1) for p in zip(f0, f1))
            g1, g2 = split(dot3(g0, b1)), split(dot3(g0, b2))
            return tri(f0), tri(stack(f0, f1, f2)), tri(f01), g0, g1, g2, 2.0 * (1.0 - rate)

        def follow(cs, ms):
            f0, f012, f01, g0, g1, g2, rest = ms
            c1, c2, c3 = (split(c) for c in cs)
            y0 = dot3(stack(c1, c2, c3), g0)
            y1 = dot3(stack(c1, c2), g1)
            y12 = dot3(c1, g2)
            y10, y20, y30 = y0[:m], y0[m : 2 * m], y0[2 * m :]
            y11, y21 = y1[:m], y1[m:]
            z = dotk(f012, y10)
            return (
                z[:m],
                dotk(f0, y20),
                dotk(f0, y30),
                z[m : 2 * m] + dotk(f0, y11),
                z[2 * m :] + dotk(f01, stack(y21 + y12, y20 + rest * y11)),
            )

        def nudge(own, moved, rate):
            own2, own3 = own[1] + rate * moved[3], own[2] + rate * moved[4]
            d1, d2, d3 = rate * (moved[0] - own[0]), rate * (moved[1] - own2), rate * (moved[2] - own3)
            return (d1, d2, d3), (own[0] + d1, own2 + d2, own3 + d3)

        own_maps = maps(k, gain)
        gain_in.wait_recv()
        lead_gain = glead[0:1, 0:m]
        lead_maps = maps(k - 1, lead_gain)

        def both_sides(rate):
            a2, b2 = curved(rate)
            return tri(a1), tri(stack(a1, a2)), b2

        sides_lead, sides_own = both_sides(lead_gain), both_sides(gain)

        def first(cs):
            for i, x in enumerate(follow(cs, lead_maps)):
                tx[i] = x

        @pl.when(k < 2)
        def _():
            get_drive.wait()
            first([start[w] for w in range(W)])

        tables[7].wait()

        grown = [tri((up[0, 64 + m : 64 + 2 * m, : 16 * i], up[1, 64 + m : 64 + 2 * m, : 16 * i])) for i in (1, 2, 3)]
        ends = [tri((up[0, 16 * i : 16 * i + 16, :m], up[1, 16 * i : 16 * i + 16, :m])) for i in (0, 1)]
        settled(abuf.at[pl.ds(0, 2 * G - 1)], a_recv)

        def gathered(i):
            total = abuf[i * G]
            if G <= 16:
                for g in range(1, G):
                    total = total + abuf[i * G + g]
            else:
                total = lax.fori_loop(1, G, lambda g, c: c + abuf[i * G + g], total)
            return total

        def table(start, size):
            start += 64 + 2 * m
            return up[0, start : start + size, :m], up[1, start : start + size, :m]

        def rows(*parts):
            return dotk(grown[len(parts) - 1], jnp.concatenate(parts, 0))

        totals = [gathered(i) for i in range(2)]
        lows, edges = [], []
        for t in totals:
            low = t[m // 2 + 8 :, :m]
            lows.append(jnp.concatenate([low, jnp.zeros((m - 8, m), F32)], 0).T[:, :16])
            edges.append(t[m // 2 : m // 2 + 8])
        lows, edges_s = split(stack(*lows)), split(stack(*edges))
        row1, row2 = (dot3(edges_s, table(2 * m * j, 2 * m)) for j in range(2))
        q1, q2, q3 = (dot3(lows, table(4 * m + 16 * j, 16)) for j in range(3))

        def project(i):
            main = unpack(totals[i][: m // 2])
            none = jnp.zeros((8, m), F32)
            r0 = stack(edges[i][:, :m], none)
            r1, r2 = (stack(r[8 * i : 8 * i + 8], none) for r in (row1, row2))
            p1, p2, p3 = (q[i * m : (i + 1) * m] for q in (q1, q2, q3))
            return [
                small[10] * main + (rows(r0) + p1),
                small[11] * main + (rows(2.0 * r1, r0) + small[13] * p1 + p2),
                small[14] * main
                + (rows(3.0 * r2, 3.0 * r1, r0) + small[15] * p1 + 1.5 * small[13] * p2 + p3),
            ]

        def settle(s, rate, sides):
            s1, s2, s3 = s
            a1, a12, b2 = sides
            s1s, s2s = split(s1), split(s2)
            by_b = dot3(stack(s1s, s2s), b1)
            by_a = dotk(a12, s1s)
            x2 = by_a[:m] + by_b[:m]
            x3 = by_b[m:] + dot3(s1s, b2) + by_a[m:]
            x3 = x3 + dotk(a1, s2 + 2.0 * (1.0 - rate) * by_b[:m])
            return s1, s2 - rate * x2, s3 - rate * x3

        before, after = project(0), project(1)
        before, after = settle(before, lead_gain, sides_lead), settle(after, gain, sides_own)

        @pl.when(k > 1)
        def _():
            widen_patch()
            chain_in.wait_recv()
            first([unpack(par[w]) for w in range(W)])

        d_lead, c_lead = nudge(before, [tx[i] for i in range(5)], lead_gain)
        def widen(x):
            return jnp.concatenate([x, jnp.zeros_like(x)], 1)

        def table(i):
            return up[0, 16 * i : 16 * (i + 1), :m], up[1, 16 * i : 16 * (i + 1), :m]

        def correct(d):
            d1, d2, d3 = d
            e1 = split(d1)
            main = d3 + small[10] * d2 + small[11] * d1
            rows = dotk(ends[0], d2 + small[12] * d1) + dotk(ends[1], e1)
            cols = dot3t(table(2), d2 + small[13] * d1) + dot3t(table(3), e1)
            corner = dot3(dotk(ends[0], e1), (up[0, 64 : 64 + m], up[1, 64 : 64 + m]))
            return jnp.concatenate([pack(main), (widen(rows + cols) + corner)[:8]], 0)

        def mend(i, g):
            return remote(
                zbuf.at[i], fix.at[level], b_send, f_recv.at[part], g, k - 1 + i
            )

        def tell(i, g):
            return remote(
                mail.at[i], modes.at[level], b_send, m_recv, g, k - 1 + i
            )

        def give(copy, i):
            def one(j):
                g = j
                if i == 0:
                    copy(i, g).start()
                else:
                    @pl.when(g != me)
                    def _():
                        copy(i, g).start()
            loop(G, one)

        def advance():
            mail[0] = pack(c_lead[W - 1])
            give(tell, 0)
            zbuf[0] = correct(d_lead)
            give(mend, 0)

        @pl.when(k >= nests - 2)
        def _():
            advance()

        d_own, c_own = nudge(after, follow(c_lead, own_maps), gain)
        for w in range(W):
            cbuf[w] = pack(c_own[w])

        @pl.when(k < nests - 2)
        def _():
            chain_out.start()

        @pl.when(k < 2)
        def _():
            widen_patch()

        @pl.when(k < nests - 2)
        def _():
            advance()

        zbuf[1] = correct(d_own)
        give(mend, 1)
        mail[1] = pack(c_own[W - 1])
        give(tell, 1)
        keep_fix.start()
        keep_modes.start()
        run_free()

    @pl.when(jnp.logical_not(is_owner))
    def _():
        widen_patch()
        run_free()

    tables[2].wait()
    tables[3].wait()

    u_wide = tri((u_t[0], u_t[1]))
    most = L // 2
    far = jnp.where(2 * px < PX, 0, 1)
    for i in range(2):
        turn = (i + far) % 2
        first = turn * most
        some = pl.ds(first, most)
        settled(fix.at[some], f_recv.at[turn])
        half = [dot3(unpack_fix(fix[first + j], m), (vt_t[0], vt_t[1])) for j in range(most)]
        done = [calm[first + j] + dotk(u_wide, half[j]) for j in range(most)]
        for j in range(most):
            state[first + j] = done[j]
        pltpu.make_async_copy(state.at[some], out.at[some], out_sem).start()
    settled(modes, m_recv)

    @pl.when(jnp.logical_not(is_owner))
    def _():
        settled(pbuf, a_send)

    @pl.when(is_owner)
    def _():
        settled(pbuf.at[pl.ds(0, L - 1)], a_send)
        settled(tally, b_send)

        @pl.when(k < nests - 2)
        def _():
            chain_out.wait_send()

    @pl.when(is_spare)
    def _():
        gain_out.wait_send()

    settle_halo(0, h_send.at[0])
    settle_halo(1, h_send.at[1])
    settled(state, out_sem)


def store(state, packed, state_out, modes_out, modes, sem):
    first = pltpu.make_async_copy(state, state_out.at[0], sem.at[0])
    second = pltpu.make_async_copy(modes, modes_out.at[0], sem.at[1])
    first.start()
    for l in range(packed.shape[0]):
        modes[l] = unpack(packed[l])
    second.start()
    first.wait()
    second.wait()


def wide_tables(cells, modes, windows):
    stages = powers(basis(cells, modes, 1), windows)
    edges = np.zeros((cells, modes))
    for e in range(windows):
        edges[e, 2 * e] = 1.0
        edges[cells - 1 - e, 2 * e + 1] = 1.0
    full = np.concatenate([stages[0], edges], 1)
    rate = 0.5 - 2 * RATE + 2 * RATE * np.cos(np.pi * np.arange(modes) / cells)
    turns = []
    for i, t in enumerate(stages):
        top = np.diag(rate**i)
        turns.append(np.concatenate([top, edges.T @ (t - stages[0] @ top)], 0))
    return stages, full, turns, rate


def body(dims, owners, initial_state, drive_modes, relax_rates, nest_offsets):
    nests, PY, PX, L, cx, cy, m, W = dims
    G, nx, ny = PY * PX, cx * PX, cy * PY
    assert nests % 2 == 0 and L % 2 == 0 and W == 3
    tall, lanes = m + 16, 2 * m
    rp, u, tu, rate_x = wide_tables(nx, m, W)
    cp, v, tv, rate_y = wide_tables(ny, m, W)
    few = 2 * (W - 1)
    u_few, v_few = u[:, :tall].copy(), np.zeros((ny, tall))
    u_few[:, m + few :] = 0.0
    v_few[:, :m] = v[:, :m]
    v_few[:, m + 4 : m + 4 + few] = v[:, m : m + few]
    both = rate_x[:, None] + rate_y[None, :]
    ends = np.zeros((4, 16, m))
    ends[0, :few], ends[1, :few] = tu[1][m : m + few], tu[2][m : m + few]
    ends[2, 4 : 4 + few], ends[3, 4 : 4 + few] = tv[1][m : m + few], tv[2][m : m + few]
    corner = np.zeros((m, lanes))
    corner[:, m + 4 : m + 4 + few] = 2.0 * tv[1][m : m + few].T
    a = [rp[0].T @ t for t in rp]
    b = [cp[0].T @ t for t in cp]
    even_x, odd_x = (rp[0].T @ basis(nx, m, RATIO, f) for f in (np.cos, np.sin))
    even_y, odd_y = ((cp[0].T @ basis(ny, m, RATIO, f)).T for f in (np.cos, np.sin))
    small = np.stack(
        [even_x, odd_x, even_y, odd_y, a[1], a[2], a[1] @ a[1], b[1], b[2], b[1] @ b[1],
         both, both**2, np.tile(2.0 * rate_y[None, :], (m, 1)), np.tile(2.0 * rate_x[:, None], (1, m)),
         both**3, np.tile(3.0 * rate_x[:, None] ** 2, (1, m))]
    ).astype(np.float32)
    here = halves(np.swapaxes(u[:, :tall].reshape(PX, cx, tall), 1, 2))
    tables = [
        halves(u_few),
        np.concatenate([here[0], here[0], here[1]], -1),
        halves(v),
        halves(v_few.T),
        halves(np.concatenate([
            np.pad(ends.reshape(64, m), ((0, 0), (0, m))),
            corner,
            np.pad(np.concatenate([t[m:tall].T for t in tu[1:]], 1), ((0, 0), (0, lanes - 16 * W))),
            np.pad(np.concatenate(tv[1:3] + [t[m : m + 16] for t in tv[1:]], 0), ((0, 0), (0, m))),
        ], 0)),
    ]
    any_space = pl.BlockSpec(memory_space=pl.ANY)
    vmem = pl.BlockSpec(memory_space=pltpu.VMEM)
    dma = pltpu.SemaphoreType.DMA
    coeffs = pltpu.VMEM((W, m // 2, lanes), F32)
    thin = m // 2 + 16
    held = pl.pallas_call(
        functools.partial(kernel, dims, owners),
        out_shape=(
            pltpu.VMEM((L, cx, cy), F32),
            pltpu.VMEM((L, m // 2, lanes), F32),
        ),
        in_specs=[any_space] * 10,
        out_specs=(any_space, any_space),
        scratch_shapes=[
            pltpu.VMEM((L, cx, cy), F32),
            pltpu.VMEM((L, thin, lanes), F32),
            pltpu.VMEM((2 * G, thin, lanes), F32),
            pltpu.VMEM((cx * L // 16, 128), F32),
            pltpu.VMEM((2, cx * L // 16, 128), F32),
            pltpu.VMEM((L, cx + 16, cy + 128), F32),
            pltpu.VMEM((L, cx, cy), F32),
            pltpu.VMEM((L, cx, cy), F32),
            pltpu.VMEM((L, m // 2 + 8, lanes), F32),
            pltpu.VMEM((2 * G - 1, m + 8, lanes), F32),
            pltpu.VMEM((2, cx, tall), BF16),
            pltpu.VMEM((2, tall, cy), BF16),
            pltpu.VMEM((2, m // 2 + 8, lanes), F32),
            pltpu.VMEM((2, m // 2, lanes), F32),
            pltpu.VMEM((W, m, m), F32),
            coeffs,
            coeffs,
            pltpu.VMEM((8, 128), F32),
            pltpu.VMEM((8, 128), F32),
            pltpu.VMEM((5, m, m), F32),
            pltpu.VMEM((tall, 3 * cx), BF16),
            pltpu.VMEM((2, cy, lanes), BF16),
            pltpu.VMEM((2, 64 + 6 * m + 16 * W, lanes), BF16),
            pltpu.VMEM((16, m, m), F32),
            pltpu.SMEM(relax_rates.shape, F32),
            pltpu.SMEM(nest_offsets.shape[::-1], jnp.int32),
            dma((10,)),
            dma,
            dma,
            dma((2,)),
            dma((2,)),
            dma((2,)),
            dma((2,)),
            dma,
            dma,
            dma((2,)),
            dma,
        ],
        compiler_params=pltpu.CompilerParams(collective_id=0, has_side_effects=True),
    )(initial_state, drive_modes, relax_rates, nest_offsets.T,
      *(jnp.asarray(t) for t in tables), jnp.asarray(small))
    return pl.pallas_call(
        store,
        out_shape=[
            jax.ShapeDtypeStruct((1, L, cx, cy), F32),
            jax.ShapeDtypeStruct((1, L, m, m), F32),
        ],
        in_specs=[any_space, vmem],
        out_specs=[any_space] * 2,
        scratch_shapes=[pltpu.VMEM((L, m, m), F32), dma((2,))],
    )(*(pltpu.with_memory_space_constraint(x, pltpu.VMEM) for x in held))


def solution(mesh):
    nests, PY, PX = (mesh.shape[n] for n in ("nest", "py", "px"))
    spec = P("nest", None, "px", "py")

    def local(initial_state, drive_modes, relax_rates, nest_offsets):
        _, L, cx, cy = initial_state.shape
        W, _, m, _ = drive_modes.shape
        places = sorted(
            range(PY * PX),
            key=lambda g: (abs(2 * (g // PY) - PX + 1) + abs(2 * (g % PY) - PY + 1), g),
        )
        dims = (nests, PY, PX, L, cx, cy, m, W)
        return body(dims, tuple(places[:L]), initial_state, drive_modes, relax_rates, nest_offsets)

    return jax.shard_map(
        local,
        mesh=mesh,
        in_specs=(spec, P(), P("nest", None), P()),
        out_specs=(spec, P("nest", None, None, None)),
        check_vma=False,
    )
```
